32 devices in a mesh: part: 4 (over x, y), fsdp: 8 (over z, core).
Axes of the slice: x: 2, y: 2, z: 4, core: 2. Of those that a mesh axis runs over, the one named last changes fastest.
Arguments:
- acts_in: bfloat16 [2, 65536, 768], P(None, ('part', 'fsdp')), parts along dimension 1
- cot_out: bfloat16 [2, 65536, 768], P(None, ('part', 'fsdp')), parts along dimension 1
- lengths: int32 [2, 32], P(None, ('part', 'fsdp')), parts along dimension 1
- w_up: bfloat16 [2, 768, 3072], replicated
- w_down: bfloat16 [2, 3072, 768], replicated
Outputs:
- output 1: float32 [8, 768, 3072], P('part', 'fsdp'), parts along dimension 0
- output 2: float32 [8, 3072, 768], P('part', 'fsdp'), parts along dimension 0
There are 4 independent parts. The reference program is written for one: setup_inputs(seed, part) draws one part's arguments, and reference() takes and returns one part's arrays. A program takes and returns all parts, laid end to end along the dimension named above; an argument that names none is the same for every part.
All inputs are finite; a program needn't handle non-finite values.
Results may differ from the reference program's by a relative error of at most 0.00977007.
Values are sent between devices in bfloat16 or wider.
A program may use at most 1 GiB of HBM per device.

```python
import jax
import jax.numpy as jnp
from jax import lax

MICRO = 2
TOK = 2048
LAYERS = 2
D = 768
FF = 3072
GROUP = 8

TOKENS = GROUP * TOK
LMIN = TOK // 4


def gelu_fwd(h_wide):
    return jax.nn.gelu(h_wide, approximate=True)


def gelu_back(h_wide, da_val):
    return jax.vjp(gelu_fwd, h_wide)[1](da_val)[0]


def draw_lengths(key_len):
    keys_len = jax.random.split(key_len, 2)
    base_len = jax.random.randint(keys_len[0], (MICRO, GROUP), LMIN, TOK + 1, jnp.int32)
    full_idx = jax.random.randint(keys_len[1], (MICRO, 1), 0, GROUP, jnp.int32)
    short_idx = (full_idx + 1) % GROUP
    col_ids = jnp.arange(GROUP, dtype=jnp.int32)[None, :]
    len_table = jnp.where(col_ids == full_idx, TOK, jnp.where(col_ids == short_idx, LMIN, base_len))
    return len_table.astype(jnp.int32)


def setup_inputs(seed: int = 0, part: int = 0) -> dict:
    key_part = jax.random.fold_in(jax.random.key(seed), part)
    keys_part = jax.random.split(key_part, 3)
    keys_shared = jax.random.split(jax.random.key(seed + 1), 2)
    acts_in = jax.random.normal(keys_part[0], (MICRO, TOKENS, D), jnp.float32)
    cot_out = jax.random.normal(keys_part[1], (MICRO, TOKENS, D), jnp.float32) * (MICRO * TOKENS) ** -0.5
    lengths = draw_lengths(keys_part[2])
    w_up = jax.random.normal(keys_shared[0], (LAYERS, D, FF), jnp.float32) * D ** -0.5
    w_down = jax.random.normal(keys_shared[1], (LAYERS, FF, D), jnp.float32) * FF ** -0.5
    return {
        "acts_in": acts_in.astype(jnp.bfloat16),
        "cot_out": cot_out.astype(jnp.bfloat16),
        "lengths": lengths,
        "w_up": w_up.astype(jnp.bfloat16),
        "w_down": w_down.astype(jnp.bfloat16),
    }


def micro_grads(acts_mb, cot_mb, w_up, w_down):
    def fwd_body(x_cur, weights):
        w_in, w_out = weights
        h_val = jnp.dot(x_cur, w_in, preferred_element_type=jnp.float32).astype(jnp.bfloat16)
        a_val = gelu_fwd(h_val.astype(jnp.float32)).astype(jnp.bfloat16)
        y_val = jnp.dot(a_val, w_out, preferred_element_type=jnp.float32).astype(jnp.bfloat16)
        x_next = (x_cur.astype(jnp.float32) + y_val.astype(jnp.float32)).astype(jnp.bfloat16)
        return x_next, (x_cur, h_val)

    _, (saved_x, saved_h) = lax.scan(fwd_body, acts_mb, (w_up, w_down))

    def bwd_body(dx_cur, layer_items):
        w_in, w_out, x_prev, h_val = layer_items
        h_wide = h_val.astype(jnp.float32)
        a_val = gelu_fwd(h_wide).astype(jnp.bfloat16)
        da_val = jnp.dot(dx_cur, w_out.T, preferred_element_type=jnp.float32)
        dh_val = gelu_back(h_wide, da_val).astype(jnp.bfloat16)
        grad_down = jnp.dot(a_val.T, dx_cur, preferred_element_type=jnp.float32)
        grad_up = jnp.dot(x_prev.T, dh_val, preferred_element_type=jnp.float32)
        dx_back = jnp.dot(dh_val, w_in.T, preferred_element_type=jnp.float32)
        dx_prev = (dx_cur.astype(jnp.float32) + dx_back).astype(jnp.bfloat16)
        return dx_prev, (grad_up, grad_down)

    _, (grads_up, grads_down) = lax.scan(bwd_body, cot_mb, (w_up, w_down, saved_x, saved_h), reverse=True)
    return grads_up, grads_down


def reference(acts_in, cot_out, lengths, w_up, w_down):
    valid_mask = jnp.arange(TOK)[None, None, :] < lengths[:, :, None]
    valid_mask = valid_mask.reshape(MICRO, TOKENS)
    cot_kept = jnp.where(valid_mask[:, :, None], cot_out, jnp.zeros_like(cot_out))

    def body(acc_pair, mb_items):
        acc_up, acc_down = acc_pair
        acts_mb, cot_mb = mb_items
        step_up, step_down = micro_grads(acts_mb, cot_mb, w_up, w_down)
        return (acc_up + step_up, acc_down + step_down), None

    zero_acc = (jnp.zeros((LAYERS, D, FF), jnp.float32), jnp.zeros((LAYERS, FF, D), jnp.float32))
    (grad_up, grad_down), _ = lax.scan(body, zero_acc, (acts_in, cot_kept))
    return grad_up, grad_down
```

```python
import functools

import jax
import jax.numpy as jnp
from jax import lax
from jax.experimental import pallas as pl
from jax.experimental.pallas import tpu as pltpu
from jax.sharding import PartitionSpec as P

MESH = pl.DeviceIdType.MESH
ANY = pl.BlockSpec(memory_space=pl.ANY)
F32 = jnp.float32
BF16 = jnp.bfloat16

C1 = 0.7978845608028654
K1 = C1 * 0.044715
K3 = 3.0 * K1

CHIPS = 4
FWD_LAG = 1
END_LAG = 4
SLOTS = 4


def dot(lhs, rhs, dims):
    return lax.dot_general(lhs, rhs, (dims, ((), ())), preferred_element_type=F32)


def gelu_parts(h_wide):
    sq = h_wide * h_wide
    th = jnp.tanh(h_wide * (C1 + K1 * sq))
    cdf = 0.5 + 0.5 * th
    return sq, th, cdf


def fwd_kernel(tiles, len_ref, x_ref, g_ref, w1_ref, w2_ref, x1_ref, r_ref, a_scr):
    step = pl.program_id(0)
    rows = x_ref.shape[0]
    left = len_ref[step // tiles] - (step % tiles) * rows
    row_ids = lax.broadcasted_iota(jnp.int32, r_ref.shape, 0)
    r_ref[...] = jnp.where(row_ids < left, g_ref[...], jnp.zeros_like(g_ref[...]))

    @pl.when(left > 0)
    def _():
        x_val = x_ref[...]
        width = w1_ref.shape[1] // 4
        for part in range(4):
            cols = slice(part * width, (part + 1) * width)
            h_val = dot(x_val, w1_ref[:, cols], ((1,), (0,))).astype(BF16).astype(F32)
            _, _, cdf = gelu_parts(h_val)
            a_scr[:, cols] = (h_val * cdf).astype(BF16)
        y_val = dot(a_scr[...], w2_ref[...], ((1,), (0,))).astype(BF16)
        x1_ref[...] = (x_val.astype(F32) + y_val.astype(F32)).astype(BF16)

    @pl.when(left <= 0)
    def _():
        x1_ref[...] = x_ref[...]


def forward(x0, g, lengths, w1, w2, micro, block):
    toks, dim = x0.shape
    ff = w1.shape[1]
    tiles = toks // micro // block
    tile_spec = pl.BlockSpec((block, dim), lambda i, n: (i, 0))
    return pl.pallas_call(
        functools.partial(fwd_kernel, tiles),
        out_shape=[jax.ShapeDtypeStruct((toks, dim), BF16)] * 2,
        grid_spec=pltpu.PrefetchScalarGridSpec(
            num_scalar_prefetch=1,
            grid=(toks // block,),
            in_specs=[
                tile_spec,
                tile_spec,
                pl.BlockSpec((dim, ff), lambda i, n: (0, 0)),
                pl.BlockSpec((ff, dim), lambda i, n: (0, 0)),
            ],
            out_specs=[tile_spec, tile_spec],
            scratch_shapes=[pltpu.VMEM((block, ff), BF16)],
        ),
        compiler_params=pltpu.CompilerParams(vmem_limit_bytes=58 * 1024 * 1024),
        name="fwd0",
    )(lengths, x0, g, w1, w2)


def grad_kernel(unit, block, x1_h, x0_h, r_h, wu_h, wd_h, gu_h, gd_h,
                xv, rv, dxa, w1v, w2v, own_u, own_v, in_u, in_v, sum_u, sum_v,
                rr_u, rr_v, rl_u, rl_v, out_u, out_v,
                x_sem, r_sem, w_sem, ds_sem, dr_sem, rs_sem, rq_sem, ls_sem, lq_sem,
                ou_sem, ov_sem, d_credit, r_credit, l_credit):
    toks, dim = xv.shape
    layers, _, ff = wu_h.shape
    tiles = toks // block
    wide = 2 * unit
    rows_u = dim // (2 * CHIPS)
    per_dev = ff // (2 * CHIPS)
    per_layer = ff // wide
    total = layers * per_layer

    me = lax.axis_index("fsdp")
    z = me // 2
    core = me % 2
    peer = z * 2 + (1 - core)

    barrier = pltpu.get_barrier_semaphore()
    pl.semaphore_signal(barrier, inc=1, device_id={"fsdp": peer}, device_id_type=MESH)

    @pl.when(z > 0)
    def _():
        pl.semaphore_signal(barrier, inc=1, device_id={"fsdp": me - 2}, device_id_type=MESH)

    @pl.when(z < CHIPS - 1)
    def _():
        pl.semaphore_signal(barrier, inc=1, device_id={"fsdp": me + 2}, device_id_type=MESH)

    def chip_of(m):
        return (1 + 3 * m) % CHIPS

    def cols_of(m):
        inner = m % per_layer
        base = 2 * per_dev * chip_of(inner) + unit * (inner // CHIPS)
        return pl.multiple_of(base, unit), pl.multiple_of(base + per_dev, unit)

    def w_copies(m):
        layer = layers - 1 - m // per_layer
        slot = m % 2
        lo, hi = cols_of(m)
        out = []
        for half, start in enumerate((lo, hi)):
            span = pl.ds(start, unit)
            here = pl.ds(half * unit, unit)
            out.append(pltpu.make_async_copy(
                wu_h.at[layer, :, span], w1v.at[slot, :, here], w_sem.at[slot, half]))
            out.append(pltpu.make_async_copy(
                wd_h.at[layer, span, :], w2v.at[slot, here, :], w_sem.at[slot, 2 + half]))
        return out

    def rows_of(i):
        return pl.ds(pl.multiple_of(i * block, block), block)

    def x_copy(src, i):
        return pltpu.make_async_copy(src.at[rows_of(i), :], xv.at[rows_of(i), :], x_sem.at[i])

    def r_copy(i):
        return pltpu.make_async_copy(r_h.at[rows_of(i), :], rv.at[rows_of(i), :], r_sem.at[i])

    for cp in w_copies(0):
        cp.start()
    for i in range(tiles):
        x_copy(x1_h, i).start()
        r_copy(i).start()

    def clear(i, carry):
        dxa[rows_of(i), :] = jnp.zeros((block, dim), F32)
        return carry

    lax.fori_loop(0, tiles, clear, 0)
    peers = 1 + jnp.where(z > 0, 1, 0) + jnp.where(z < CHIPS - 1, 1, 0)
    pl.semaphore_wait(barrier, peers)

    def compute(m, back):
        slot = m % 2
        own_u[slot] = jnp.zeros(own_u.shape[1:], F32)
        own_v[slot] = jnp.zeros(own_v.shape[1:], F32)
        w1c = w1v.at[slot]
        w2c = w2v.at[slot]

        def tile(i, carry):
            @pl.when(m % per_layer == 0)
            def _():
                x_copy(x1_h, i).wait()
                if back:
                    r_copy(i).wait()
                else:
                    rv[rows_of(i), :] = (rv[rows_of(i), :].astype(F32) + dxa[rows_of(i), :]).astype(BF16)

            x_i = xv[rows_of(i), :]
            r_i = rv[rows_of(i), :]
            h_val = dot(x_i, w1c[...], ((1,), (0,))).astype(BF16).astype(F32)
            da_val = dot(r_i, w2c[...], ((1,), (1,)))
            sq, th, cdf = gelu_parts(h_val)
            a_val = (h_val * cdf).astype(BF16)
            slope = cdf + (h_val * (0.5 - 0.5 * (th * th))) * (C1 + K3 * sq)
            dh_val = (da_val * slope).astype(BF16)
            own_v[slot] += dot(a_val, r_i, ((0,), (0,))).reshape(own_v.shape[1:])
            own_u[slot] += dot(x_i, dh_val, ((0,), (0,))).reshape(own_u.shape[1:])
            if back:
                dxa[rows_of(i), :] += dot(dh_val, w1c[...], ((1,), (1,)))
            return carry

        lax.fori_loop(0, tiles, tile, 0)

    def remote(src, dst, ssem, rsem, dev):
        return pltpu.make_async_remote_copy(
            src_ref=src, dst_ref=dst, send_sem=ssem, recv_sem=rsem,
            device_id={"fsdp": dev}, device_id_type=MESH)

    def d_copies(m):
        slot = m % 2
        return (
            remote(own_u.at[slot, :, 1 - core], in_u.at[slot], ds_sem.at[0, slot], dr_sem.at[0, slot], peer),
            remote(own_v.at[slot, 1 - core], in_v.at[slot], ds_sem.at[1, slot], dr_sem.at[1, slot], peer),
        )

    def line_copies(m, zz, going, first):
        slot = m % SLOTS
        if going > 0:
            blocks, dst_u, dst_v, ssem, qsem = pl.ds(zz + 1, CHIPS - 1 - zz), rr_u, rr_v, rs_sem, rq_sem
        else:
            blocks, dst_u, dst_v, ssem, qsem = pl.ds(0, zz), rl_u, rl_v, ls_sem, lq_sem
        src_u, src_v = (sum_u, sum_v) if first else (dst_u, dst_v)
        dev = me + 2 * going
        return (
            remote(src_u.at[slot, blocks], dst_u.at[slot, blocks], ssem.at[0, slot], qsem.at[0, slot], dev),
            remote(src_v.at[slot], dst_v.at[slot], ssem.at[1, slot], qsem.at[1, slot], dev),
        )

    def beyond(m, zz, going):
        return chip_of(m % per_layer) > zz if going > 0 else chip_of(m % per_layer) < zz

    def send_line(m, zz, going, first):
        credit = r_credit if going > 0 else l_credit

        @pl.when(m >= SLOTS)
        def _():
            pl.semaphore_wait(credit, 1)

        cu, cv = line_copies(m, zz, going, first)
        cu.start()

        @pl.when(beyond(m, zz, going))
        def _():
            cv.start()

    def wait_line(m, zz, going):
        cu, cv = line_copies(m, zz, going, False)
        cu.wait_recv()

        @pl.when(beyond(m, zz, going))
        def _():
            cv.wait_recv()

    def wait_sent(m, zz, going, first):
        cu, cv = line_copies(m, zz, going, first)
        cu.wait_send()

        @pl.when(beyond(m, zz, going))
        def _():
            cv.wait_send()

    def flow(m, zz, going):
        slot = m % SLOTS
        got_u, got_v = (rr_u, rr_v) if going > 0 else (rl_u, rl_v)
        first = zz == (0 if going > 0 else CHIPS - 1)
        last = zz == (CHIPS - 1 if going > 0 else 0)
        ahead = FWD_LAG + (zz if going > 0 else CHIPS - 1 - zz)
        other = FWD_LAG + (CHIPS - 1 - zz if going > 0 else zz)
        if not first:
            wait_line(m, zz - going, going)
            lo, hi = (zz, CHIPS) if going > 0 else (0, zz + 1)
            keep = ahead < other
            if not keep:
                lo, hi = (zz + 1, CHIPS) if going > 0 else (0, zz)
            if hi > lo:
                got_u[slot, lo:hi] += sum_u[slot, lo:hi]
            owner = chip_of(m % per_layer)
            if going > 0:
                mine = owner >= zz if keep else owner > zz
            else:
                mine = owner <= zz if keep else owner < zz

            @pl.when(mine)
            def _():
                got_v[slot] += sum_v[slot]

        if not last:
            send_line(m, zz, going, first)

    def out_copies_u(m):
        layer = layers - 1 - m // per_layer
        slot = m % 2
        lo, hi = cols_of(m)
        return [
            pltpu.make_async_copy(out_u.at[slot, :, pl.ds(half * unit, unit)],
                                  gu_h.at[layer, :, pl.ds(start, unit)], ou_sem.at[slot, half])
            for half, start in enumerate((lo, hi))
        ]

    def out_copy_v(m):
        layer = layers - 1 - m // per_layer
        start = pl.multiple_of(unit * ((m % per_layer) // CHIPS), unit)
        return pltpu.make_async_copy(out_v, gd_h.at[layer, pl.ds(start, unit), :], ov_sem)

    def finish(m, zz):
        slot = m % SLOTS

        @pl.when(m >= 2)
        def _():
            for cp in out_copies_u(m - 2):
                cp.wait()

        parts_u, parts_v = [], []
        if zz == 0 or zz == CHIPS - 1:
            parts_u.append(sum_u)
            parts_v.append(sum_v)
        if zz > 0:
            parts_u.append(rr_u)
            parts_v.append(rr_v)
        if zz < CHIPS - 1:
            parts_u.append(rl_u)
            parts_v.append(rl_v)
        out_u[m % 2] = parts_u[0][slot, zz] + parts_u[1][slot, zz]
        for cp in out_copies_u(m):
            cp.start()

        @pl.when(chip_of(m % per_layer) == zz)
        def _():
            @pl.when(m >= CHIPS)
            def _():
                out_copy_v(m - CHIPS).wait()

            out_v[...] = parts_v[0][slot] + parts_v[1][slot]
            out_copy_v(m).start()

        if zz < CHIPS - 1:
            wait_sent(m, zz, 1, zz == 0)
        if zz > 0:
            wait_sent(m, zz, -1, zz == CHIPS - 1)

        @pl.when(m < total - SLOTS)
        def _():
            if zz > 0:
                pl.semaphore_signal(r_credit, inc=1, device_id={"fsdp": me - 2}, device_id_type=MESH)
            if zz < CHIPS - 1:
                pl.semaphore_signal(l_credit, inc=1, device_id={"fsdp": me + 2}, device_id_type=MESH)

    def live(m):
        return jnp.logical_and(m >= 0, m < total)

    def iteration(t, carry):
        @pl.when(t < total)
        def _():
            @pl.when(t + 1 < total)
            def _():
                for cp in w_copies(t + 1):
                    cp.start()

            for cp in w_copies(t):
                cp.wait()

            @pl.when(t == per_layer)
            def _():
                for i in range(tiles):
                    x_copy(x0_h, i).start()

            @pl.when(t < per_layer)
            def _():
                compute(t, True)

            @pl.when(t >= per_layer)
            def _():
                compute(t, False)

            @pl.when(t >= 2)
            def _():
                pl.semaphore_wait(d_credit, 1)

            for cp in d_copies(t):
                cp.start()

        m_chip = t - FWD_LAG

        @pl.when(live(m_chip))
        def _():
            slot2 = m_chip % 2
            slot = m_chip % SLOTS
            for cp in d_copies(m_chip):
                cp.wait_recv()
            sum_u[slot] = own_u[slot2, :, core] + in_u[slot2]
            sum_v[slot] = own_v[slot2, core] + in_v[slot2]
            for cp in d_copies(m_chip):
                cp.wait_send()

            @pl.when(m_chip < total - 2)
            def _():
                pl.semaphore_signal(d_credit, inc=1, device_id={"fsdp": peer}, device_id_type=MESH)

        for zz in range(CHIPS):
            @pl.when(z == zz)
            def _():
                lags = sorted([(FWD_LAG + zz, 1), (FWD_LAG + CHIPS - 1 - zz, -1)])
                for lag, going in lags:
                    m = t - lag

                    @pl.when(live(m))
                    def _():
                        flow(m, zz, going)

                m_end = t - END_LAG

                @pl.when(live(m_end))
                def _():
                    finish(m_end, zz)

        return carry

    lax.fori_loop(0, total + END_LAG, iteration, 0)

    for m in (total - 2, total - 1):
        for cp in out_copies_u(m):
            cp.wait()
    out_copy_v(total - CHIPS).wait()


def gradients(x1, x0, r, w_up, w_down, block, unit):
    toks, dim = x0.shape
    layers, _, ff = w_up.shape
    rows_u = dim // (2 * CHIPS)
    wide = 2 * unit
    tiles = toks // block
    dma = pltpu.SemaphoreType.DMA
    vm = pltpu.VMEM
    u_blk = (CHIPS, rows_u, wide)
    v_blk = (unit, dim)
    scratch = [
        vm((toks, dim), BF16), vm((toks, dim), BF16), vm((toks, dim), F32),
        vm((2, dim, wide), BF16), vm((2, wide, dim), BF16),
        vm((2, CHIPS, 2, rows_u, wide), F32), vm((2, 2) + v_blk, F32),
        vm((2,) + u_blk, F32), vm((2,) + v_blk, F32),
        vm((SLOTS,) + u_blk, F32), vm((SLOTS,) + v_blk, F32),
        vm((SLOTS,) + u_blk, F32), vm((SLOTS,) + v_blk, F32),
        vm((SLOTS,) + u_blk, F32), vm((SLOTS,) + v_blk, F32),
        vm((2, rows_u, wide), F32), vm(v_blk, F32),
        dma((tiles,)), dma((tiles,)), dma((2, 4)),
        dma((2, 2)), dma((2, 2)),
        dma((2, SLOTS)), dma((2, SLOTS)), dma((2, SLOTS)), dma((2, SLOTS)),
        dma((2, 2)), dma,
        pltpu.SemaphoreType.REGULAR, pltpu.SemaphoreType.REGULAR, pltpu.SemaphoreType.REGULAR,
    ]
    return pl.pallas_call(
        functools.partial(grad_kernel, unit, block),
        out_shape=[
            jax.ShapeDtypeStruct((layers, rows_u, ff), F32),
            jax.ShapeDtypeStruct((layers, ff // (2 * CHIPS), dim), F32),
        ],
        in_specs=[ANY] * 5,
        out_specs=[ANY] * 2,
        scratch_shapes=scratch,
        compiler_params=pltpu.CompilerParams(
            collective_id=0, has_side_effects=True, vmem_limit_bytes=62 * 1024 * 1024),
        name="grads",
    )(x1, x0, r, w_up, w_down)


def solution(mesh, block=512, unit=128):
    def local_step(acts_in, cot_out, lengths, w_up, w_down):
        micro, tok_rows, dim = acts_in.shape
        x0 = acts_in.reshape(micro * tok_rows, dim)
        g = cot_out.reshape(micro * tok_rows, dim)
        x1, r = forward(x0, g, lengths.reshape(micro), w_up[0], w_down[0], micro, block)
        return gradients(x1, x0, r, w_up, w_down, block, unit)

    act_spec = P(None, ("part", "fsdp"), None)
    grad_spec = P("part", "fsdp", None)
    return jax.shard_map(
        local_step, mesh=mesh,
        in_specs=(act_spec, act_spec, P(None, ("part", "fsdp")), P(), P()),
        out_specs=(grad_spec, grad_spec), check_vma=False)
```

```python
import functools

import jax
import jax.numpy as jnp
from jax import lax
from jax.experimental import pallas as pl
from jax.experimental.pallas import tpu as pltpu
from jax.sharding import PartitionSpec as P

MESH = pl.DeviceIdType.MESH
ANY = pl.BlockSpec(memory_space=pl.ANY)
F32 = jnp.float32
BF16 = jnp.bfloat16

C1 = 0.7978845608028654
K1 = C1 * 0.044715
K3 = 3.0 * K1

CHIPS = 4
SLOTS = 4
PIECES = 4


def dot(lhs, rhs, dims):
    return lax.dot_general(lhs, rhs, (dims, ((), ())), preferred_element_type=F32)


def gelu_parts(h_wide):
    sq = h_wide * h_wide
    th = jnp.tanh(h_wide * (C1 + K1 * sq))
    cdf = 0.5 + 0.5 * th
    return sq, th, cdf


def fwd_kernel(tiles, len_ref, x_ref, g_ref, w1_ref, w2_ref, x1_ref, r_ref, a_scr):
    step = pl.program_id(0)
    rows = x_ref.shape[0]
    left = len_ref[step // tiles] - (step % tiles) * rows
    row_ids = lax.broadcasted_iota(jnp.int32, r_ref.shape, 0)
    r_ref[...] = jnp.where(row_ids < left, g_ref[...], jnp.zeros_like(g_ref[...]))

    @pl.when(left > 0)
    def _():
        x_val = x_ref[...]
        width = w1_ref.shape[1] // 4
        for part in range(4):
            cols = slice(part * width, (part + 1) * width)
            h_val = dot(x_val, w1_ref[:, cols], ((1,), (0,))).astype(BF16).astype(F32)
            _, _, cdf = gelu_parts(h_val)
            a_scr[:, cols] = (h_val * cdf).astype(BF16)
        y_val = dot(a_scr[...], w2_ref[...], ((1,), (0,))).astype(BF16)
        x1_ref[...] = (x_val.astype(F32) + y_val.astype(F32)).astype(BF16)

    @pl.when(left <= 0)
    def _():
        x1_ref[...] = x_ref[...]


def forward(x0, g, lengths, w1, w2, micro, block):
    toks, dim = x0.shape
    ff = w1.shape[2]
    tiles = toks // micro // block
    tile_spec = pl.BlockSpec((block, dim), lambda i, n: (i, 0))
    return pl.pallas_call(
        functools.partial(fwd_kernel, tiles),
        out_shape=[jax.ShapeDtypeStruct((toks, dim), BF16)] * 2,
        grid_spec=pltpu.PrefetchScalarGridSpec(
            num_scalar_prefetch=1,
            grid=(toks // block,),
            in_specs=[
                tile_spec,
                tile_spec,
                pl.BlockSpec((None, dim, ff), lambda i, n: (0, 0, 0)),
                pl.BlockSpec((None, ff, dim), lambda i, n: (0, 0, 0)),
            ],
            out_specs=[tile_spec, tile_spec],
            scratch_shapes=[pltpu.VMEM((block, ff), BF16)],
        ),
        compiler_params=pltpu.CompilerParams(vmem_limit_bytes=58 * 1024 * 1024),
        name="fwd0",
    )(lengths, x0, g, w1, w2)


def grad_kernel(unit, block, x1_h, x0_h, r_h, wu_h, wd_h, gu_h, gd_h,
                xv, rv, dxa, slope_v, w1v, w2v, own_u, own_v, in_u, in_v, sum_u, sum_v,
                rr_u, rr_v, rl_u, rl_v, out_u, out_v,
                x_sem, r_sem, w_sem, ds_sem, dr_sem,
                rs_u, rq_u, ls_u, lq_u, rs_v, rq_v, ls_v, lq_v,
                ou_sem, ov_sem, du_credit, dv_credit, ru_credit, lu_credit, rv_credit, lv_credit):
    toks, dim = xv.shape
    layers, _, ff = wu_h.shape
    tiles = toks // block
    wide = 2 * unit
    per_dev = ff // (2 * CHIPS)
    per_layer = ff // wide
    total = layers * per_layer
    piece = unit // PIECES

    me = lax.axis_index("fsdp")
    z = me // 2
    core = me % 2
    peer = z * 2 + (1 - core)

    def signal(sem, dev):
        pl.semaphore_signal(sem, inc=1, device_id={"fsdp": dev}, device_id_type=MESH)

    barrier = pltpu.get_barrier_semaphore()
    signal(barrier, peer)

    @pl.when(z > 0)
    def _():
        signal(barrier, me - 2)

    @pl.when(z < CHIPS - 1)
    def _():
        signal(barrier, me + 2)

    def layer_of(m):
        return layers - 1 - m // per_layer

    def owner_of(m):
        return (1 + 3 * (m % per_layer)) % CHIPS

    def cols_of(m):
        base = 2 * per_dev * owner_of(m) + unit * ((m % per_layer) // CHIPS)
        return pl.multiple_of(base, unit), pl.multiple_of(base + per_dev, unit)

    def w_copies(m):
        slot = m % 2
        out = []
        for half, start in enumerate(cols_of(m)):
            span = pl.ds(start, unit)
            here = pl.ds(half * unit, unit)
            out.append(pltpu.make_async_copy(
                wu_h.at[layer_of(m), :, span], w1v.at[slot, :, here], w_sem.at[slot, half]))
            out.append(pltpu.make_async_copy(
                wd_h.at[layer_of(m), span, :], w2v.at[slot, here, :], w_sem.at[slot, 2 + half]))
        return out

    def rows_of(i):
        return pl.ds(pl.multiple_of(i * block, block), block)

    def x_copy(src, i):
        return pltpu.make_async_copy(src.at[rows_of(i), :], xv.at[rows_of(i), :], x_sem.at[i])

    def r_copy(i):
        return pltpu.make_async_copy(r_h.at[rows_of(i), :], rv.at[rows_of(i), :], r_sem.at[i])

    for cp in w_copies(0):
        cp.start()
    for i in range(tiles):
        x_copy(x1_h, i).start()
        r_copy(i).start()

    def clear(i, carry):
        dxa[rows_of(i), :] = jnp.zeros((block, dim), F32)
        return carry

    lax.fori_loop(0, tiles, clear, 0)
    peers = 1 + jnp.where(z > 0, 1, 0) + jnp.where(z < CHIPS - 1, 1, 0)
    pl.semaphore_wait(barrier, peers)

    def compute_v(m, back):
        own_v[...] = jnp.zeros(own_v.shape, F32)
        w1c = w1v.at[m % 2]

        def tile(i, carry):
            @pl.when(m % per_layer == 0)
            def _():
                x_copy(x1_h, i).wait()
                if back:
                    r_copy(i).wait()
                else:
                    rv[rows_of(i), :] = (rv[rows_of(i), :].astype(F32) + dxa[rows_of(i), :]).astype(BF16)

            h_val = dot(xv[rows_of(i), :], w1c[...], ((1,), (0,))).astype(BF16).astype(F32)
            sq, th, cdf = gelu_parts(h_val)
            a_val = (h_val * cdf).astype(BF16)
            slope_v[rows_of(i), :] = cdf + (h_val * (0.5 - 0.5 * (th * th))) * (C1 + K3 * sq)
            own_v[...] += dot(a_val, rv[rows_of(i), :], ((0,), (0,))).reshape(own_v.shape)
            return carry

        lax.fori_loop(0, tiles, tile, 0)

    def compute_u(m, back):
        own_u[...] = jnp.zeros(own_u.shape, F32)
        w1c = w1v.at[m % 2]
        w2c = w2v.at[m % 2]

        def tile(i, carry):
            da_val = dot(rv[rows_of(i), :], w2c[...], ((1,), (1,)))
            dh_val = (da_val * slope_v[rows_of(i), :]).astype(BF16)
            own_u[...] += dot(xv[rows_of(i), :], dh_val, ((0,), (0,))).reshape(own_u.shape)
            if back:
                dxa[rows_of(i), :] += dot(dh_val, w1c[...], ((1,), (1,)))
            return carry

        lax.fori_loop(0, tiles, tile, 0)

    def remote(src, dst, ssem, rsem, dev):
        return pltpu.make_async_remote_copy(
            src_ref=src, dst_ref=dst, send_sem=ssem, recv_sem=rsem,
            device_id={"fsdp": dev}, device_id_type=MESH)

    d_u = remote(own_u.at[:, 1 - core], in_u, ds_sem.at[0], dr_sem.at[0], peer)
    d_v = remote(own_v.at[1 - core], in_v, ds_sem.at[1], dr_sem.at[1], peer)

    def far_first(zz, going):
        return list(range(CHIPS - 1, zz, -1)) if going > 0 else list(range(zz))

    def u_copy(m, b, going, first):
        slot = m % SLOTS
        dst, ssem, qsem = (rr_u, rs_u, rq_u) if going > 0 else (rl_u, ls_u, lq_u)
        src = sum_u if first else dst
        return remote(src.at[slot, b], dst.at[slot, b], ssem.at[b, slot], qsem.at[b, slot], me + 2 * going)

    def v_copy(m, p, going, first):
        slot = m % SLOTS
        dst, ssem, qsem = (rr_v, rs_v, rq_v) if going > 0 else (rl_v, ls_v, lq_v)
        src = sum_v if first else dst
        part = pl.ds(p * piece, piece)
        return remote(src.at[slot, part], dst.at[slot, part], ssem.at[p, slot], qsem.at[p, slot], me + 2 * going)

    def beyond(m, zz, going):
        return owner_of(m) > zz if going > 0 else owner_of(m) < zz

    def ends(zz, going):
        start, stop = (0, CHIPS - 1) if going > 0 else (CHIPS - 1, 0)
        return zz == start, zz == stop

    def keeps(zz, going):
        dist = zz if going > 0 else CHIPS - 1 - zz
        return 2 * dist < CHIPS - 1

    def flow_u(m, zz, going):
        slot = m % SLOTS
        got, credit = (rr_u, ru_credit) if going > 0 else (rl_u, lu_credit)
        first, last = ends(zz, going)
        if not last:
            @pl.when(m >= SLOTS)
            def _():
                pl.semaphore_wait(credit, 1)

        for b in far_first(zz, going):
            if not first:
                u_copy(m, b, going, False).wait_recv()
                got[slot, b] += sum_u[slot, b]
            u_copy(m, b, going, first).start()
        if not first:
            u_copy(m, zz, going, False).wait_recv()
            if keeps(zz, going):
                got[slot, zz] += sum_u[slot, zz]

    def flow_v(m, zz, going):
        slot = m % SLOTS
        got, credit = (rr_v, rv_credit) if going > 0 else (rl_v, lv_credit)
        first, last = ends(zz, going)
        if not last:
            @pl.when(beyond(m, zz, going))
            def _():
                @pl.when(m >= SLOTS)
                def _():
                    pl.semaphore_wait(credit, 1)

                for p in range(PIECES):
                    if not first:
                        v_copy(m, p, going, False).wait_recv()
                        part = pl.ds(p * piece, piece)
                        got[slot, part] += sum_v[slot, part]
                    v_copy(m, p, going, first).start()

        if not first:
            @pl.when(owner_of(m) == zz)
            def _():
                for p in range(PIECES):
                    v_copy(m, p, going, False).wait_recv()
                if keeps(zz, going):
                    got[slot] += sum_v[slot]

    def out_copies_u(m):
        slot = m % 2
        return [
            pltpu.make_async_copy(out_u.at[slot, :, pl.ds(half * unit, unit)],
                                  gu_h.at[layer_of(m), :, pl.ds(start, unit)], ou_sem.at[slot, half])
            for half, start in enumerate(cols_of(m))
        ]

    def out_copy_v(m):
        start = pl.multiple_of(unit * ((m % per_layer) // CHIPS), unit)
        return pltpu.make_async_copy(out_v, gd_h.at[layer_of(m), pl.ds(start, unit), :], ov_sem)

    def terms(zz, total_ref, right_ref, left_ref):
        if zz == 0:
            return total_ref, left_ref
        if zz == CHIPS - 1:
            return total_ref, right_ref
        return right_ref, left_ref

    def finish_u(m, zz):
        slot = m % SLOTS

        @pl.when(m >= 2)
        def _():
            for cp in out_copies_u(m - 2):
                cp.wait()

        one, two = terms(zz, sum_u, rr_u, rl_u)
        out_u[m % 2] = one[slot, zz] + two[slot, zz]
        for cp in out_copies_u(m):
            cp.start()
        for going in (1, -1):
            for b in far_first(zz, going):
                u_copy(m, b, going, ends(zz, going)[0]).wait_send()

        @pl.when(m < total - SLOTS)
        def _():
            if zz > 0:
                signal(ru_credit, me - 2)
            if zz < CHIPS - 1:
                signal(lu_credit, me + 2)

    def finish_v(m, zz):
        slot = m % SLOTS

        @pl.when(owner_of(m) == zz)
        def _():
            @pl.when(m >= CHIPS)
            def _():
                out_copy_v(m - CHIPS).wait()

            one, two = terms(zz, sum_v, rr_v, rl_v)
            out_v[...] = one[slot] + two[slot]
            out_copy_v(m).start()

        for going in (1, -1):
            first, last = ends(zz, going)
            if not last:
                @pl.when(beyond(m, zz, going))
                def _():
                    for p in range(PIECES):
                        v_copy(m, p, going, first).wait_send()

            if not first:
                credit = rv_credit if going > 0 else lv_credit

                @pl.when(jnp.logical_and(beyond(m, zz - going, going), m < total - SLOTS))
                def _():
                    signal(credit, me - 2 * going)

    def live(m):
        return jnp.logical_and(m >= 0, m < total)

    def sums(t, lag, pair, mine, got, into, credit, flow, finish):
        m_core = t - lag

        @pl.when(live(m_core))
        def _():
            pair.wait_recv()
            into[m_core % SLOTS] = mine() + got[...]
            pair.wait_send()

            @pl.when(m_core < total - 1)
            def _():
                signal(credit, peer)

        for zz in range(CHIPS):
            @pl.when(z == zz)
            def _():
                for ahead, going in sorted([(zz, 1), (CHIPS - 1 - zz, -1)]):
                    m = t - lag - ahead

                    @pl.when(live(m))
                    def _():
                        flow(m, zz, going)

                m_end = t - lag - (CHIPS - 1)

                @pl.when(live(m_end))
                def _():
                    finish(m_end, zz)

    def send_pair(t, pair, credit):
        @pl.when(t > 0)
        def _():
            pl.semaphore_wait(credit, 1)

        pair.start()

    def iteration(t, carry):
        back = t < per_layer
        front = jnp.logical_and(t >= per_layer, t < total)

        @pl.when(t < total)
        def _():
            @pl.when(t + 1 < total)
            def _():
                for cp in w_copies(t + 1):
                    cp.start()

            for cp in w_copies(t):
                cp.wait()

            @pl.when(t == per_layer)
            def _():
                for i in range(tiles):
                    x_copy(x0_h, i).start()

        @pl.when(back)
        def _():
            compute_v(t, True)

        @pl.when(front)
        def _():
            compute_v(t, False)

        @pl.when(t < total)
        def _():
            send_pair(t, d_v, dv_credit)

        sums(t, 1, d_u, lambda: own_u[:, core], in_u, sum_u, du_credit, flow_u, finish_u)

        @pl.when(back)
        def _():
            compute_u(t, True)

        @pl.when(front)
        def _():
            compute_u(t, False)

        @pl.when(t < total)
        def _():
            send_pair(t, d_u, du_credit)

        sums(t, 0, d_v, lambda: own_v[core], in_v, sum_v, dv_credit, flow_v, finish_v)
        return carry

    lax.fori_loop(0, total + CHIPS, iteration, 0)

    for m in (total - 2, total - 1):
        for cp in out_copies_u(m):
            cp.wait()
    out_copy_v(total - CHIPS).wait()


def gradients(x1, x0, r, w_up, w_down, block, unit):
    toks, dim = x0.shape
    layers, _, ff = w_up.shape
    rows_u = dim // (2 * CHIPS)
    wide = 2 * unit
    tiles = toks // block
    dma = pltpu.SemaphoreType.DMA
    vm = pltpu.VMEM
    u_blk = (CHIPS, rows_u, wide)
    v_blk = (unit, dim)
    line_sems = [dma((CHIPS, SLOTS))] * 4 + [dma((PIECES, SLOTS))] * 4
    scratch = [
        vm((toks, dim), BF16), vm((toks, dim), BF16), vm((toks, dim), F32), vm((toks, wide), F32),
        vm((2, dim, wide), BF16), vm((2, wide, dim), BF16),
        vm((CHIPS, 2, rows_u, wide), F32), vm((2,) + v_blk, F32),
        vm(u_blk, F32), vm(v_blk, F32),
        vm((SLOTS,) + u_blk, F32), vm((SLOTS,) + v_blk, F32),
        vm((SLOTS,) + u_blk, F32), vm((SLOTS,) + v_blk, F32),
        vm((SLOTS,) + u_blk, F32), vm((SLOTS,) + v_blk, F32),
        vm((2, rows_u, wide), F32), vm(v_blk, F32),
        dma((tiles,)), dma((tiles,)), dma((2, 4)), dma((2,)), dma((2,)),
        *line_sems,
        dma((2, 2)), dma,
    ] + [pltpu.SemaphoreType.REGULAR] * 6
    return pl.pallas_call(
        functools.partial(grad_kernel, unit, block),
        out_shape=[
            jax.ShapeDtypeStruct((layers, rows_u, ff), F32),
            jax.ShapeDtypeStruct((layers, ff // (2 * CHIPS), dim), F32),
        ],
        in_specs=[ANY] * 5,
        out_specs=[ANY] * 2,
        scratch_shapes=scratch,
        compiler_params=pltpu.CompilerParams(
            collective_id=0, has_side_effects=True, vmem_limit_bytes=62 * 1024 * 1024),
        name="grads",
    )(x1, x0, r, w_up, w_down)


def solution(mesh, block=512, unit=128):
    def local_step(acts_in, cot_out, lengths, w_up, w_down):
        micro, tok_rows, dim = acts_in.shape
        x0 = acts_in.reshape(micro * tok_rows, dim)
        g = cot_out.reshape(micro * tok_rows, dim)
        x1, r = forward(x0, g, lengths.reshape(micro), w_up, w_down, micro, block)
        return gradients(x1, x0, r, w_up, w_down, block, unit)

    act_spec = P(None, ("part", "fsdp"), None)
    grad_spec = P("part", "fsdp", None)
    return jax.shard_map(
        local_step, mesh=mesh,
        in_specs=(act_spec, act_spec, P(None, ("part", "fsdp")), P(), P()),
        out_specs=(grad_spec, grad_spec), check_vma=False)
```

```python
import functools

import jax
import jax.numpy as jnp
from jax import lax
from jax.experimental import pallas as pl
from jax.experimental.pallas import tpu as pltpu
from jax.sharding import PartitionSpec as P

MESH = pl.DeviceIdType.MESH
ANY = pl.BlockSpec(memory_space=pl.ANY)
F32 = jnp.float32
BF16 = jnp.bfloat16

C1 = 0.7978845608028654
K1 = C1 * 0.044715
K3 = 3.0 * K1

CHIPS = 4
SLOTS = 4
WSLOTS = 3


def dot(lhs, rhs, dims):
    return lax.dot_general(lhs, rhs, (dims, ((), ())), preferred_element_type=F32)


def gelu_parts(h_wide):
    sq = h_wide * h_wide
    th = jnp.tanh(h_wide * (C1 + K1 * sq))
    cdf = 0.5 + 0.5 * th
    return sq, th, cdf


def gelu_pair(h_wide):
    sq, th, cdf = gelu_parts(h_wide)
    slope = cdf + (h_wide * (0.5 - 0.5 * (th * th))) * (C1 + K3 * sq)
    return (h_wide * cdf).astype(BF16), slope


def fwd_kernel(tiles, len_ref, x_ref, g_ref, w1_ref, w2_ref, x1_ref, r_ref, a_scr):
    step = pl.program_id(0)
    rows = x_ref.shape[0]
    left = len_ref[step // tiles] - (step % tiles) * rows
    row_ids = lax.broadcasted_iota(jnp.int32, r_ref.shape, 0)
    r_ref[...] = jnp.where(row_ids < left, g_ref[...], jnp.zeros_like(g_ref[...]))

    @pl.when(left > 0)
    def _():
        x_val = x_ref[...]
        width = w1_ref.shape[1] // 4
        for part in range(4):
            cols = slice(part * width, (part + 1) * width)
            h_val = dot(x_val, w1_ref[:, cols], ((1,), (0,))).astype(BF16).astype(F32)
            _, _, cdf = gelu_parts(h_val)
            a_scr[:, cols] = (h_val * cdf).astype(BF16)
        y_val = dot(a_scr[...], w2_ref[...], ((1,), (0,))).astype(BF16)
        x1_ref[...] = (x_val.astype(F32) + y_val.astype(F32)).astype(BF16)

    @pl.when(left <= 0)
    def _():
        x1_ref[...] = x_ref[...]


def forward(x0, g, lengths, w1, w2, micro, block):
    toks, dim = x0.shape
    ff = w1.shape[2]
    tiles = toks // micro // block
    tile_spec = pl.BlockSpec((block, dim), lambda i, n: (i, 0))
    return pl.pallas_call(
        functools.partial(fwd_kernel, tiles),
        out_shape=[jax.ShapeDtypeStruct((toks, dim), BF16)] * 2,
        grid_spec=pltpu.PrefetchScalarGridSpec(
            num_scalar_prefetch=1,
            grid=(toks // block,),
            in_specs=[
                tile_spec,
                tile_spec,
                pl.BlockSpec((None, dim, ff), lambda i, n: (0, 0, 0)),
                pl.BlockSpec((None, ff, dim), lambda i, n: (0, 0, 0)),
            ],
            out_specs=[tile_spec, tile_spec],
            scratch_shapes=[pltpu.VMEM((block, ff), BF16)],
        ),
        compiler_params=pltpu.CompilerParams(vmem_limit_bytes=58 * 1024 * 1024),
        name="fwd0",
    )(lengths, x0, g, w1, w2)


def grad_kernel(unit, block, x1_h, x0_h, r_h, wu_h, wd_h, gu_h, gd_h,
                xv, rv, dxa, slope_v, w1v, w2v, own_u, own_v, in_u, in_v, sum_u, sum_v,
                rr_u, rr_v, rl_u, rl_v, out_u, out_v,
                x_sem, r_sem, w_sem, ds_sem, dr_sem,
                rs_u, rq_u, ls_u, lq_u, rs_v, rq_v, ls_v, lq_v,
                ou_sem, ov_sem, du_credit, dv_credit, ru_credit, lu_credit, rv_credit, lv_credit):
    toks, dim = xv.shape
    layers, _, ff = wu_h.shape
    tiles = toks // block
    wide = 2 * unit
    per_dev = ff // (2 * CHIPS)
    per_layer = ff // wide
    total = layers * per_layer
    switch = per_layer + 2
    last_step = total + 2

    me = lax.axis_index("fsdp")
    z = me // 2
    core = me % 2
    peer = z * 2 + (1 - core)

    def signal(sem, dev):
        pl.semaphore_signal(sem, inc=1, device_id={"fsdp": dev}, device_id_type=MESH)

    barrier = pltpu.get_barrier_semaphore()
    signal(barrier, peer)

    @pl.when(z > 0)
    def _():
        signal(barrier, me - 2)

    @pl.when(z < CHIPS - 1)
    def _():
        signal(barrier, me + 2)

    def layer_of(m):
        return layers - 1 - m // per_layer

    def owner_of(m):
        return (1 + 3 * (m % per_layer)) % CHIPS

    def cols_of(m):
        base = 2 * per_dev * owner_of(m) + unit * ((m % per_layer) // CHIPS)
        return pl.multiple_of(base, unit), pl.multiple_of(base + per_dev, unit)

    def w_copies(m):
        slot = m % WSLOTS
        out = []
        for half, start in enumerate(cols_of(m)):
            span = pl.ds(start, unit)
            here = pl.ds(half * unit, unit)
            out.append(pltpu.make_async_copy(
                wu_h.at[layer_of(m), :, span], w1v.at[slot, :, here], w_sem.at[slot, half]))
            out.append(pltpu.make_async_copy(
                wd_h.at[layer_of(m), span, :], w2v.at[slot, here, :], w_sem.at[slot, 2 + half]))
        return out

    def rows_of(i):
        return pl.ds(pl.multiple_of(i * block, block), block)

    def x_copy(src, i):
        return pltpu.make_async_copy(src.at[rows_of(i), :], xv.at[rows_of(i), :], x_sem.at[i])

    def r_copy(i):
        return pltpu.make_async_copy(r_h.at[rows_of(i), :], rv.at[rows_of(i), :], r_sem.at[i])

    for cp in w_copies(0):
        cp.start()
    for i in range(tiles):
        x_copy(x1_h, i).start()
        r_copy(i).start()

    def clear(i, carry):
        dxa[rows_of(i), :] = jnp.zeros((block, dim), F32)
        return carry

    lax.fori_loop(0, tiles, clear, 0)
    peers = 1 + jnp.where(z > 0, 1, 0) + jnp.where(z < CHIPS - 1, 1, 0)
    pl.semaphore_wait(barrier, peers)

    def v_tile(m, i):
        h_val = dot(xv[rows_of(i), :], w1v[m % WSLOTS], ((1,), (0,))).astype(BF16).astype(F32)
        a_val, slope_v[rows_of(i), :] = gelu_pair(h_val)
        own_v[m % 2] += dot(a_val, rv[rows_of(i), :], ((0,), (0,))).reshape(own_v.shape[1:])

    def u_tile(m, i, back):
        da_val = dot(rv[rows_of(i), :], w2v[m % WSLOTS], ((1,), (1,)))
        dh_val = (da_val * slope_v[rows_of(i), :]).astype(BF16)
        own_u[m % 2] += dot(xv[rows_of(i), :], dh_val, ((0,), (0,))).reshape(own_u.shape[1:])
        if back:
            dxa[rows_of(i), :] += dot(dh_val, w1v[m % WSLOTS], ((1,), (1,)))

    def both_tile(mv, mu, i, back):
        rows = rows_of(i)
        x_i, r_i = xv[rows, :], rv[rows, :]
        da_val = dot(r_i, w2v[mu % WSLOTS], ((1,), (1,)))
        dh_val = (da_val * slope_v[rows, :]).astype(BF16)
        h_val = dot(x_i, w1v[mv % WSLOTS], ((1,), (0,))).astype(BF16).astype(F32)
        if back:
            dxa[rows, :] += dot(dh_val, w1v[mu % WSLOTS], ((1,), (1,)))
        a_val, slope_v[rows, :] = gelu_pair(h_val)
        own_u[mu % 2] += dot(x_i, dh_val, ((0,), (0,))).reshape(own_u.shape[1:])
        own_v[mv % 2] += dot(a_val, r_i, ((0,), (0,))).reshape(own_v.shape[1:])

    def arrive(n, i):
        @pl.when(n == 0)
        def _():
            x_copy(x1_h, i).wait()
            r_copy(i).wait()

        @pl.when(n == switch)
        def _():
            x_copy(x0_h, i).wait()
            rv[rows_of(i), :] = (rv[rows_of(i), :].astype(F32) + dxa[rows_of(i), :]).astype(BF16)

    def remote(src, dst, ssem, rsem, dev):
        return pltpu.make_async_remote_copy(
            src_ref=src, dst_ref=dst, send_sem=ssem, recv_sem=rsem,
            device_id={"fsdp": dev}, device_id_type=MESH)

    def d_u(m):
        slot = m % 2
        return remote(own_u.at[slot, :, 1 - core], in_u.at[slot], ds_sem.at[0, slot], dr_sem.at[0, slot], peer)

    def d_v(m):
        slot = m % 2
        return remote(own_v.at[slot, 1 - core], in_v.at[slot], ds_sem.at[1, slot], dr_sem.at[1, slot], peer)

    def u_copy(m, zz, going, first):
        slot = m % SLOTS
        dst, ssem, qsem = (rr_u, rs_u, rq_u) if going > 0 else (rl_u, ls_u, lq_u)
        src = sum_u if first else dst
        part = pl.ds(zz + 1, CHIPS - 1 - zz) if going > 0 else pl.ds(0, zz)
        return remote(src.at[slot, part], dst.at[slot, part], ssem.at[slot], qsem.at[slot], me + 2 * going)

    def v_copy(m, going, first):
        slot = m % SLOTS
        dst, ssem, qsem = (rr_v, rs_v, rq_v) if going > 0 else (rl_v, ls_v, lq_v)
        src = sum_v if first else dst
        return remote(src.at[slot], dst.at[slot], ssem.at[slot], qsem.at[slot], me + 2 * going)

    def beyond(m, zz, going):
        return owner_of(m) > zz if going > 0 else owner_of(m) < zz

    def ends(zz, going):
        start, stop = (0, CHIPS - 1) if going > 0 else (CHIPS - 1, 0)
        return zz == start, zz == stop

    def keeps(zz, going):
        dist = zz if going > 0 else CHIPS - 1 - zz
        return 2 * dist < CHIPS - 1

    def flow_u(m, zz, going):
        slot = m % SLOTS
        got, credit = (rr_u, ru_credit) if going > 0 else (rl_u, lu_credit)
        first, last = ends(zz, going)
        if not first:
            u_copy(m, zz - going, going, False).wait_recv()
            near = zz if keeps(zz, going) else zz + going
            lo, hi = (near, CHIPS) if going > 0 else (0, near + 1)
            if hi > lo:
                got[slot, lo:hi] += sum_u[slot, lo:hi]
        if not last:
            @pl.when(m >= SLOTS)
            def _():
                pl.semaphore_wait(credit, 1)

            u_copy(m, zz, going, first).start()

    def flow_v(m, zz, going):
        slot = m % SLOTS
        got, credit = (rr_v, rv_credit) if going > 0 else (rl_v, lv_credit)
        first, last = ends(zz, going)
        if not first:
            @pl.when(beyond(m, zz - going, going))
            def _():
                v_copy(m, going, False).wait_recv()

            @pl.when(beyond(m, zz - going if keeps(zz, going) else zz, going))
            def _():
                got[slot] += sum_v[slot]

        if not last:
            @pl.when(beyond(m, zz, going))
            def _():
                @pl.when(m >= SLOTS)
                def _():
                    pl.semaphore_wait(credit, 1)

                v_copy(m, going, first).start()

    def out_copies_u(m):
        slot = m % 2
        return [
            pltpu.make_async_copy(out_u.at[slot, :, pl.ds(half * unit, unit)],
                                  gu_h.at[layer_of(m), :, pl.ds(start, unit)], ou_sem.at[slot, half])
            for half, start in enumerate(cols_of(m))
        ]

    def out_copy_v(m):
        start = pl.multiple_of(unit * ((m % per_layer) // CHIPS), unit)
        return pltpu.make_async_copy(out_v, gd_h.at[layer_of(m), pl.ds(start, unit), :], ov_sem)

    def terms(zz, total_ref, right_ref, left_ref):
        if zz == 0:
            return total_ref, left_ref
        if zz == CHIPS - 1:
            return total_ref, right_ref
        return right_ref, left_ref

    def finish_u(m, zz):
        slot = m % SLOTS

        @pl.when(m >= 2)
        def _():
            for cp in out_copies_u(m - 2):
                cp.wait()

        one, two = terms(zz, sum_u, rr_u, rl_u)
        out_u[m % 2] = one[slot, zz] + two[slot, zz]
        for cp in out_copies_u(m):
            cp.start()
        for going in (1, -1):
            first, last = ends(zz, going)
            if not last:
                u_copy(m, zz, going, first).wait_send()

        @pl.when(m < total - SLOTS)
        def _():
            if zz > 0:
                signal(ru_credit, me - 2)
            if zz < CHIPS - 1:
                signal(lu_credit, me + 2)

    def finish_v(m, zz):
        slot = m % SLOTS

        @pl.when(owner_of(m) == zz)
        def _():
            @pl.when(m >= CHIPS)
            def _():
                out_copy_v(m - CHIPS).wait()

            one, two = terms(zz, sum_v, rr_v, rl_v)
            out_v[...] = one[slot] + two[slot]
            out_copy_v(m).start()

        for going in (1, -1):
            first, last = ends(zz, going)
            if not last:
                @pl.when(beyond(m, zz, going))
                def _():
                    v_copy(m, going, first).wait_send()

            if not first:
                credit = rv_credit if going > 0 else lv_credit

                @pl.when(jnp.logical_and(beyond(m, zz - going, going), m < total - SLOTS))
                def _():
                    signal(credit, me - 2 * going)

    def v_of(n):
        m = jnp.where(n == 0, 0, jnp.where(n < switch, n - 1, n - 2))
        none = (n < 0) | (n == 1) | (n == switch - 1) | (n >= last_step)
        return jnp.where(none, -1, m)

    def u_of(n):
        m = jnp.where(n == 1, 0, jnp.where(n < switch, n - 2, n - 3))
        none = (n < 1) | (n == 2) | (n == switch) | (n > last_step)
        return jnp.where(none, -1, m)

    def sums(n, index, pair, mine, got, into, credit, flow, finish):
        m_core = index(n - 1)

        @pl.when(m_core >= 0)
        def _():
            pair(m_core).wait_recv()
            into[m_core % SLOTS] = mine(m_core % 2) + got[m_core % 2]
            pair(m_core).wait_send()

            @pl.when(m_core < total - 2)
            def _():
                signal(credit, peer)

        for zz in range(CHIPS):
            @pl.when(z == zz)
            def _():
                for ahead, going in sorted([(zz, 1), (CHIPS - 1 - zz, -1)]):
                    m = index(n - 1 - ahead)

                    @pl.when(m >= 0)
                    def _():
                        flow(m, zz, going)

                m_end = index(n - CHIPS)

                @pl.when(m_end >= 0)
                def _():
                    finish(m_end, zz)

    def all_sums(n):
        sums(n, v_of, d_v, lambda slot: own_v[slot, core], in_v, sum_v, dv_credit, flow_v, finish_v)
        sums(n, u_of, d_u, lambda slot: own_u[slot, :, core], in_u, sum_u, du_credit, flow_u, finish_u)

    def step(n, carry):
        mv, mu = v_of(n), u_of(n)
        has_v, has_u = mv >= 0, mu >= 0
        both = has_v & has_u
        back = n < switch

        @pl.when(has_v)
        def _():
            @pl.when(mv + 1 < total)
            def _():
                for cp in w_copies(mv + 1):
                    cp.start()

            for cp in w_copies(mv):
                cp.wait()

        @pl.when(n == switch)
        def _():
            for i in range(tiles):
                x_copy(x0_h, i).start()

        @pl.when(has_v)
        def _():
            own_v[mv % 2] = jnp.zeros(own_v.shape[1:], F32)

        @pl.when(has_u)
        def _():
            own_u[mu % 2] = jnp.zeros(own_u.shape[1:], F32)

        early = jnp.where(n == 1, 0, tiles // 4)

        def half(phase, c):
            lo = jnp.where(phase == 0, 0, early)
            hi = jnp.where(phase == 0, early, tiles)

            def loop(cond, body):
                @pl.when(cond)
                def _():
                    lax.fori_loop(lo, hi, body, 0)

            def v_body(i, c):
                arrive(n, i)
                v_tile(mv, i)
                return c

            def u_body(is_back):
                def body(i, c):
                    u_tile(mu, i, is_back)
                    return c
                return body

            def both_body(is_back):
                def body(i, c):
                    both_tile(mv, mu, i, is_back)
                    return c
                return body

            loop(has_v & ~has_u, v_body)
            loop(has_u & ~has_v & back, u_body(True))
            loop(has_u & ~has_v & ~back, u_body(False))
            loop(both & back, both_body(True))
            loop(both & ~back, both_body(False))

            @pl.when(phase == 0)
            def _():
                all_sums(n)

            return c

        lax.fori_loop(0, 2, half, 0)

        def send_pair(m, pair, credit):
            @pl.when(m >= 0)
            def _():
                @pl.when(m >= 2)
                def _():
                    pl.semaphore_wait(credit, 1)

                pair(m).start()

        send_pair(mv, d_v, dv_credit)
        send_pair(mu, d_u, du_credit)
        return carry

    lax.fori_loop(0, last_step + CHIPS + 1, step, 0)

    for m in (total - 2, total - 1):
        for cp in out_copies_u(m):
            cp.wait()
    out_copy_v(total - CHIPS).wait()


def gradients(x1, x0, r, w_up, w_down, block, unit):
    toks, dim = x0.shape
    layers, _, ff = w_up.shape
    rows_u = dim // (2 * CHIPS)
    wide = 2 * unit
    tiles = toks // block
    dma = pltpu.SemaphoreType.DMA
    vm = pltpu.VMEM
    u_blk = (CHIPS, rows_u, wide)
    v_blk = (unit, dim)
    scratch = [
        vm((toks, dim), BF16), vm((toks, dim), BF16), vm((toks, dim), F32), vm((toks, wide), F32),
        vm((WSLOTS, dim, wide), BF16), vm((WSLOTS, wide, dim), BF16),
        vm((2, CHIPS, 2, rows_u, wide), F32), vm((2, 2) + v_blk, F32),
        vm((2,) + u_blk, F32), vm((2,) + v_blk, F32),
        vm((SLOTS,) + u_blk, F32), vm((SLOTS,) + v_blk, F32),
        vm((SLOTS,) + u_blk, F32), vm((SLOTS,) + v_blk, F32),
        vm((SLOTS,) + u_blk, F32), vm((SLOTS,) + v_blk, F32),
        vm((2, rows_u, wide), F32), vm(v_blk, F32),
        dma((tiles,)), dma((tiles,)), dma((WSLOTS, 4)), dma((2, 2)), dma((2, 2)),
    ] + [dma((SLOTS,))] * 8 + [dma((2, 2)), dma] + [pltpu.SemaphoreType.REGULAR] * 6
    return pl.pallas_call(
        functools.partial(grad_kernel, unit, block),
        out_shape=[
            jax.ShapeDtypeStruct((layers, rows_u, ff), F32),
            jax.ShapeDtypeStruct((layers, ff // (2 * CHIPS), dim), F32),
        ],
        in_specs=[ANY] * 5,
        out_specs=[ANY] * 2,
        scratch_shapes=scratch,
        compiler_params=pltpu.CompilerParams(
            collective_id=0, has_side_effects=True, vmem_limit_bytes=62 * 1024 * 1024),
        name="grads",
    )(x1, x0, r, w_up, w_down)


def solution(mesh, block=512, unit=128):
    def local_step(acts_in, cot_out, lengths, w_up, w_down):
        micro, tok_rows, dim = acts_in.shape
        x0 = acts_in.reshape(micro * tok_rows, dim)
        g = cot_out.reshape(micro * tok_rows, dim)
        x1, r = forward(x0, g, lengths.reshape(micro), w_up, w_down, micro, block)
        return gradients(x1, x0, r, w_up, w_down, block, unit)

    act_spec = P(None, ("part", "fsdp"), None)
    grad_spec = P("part", "fsdp", None)
    return jax.shard_map(
        local_step, mesh=mesh,
        in_specs=(act_spec, act_spec, P(None, ("part", "fsdp")), P(), P()),
        out_specs=(grad_spec, grad_spec), check_vma=False)
```

```python
import functools

import jax
import jax.numpy as jnp
from jax import lax
from jax.experimental import pallas as pl
from jax.experimental.pallas import tpu as pltpu
from jax.sharding import PartitionSpec as P

MESH = pl.DeviceIdType.MESH
F32 = jnp.float32
BF16 = jnp.bfloat16

C1 = 0.7978845608028654
K1 = C1 * 0.044715
K3 = 3.0 * K1

CHIPS = 4
HOP = 2
SLOTS = 8
PARTS = 4
SHIFT = 1


def dot(lhs, rhs, dims):
    return lax.dot_general(lhs, rhs, (dims, ((), ())), preferred_element_type=F32)


def gelu_parts(h_wide):
    sq = h_wide * h_wide
    th = jnp.tanh(h_wide * (C1 + K1 * sq))
    return sq, th, 0.5 + 0.5 * th


def kernel(unit, block, micro, len_s, x0_h, g_h, wu_h, wd_h, gu_h, gd_h,
           xv, rv, x_extra, w1v, w2v, own_u, own_v, in_u, in_v, sum_u, sum_v,
           rr_u, rr_v, rl_u, rl_v, out_u, out_v,
           x_sem, r_sem, w_sem, f_sem, t_send, t_recv, ds_sem, dr_sem,
           rs_u, rq_u, ls_u, lq_u, rs_v, rq_v, ls_v, lq_v,
           ou_sem, ov_sem, du_credit, dv_credit, ru_credit, lu_credit, rv_credit, lv_credit):
    toks, dim = x0_h.shape
    layers, _, ff = wu_h.shape
    tiles = toks // block
    wide = 2 * unit
    per_dev = ff // (2 * CHIPS)
    per_layer = ff // wide
    total = layers * per_layer

    me = lax.axis_index("fsdp")
    z = me // 2
    core = me % 2
    peer = z * 2 + (1 - core)
    at_end = (z == 0) | (z == CHIPS - 1)
    inward = jnp.where(z < CHIPS // 2, me + 2, me - 2)
    outward = jnp.where(z < CHIPS // 2, me - 2, me + 2)
    mine = jnp.where(at_end, tiles - SHIFT, tiles + SHIFT)

    def signal(sem, dev):
        pl.semaphore_signal(sem, inc=1, device_id={"fsdp": dev}, device_id_type=MESH)

    def remote(src, dst, ssem, rsem, dev):
        return pltpu.make_async_remote_copy(
            src_ref=src, dst_ref=dst, send_sem=ssem, recv_sem=rsem,
            device_id={"fsdp": dev}, device_id_type=MESH)

    barrier = pltpu.get_barrier_semaphore()
    signal(barrier, peer)

    @pl.when(z > 0)
    def _():
        signal(barrier, me - 2)

    @pl.when(z < CHIPS - 1)
    def _():
        signal(barrier, me + 2)

    def layer_of(m):
        return layers - 1 - m // per_layer

    def owner_of(m):
        return (1 + 3 * (m % per_layer)) % CHIPS

    def cols_of(m):
        base = 2 * per_dev * owner_of(m) + unit * ((m % per_layer) // CHIPS)
        return pl.multiple_of(base, unit), pl.multiple_of(base + per_dev, unit)

    def w_copies(m):
        slot = m % 2
        out = []
        for half, start in enumerate(cols_of(m)):
            span = pl.ds(start, unit)
            here = pl.ds(half * unit, unit)
            out.append(pltpu.make_async_copy(
                wu_h.at[layer_of(m), :, span], w1v.at[slot, :, here], w_sem.at[slot, half]))
            out.append(pltpu.make_async_copy(
                wd_h.at[layer_of(m), span, :], w2v.at[slot, here, :], w_sem.at[slot, 2 + half]))
        return out

    def rows_of(i):
        return pl.ds(pl.multiple_of(i * block, block), block)

    def x_copy(i):
        return pltpu.make_async_copy(x0_h.at[rows_of(i), :], xv.at[rows_of(i), :], x_sem.at[i])

    def r_copy(i):
        return pltpu.make_async_copy(g_h.at[rows_of(i), :], rv.at[rows_of(i), :], r_sem.at[i])

    def mask(i):
        per = tiles // micro
        left = len_s[i // per] - (i % per) * block
        r_val = rv[rows_of(i), :]
        row_ids = lax.broadcasted_iota(jnp.int32, r_val.shape, 0)
        rv[rows_of(i), :] = jnp.where(row_ids < left, r_val, jnp.zeros_like(r_val))

    def tile_copies(k, dev):
        src = rows_of(tiles - SHIFT + k)
        dst = rows_of(tiles + k)
        return [
            remote(xv.at[src, :], xv.at[dst, :], t_send.at[0, k], t_recv.at[0, k], dev),
            remote(rv.at[src, :], rv.at[dst, :], t_send.at[1, k], t_recv.at[1, k], dev),
        ]

    def forward(w1f, w2f, a_scr):
        width = ff // PARTS

        def w1_copy(part):
            cols = pl.ds(part * width, width)
            return pltpu.make_async_copy(wu_h.at[0, :, cols], w1f.at[:, cols], f_sem.at[part])

        w2_copy = pltpu.make_async_copy(wd_h.at[0], w2f, f_sem.at[PARTS])
        for k in range(SHIFT):
            @pl.when(at_end)
            def _():
                x_copy(tiles - SHIFT + k).start()
                r_copy(tiles - SHIFT + k).start()

        for i in range(tiles - SHIFT):
            x_copy(i).start()
            if i == 0:
                for part in range(PARTS):
                    w1_copy(part).start()
                w2_copy.start()
        for i in range(tiles - SHIFT):
            r_copy(i).start()

        @pl.when(~at_end)
        def _():
            for k in range(SHIFT):
                x_copy(tiles - SHIFT + k).start()
                r_copy(tiles - SHIFT + k).start()

        for cp in w_copies(0):
            cp.start()
        peers = 1 + jnp.where(z > 0, 1, 0) + jnp.where(z < CHIPS - 1, 1, 0)
        pl.semaphore_wait(barrier, peers)

        @pl.when(at_end)
        def _():
            for k in range(SHIFT):
                i = tiles - SHIFT + k
                x_copy(i).wait()
                r_copy(i).wait()
                mask(i)
                for cp in tile_copies(k, inward):
                    cp.start()

        def tile(i, first):
            @pl.when(i < tiles)
            def _():
                x_copy(i).wait()
                r_copy(i).wait()
                mask(i)

            for k in range(SHIFT):
                @pl.when(i == tiles + k)
                def _():
                    for cp in tile_copies(k, outward):
                        cp.wait_recv()
                    x_extra[k * block:(k + 1) * block, :] = xv[rows_of(i), :]

            x_val = xv[rows_of(i), :]
            for part in range(PARTS):
                cols = slice(part * width, (part + 1) * width)

                if first:
                    w1_copy(part).wait()
                h_val = dot(x_val, w1f[:, cols], ((1,), (0,))).astype(BF16).astype(F32)
                _, _, cdf = gelu_parts(h_val)
                a_scr[:, cols] = (h_val * cdf).astype(BF16)

            if first:
                w2_copy.wait()
            y_val = dot(a_scr[...], w2f[...], ((1,), (0,))).astype(BF16)
            xv[rows_of(i), :] = (x_val.astype(F32) + y_val.astype(F32)).astype(BF16)

        def rest(i, carry):
            tile(i, False)
            return carry

        tile(0, True)
        lax.fori_loop(1, mine, rest, 0)

        @pl.when(at_end)
        def _():
            for k in range(SHIFT):
                for cp in tile_copies(k, inward):
                    cp.wait_send()

    pl.run_scoped(
        forward,
        pltpu.VMEM((dim, ff), BF16), pltpu.VMEM((ff, dim), BF16), pltpu.VMEM((block, ff), BF16))

    def backward(dxa):
        def clear(i, carry):
            dxa[rows_of(i), :] = jnp.zeros((block, dim), F32)
            return carry

        lax.fori_loop(0, mine, clear, 0)

        def tile(m, i, back):
            slot = m % 2
            rows = rows_of(i)

            @pl.when(m == per_layer)
            def _():
                @pl.when(i < tiles)
                def _():
                    x_copy(i).wait()

                for k in range(SHIFT):
                    @pl.when(i == tiles + k)
                    def _():
                        xv[rows, :] = x_extra[k * block:(k + 1) * block, :]

                rv[rows, :] = (rv[rows, :].astype(F32) + dxa[rows, :]).astype(BF16)

            x_i, r_i = xv[rows, :], rv[rows, :]
            h_val = dot(x_i, w1v[slot], ((1,), (0,))).astype(BF16).astype(F32)
            da_val = dot(r_i, w2v[slot], ((1,), (1,)))
            sq, th, cdf = gelu_parts(h_val)
            a_val = (h_val * cdf).astype(BF16)
            slope = cdf + (h_val * (0.5 - 0.5 * (th * th))) * (C1 + K3 * sq)
            dh_val = (da_val * slope).astype(BF16)
            own_v[slot] += dot(a_val, r_i, ((0,), (0,))).reshape(own_v.shape[1:])
            own_u[slot] += dot(x_i, dh_val, ((0,), (0,))).reshape(own_u.shape[1:])
            if back:
                dxa[rows, :] += dot(dh_val, w1v[slot], ((1,), (1,)))

        def d_copies(m):
            slot = m % 2
            return (
                remote(own_u.at[slot, :, 1 - core], in_u.at[slot], ds_sem.at[0, slot], dr_sem.at[0, slot], peer),
                remote(own_v.at[slot, 1 - core], in_v.at[slot], ds_sem.at[1, slot], dr_sem.at[1, slot], peer),
            )

        def u_copy(m, zz, going, first):
            slot = m % SLOTS
            dst, ssem, qsem = (rr_u, rs_u, rq_u) if going > 0 else (rl_u, ls_u, lq_u)
            src = sum_u if first else dst
            part = pl.ds(zz + 1, CHIPS - 1 - zz) if going > 0 else pl.ds(0, zz)
            return remote(src.at[slot, part], dst.at[slot, part], ssem.at[slot], qsem.at[slot], me + 2 * going)

        def v_copy(m, going, first):
            slot = m % SLOTS
            dst, ssem, qsem = (rr_v, rs_v, rq_v) if going > 0 else (rl_v, ls_v, lq_v)
            src = sum_v if first else dst
            return remote(src.at[slot], dst.at[slot], ssem.at[slot], qsem.at[slot], me + 2 * going)

        def beyond(m, zz, going):
            return owner_of(m) > zz if going > 0 else owner_of(m) < zz

        def ends(zz, going):
            start, stop = (0, CHIPS - 1) if going > 0 else (CHIPS - 1, 0)
            return zz == start, zz == stop

        def turn(zz, going):
            return zz if going > 0 else CHIPS - 1 - zz

        def keeps(zz, going):
            return 2 * turn(zz, going) < CHIPS - 1

        def flow(m, zz, going):
            slot = m % SLOTS
            first, last = ends(zz, going)
            got, credit = (rr_u, ru_credit) if going > 0 else (rl_u, lu_credit)
            if not first:
                u_copy(m, zz - going, going, False).wait_recv()
                near = zz if keeps(zz, going) else zz + going
                lo, hi = (near, CHIPS) if going > 0 else (0, near + 1)
                if hi > lo:
                    got[slot, lo:hi] += sum_u[slot, lo:hi]
            if not last:
                @pl.when(m >= SLOTS)
                def _():
                    pl.semaphore_wait(credit, 1)

                u_copy(m, zz, going, first).start()

            got, credit = (rr_v, rv_credit) if going > 0 else (rl_v, lv_credit)
            if not first:
                @pl.when(beyond(m, zz - going, going))
                def _():
                    v_copy(m, going, False).wait_recv()

                @pl.when(beyond(m, zz - going if keeps(zz, going) else zz, going))
                def _():
                    got[slot] += sum_v[slot]

            if not last:
                @pl.when(beyond(m, zz, going))
                def _():
                    @pl.when(m >= SLOTS)
                    def _():
                        pl.semaphore_wait(credit, 1)

                    v_copy(m, going, first).start()

        def out_copies_u(m):
            slot = m % 2
            return [
                pltpu.make_async_copy(out_u.at[slot, :, pl.ds(half * unit, unit)],
                                      gu_h.at[layer_of(m), :, pl.ds(start, unit)], ou_sem.at[slot, half])
                for half, start in enumerate(cols_of(m))
            ]

        def out_copy_v(m):
            start = pl.multiple_of(unit * ((m % per_layer) // CHIPS), unit)
            return pltpu.make_async_copy(out_v, gd_h.at[layer_of(m), pl.ds(start, unit), :], ov_sem)

        def terms(zz, total_ref, right_ref, left_ref):
            if zz == 0:
                return total_ref, left_ref
            if zz == CHIPS - 1:
                return total_ref, right_ref
            return right_ref, left_ref

        def finish(m, zz):
            slot = m % SLOTS

            @pl.when(m >= 2)
            def _():
                for cp in out_copies_u(m - 2):
                    cp.wait()

            one, two = terms(zz, sum_u, rr_u, rl_u)
            out_u[m % 2] = one[slot, zz] + two[slot, zz]
            for cp in out_copies_u(m):
                cp.start()

            @pl.when(owner_of(m) == zz)
            def _():
                @pl.when(m >= CHIPS)
                def _():
                    out_copy_v(m - CHIPS).wait()

                one, two = terms(zz, sum_v, rr_v, rl_v)
                out_v[...] = one[slot] + two[slot]
                out_copy_v(m).start()

            again = m < total - SLOTS
            for going in (1, -1):
                first, last = ends(zz, going)
                if not last:
                    u_copy(m, zz, going, first).wait_send()

                    @pl.when(beyond(m, zz, going))
                    def _():
                        v_copy(m, going, first).wait_send()

                if not first:
                    @pl.when(again)
                    def _():
                        signal(ru_credit if going > 0 else lu_credit, me - 2 * going)

                    @pl.when(again & beyond(m, zz - going, going))
                    def _():
                        signal(rv_credit if going > 0 else lv_credit, me - 2 * going)

        def upto(k, n):
            late = n - total
            draining = jnp.where(late < k, total + 1 - HOP * (k - late), total)
            return jnp.maximum(jnp.where(n < total, n - HOP * k, draining), 0)

        def turns(k, n, body):
            def one(m, carry):
                body(m)
                return carry

            lax.fori_loop(upto(k, n - 1), upto(k, n), one, 0)

        def add_cores(m):
            for cp in d_copies(m):
                cp.wait_recv()
            sum_u[m % SLOTS] = own_u[m % 2, :, core] + in_u[m % 2]
            sum_v[m % SLOTS] = own_v[m % 2, core] + in_v[m % 2]
            for cp in d_copies(m):
                cp.wait_send()

            @pl.when(m < total - 2)
            def _():
                signal(du_credit, peer)
                signal(dv_credit, peer)

        def all_sums(n):
            turns(0, n, add_cores)
            for zz in range(CHIPS):
                @pl.when(z == zz)
                def _():
                    near, far = sorted((1, -1), key=lambda going: turn(zz, going))

                    def go(going):
                        turns(turn(zz, going), n, lambda m: flow(m, zz, going))

                    if turn(zz, near) == 0:
                        go(near)
                        go(far)
                    else:
                        @pl.when(n < total)
                        def _():
                            go(near)

                        go(far)

                        @pl.when(n >= total)
                        def _():
                            go(near)

                    turns(CHIPS - 1, n, lambda m: finish(m, zz))

        def step(n, carry):
            run = n < total

            @pl.when(run)
            def _():
                @pl.when(n + 1 < total)
                def _():
                    for cp in w_copies(n + 1):
                        cp.start()

                for cp in w_copies(n):
                    cp.wait()

                own_u[n % 2] = jnp.zeros(own_u.shape[1:], F32)
                own_v[n % 2] = jnp.zeros(own_v.shape[1:], F32)

                @pl.when(n == per_layer)
                def _():
                    for i in range(tiles - SHIFT):
                        x_copy(i).start()

                    @pl.when(~at_end)
                    def _():
                        for k in range(SHIFT):
                            x_copy(tiles - SHIFT + k).start()

            early = jnp.minimum((3 * n + 1) // 2, mine)

            def half(phase, c):
                lo = jnp.where(phase == 0, 0, early)
                hi = jnp.where(phase == 0, early, mine)

                def loop(cond, back):
                    @pl.when(cond)
                    def _():
                        def body(i, cc):
                            tile(n, i, back)
                            return cc

                        lax.fori_loop(lo, hi, body, 0)

                loop(run & (n < per_layer), True)
                loop(run & (n >= per_layer), False)

                @pl.when(run & (phase == 1))
                def _():
                    @pl.when(n >= 2)
                    def _():
                        pl.semaphore_wait(du_credit, 1)
                        pl.semaphore_wait(dv_credit, 1)

                    for cp in d_copies(n):
                        cp.start()

                @pl.when((phase == 0) == (early < mine))
                def _():
                    all_sums(n)

                return c

            lax.fori_loop(0, 2, half, 0)
            return carry

        lax.fori_loop(0, total + CHIPS, step, 0)

        for m in (total - 2, total - 1):
            for cp in out_copies_u(m):
                cp.wait()
        out_copy_v(total - CHIPS).wait()

    pl.run_scoped(backward, pltpu.VMEM(xv.shape, F32))


def gradients(x0, g, lengths, w_up, w_down, block, unit):
    toks, dim = x0.shape
    micro = lengths.shape[0]
    layers, _, ff = w_up.shape
    rows_u = dim // (2 * CHIPS)
    wide = 2 * unit
    tiles = toks // block
    held = toks + SHIFT * block
    dma = pltpu.SemaphoreType.DMA
    vm = pltpu.VMEM
    u_blk = (CHIPS, rows_u, wide)
    v_blk = (unit, dim)
    scratch = [
        vm((held, dim), BF16), vm((held, dim), BF16), vm((SHIFT * block, dim), BF16),
        vm((2, dim, wide), BF16), vm((2, wide, dim), BF16),
        vm((2, CHIPS, 2, rows_u, wide), F32), vm((2, 2) + v_blk, F32),
        vm((2,) + u_blk, F32), vm((2,) + v_blk, F32),
        vm((SLOTS,) + u_blk, F32), vm((SLOTS,) + v_blk, F32),
        vm((SLOTS,) + u_blk, F32), vm((SLOTS,) + v_blk, F32),
        vm((SLOTS,) + u_blk, F32), vm((SLOTS,) + v_blk, F32),
        vm((2, rows_u, wide), F32), vm(v_blk, F32),
        dma((tiles,)), dma((tiles,)), dma((2, 4)), dma((PARTS + 1,)),
        dma((2, SHIFT)), dma((2, SHIFT)), dma((2, 2)), dma((2, 2)),
    ] + [dma((SLOTS,))] * 8 + [dma((2, 2)), dma] + [pltpu.SemaphoreType.REGULAR] * 6
    any_space = pl.BlockSpec(memory_space=pl.ANY)
    return pl.pallas_call(
        functools.partial(kernel, unit, block, micro),
        out_shape=[
            jax.ShapeDtypeStruct((layers, rows_u, ff), F32),
            jax.ShapeDtypeStruct((layers, ff // (2 * CHIPS), dim), F32),
        ],
        in_specs=[pl.BlockSpec(memory_space=pltpu.SMEM)] + [any_space] * 4,
        out_specs=[any_space] * 2,
        scratch_shapes=scratch,
        compiler_params=pltpu.CompilerParams(
            collective_id=0, has_side_effects=True, vmem_limit_bytes=62 * 1024 * 1024),
        name="grads",
    )(lengths, x0, g, w_up, w_down)


def solution(mesh, block=512, unit=128):
    def local_step(acts_in, cot_out, lengths, w_up, w_down):
        micro, tok_rows, dim = acts_in.shape
        x0 = acts_in.reshape(micro * tok_rows, dim)
        g = cot_out.reshape(micro * tok_rows, dim)
        return gradients(x0, g, lengths.reshape(micro), w_up, w_down, block, unit)

    act_spec = P(None, ("part", "fsdp"), None)
    grad_spec = P("part", "fsdp", None)
    return jax.shard_map(
        local_step, mesh=mesh,
        in_specs=(act_spec, act_spec, P(None, ("part", "fsdp")), P(), P()),
        out_specs=(grad_spec, grad_spec), check_vma=False)
```

```python
import functools

import jax
import jax.numpy as jnp
from jax import lax
from jax.experimental import pallas as pl
from jax.experimental.pallas import tpu as pltpu
from jax.sharding import PartitionSpec as P

MESH = pl.DeviceIdType.MESH
F32 = jnp.float32
BF16 = jnp.bfloat16

C1 = 0.7978845608028654
K1 = C1 * 0.044715
K3 = 3.0 * K1

CHIPS = 4
HOP = 2
SLOTS = 8
PIECES = 4
PARTS = 4


def dot(lhs, rhs, dims):
    return lax.dot_general(lhs, rhs, (dims, ((), ())), preferred_element_type=F32)


def gelu_parts(h_wide):
    sq = h_wide * h_wide
    th = jnp.tanh(h_wide * (C1 + K1 * sq))
    return sq, th, 0.5 + 0.5 * th


def kernel(unit, block, fblock, micro, len_s, x0_h, g_h, wu_h, wd_h, gu_h, gd_h,
           xv, rv, w1v, w2v, own_u, own_v, in_u, in_v, sum_u, sum_v,
           rr_u, rr_v, rl_u, rl_v, out_u, out_v,
           x_sem, r_sem, w_sem, f_sem, ds_sem, dr_sem,
           rs_u, rq_u, ls_u, lq_u, rs_v, rq_v, ls_v, lq_v,
           ou_sem, ov_sem, du_credit, dv_credit, ru_credit, lu_credit, rv_credit, lv_credit):
    toks, dim = x0_h.shape
    layers, _, ff = wu_h.shape
    tiles = toks // block
    ftiles = toks // fblock
    piece = unit // PIECES
    wide = 2 * unit
    per_dev = ff // (2 * CHIPS)
    per_layer = ff // wide
    total = layers * per_layer

    me = lax.axis_index("fsdp")
    z = me // 2
    core = me % 2
    peer = z * 2 + (1 - core)

    def signal(sem, dev):
        pl.semaphore_signal(sem, inc=1, device_id={"fsdp": dev}, device_id_type=MESH)

    def remote(src, dst, ssem, rsem, dev):
        return pltpu.make_async_remote_copy(
            src_ref=src, dst_ref=dst, send_sem=ssem, recv_sem=rsem,
            device_id={"fsdp": dev}, device_id_type=MESH)

    barrier = pltpu.get_barrier_semaphore()
    signal(barrier, peer)

    @pl.when(z > 0)
    def _():
        signal(barrier, me - 2)

    @pl.when(z < CHIPS - 1)
    def _():
        signal(barrier, me + 2)

    def layer_of(m):
        return layers - 1 - m // per_layer

    def owner_of(m):
        return (1 + 3 * (m % per_layer)) % CHIPS

    def cols_of(m):
        base = 2 * per_dev * owner_of(m) + unit * ((m % per_layer) // CHIPS)
        return pl.multiple_of(base, unit), pl.multiple_of(base + per_dev, unit)

    def w_copies(m):
        slot = m % 2
        out = []
        for half, start in enumerate(cols_of(m)):
            span = pl.ds(start, unit)
            here = pl.ds(half * unit, unit)
            out.append(pltpu.make_async_copy(
                wu_h.at[layer_of(m), :, span], w1v.at[slot, :, here], w_sem.at[slot, half]))
            out.append(pltpu.make_async_copy(
                wd_h.at[layer_of(m), span, :], w2v.at[slot, here, :], w_sem.at[slot, 2 + half]))
        return out

    def rows_of(i):
        return pl.ds(pl.multiple_of(i * block, block), block)

    def frows_of(i):
        return pl.ds(pl.multiple_of(i * fblock, fblock), fblock)

    def x_copy(i):
        return pltpu.make_async_copy(x0_h.at[frows_of(i), :], xv.at[frows_of(i), :], x_sem.at[i])

    def r_copy(i):
        return pltpu.make_async_copy(g_h.at[frows_of(i), :], rv.at[frows_of(i), :], r_sem.at[i])

    def mask(i):
        per = ftiles // micro
        left = len_s[i // per] - (i % per) * fblock
        r_val = rv[frows_of(i), :]
        row_ids = lax.broadcasted_iota(jnp.int32, r_val.shape, 0)
        rv[frows_of(i), :] = jnp.where(row_ids < left, r_val, jnp.zeros_like(r_val))

    def forward(w1f, w2f, a_scr):
        width = ff // PARTS

        def w1_copy(part):
            cols = pl.ds(part * width, width)
            return pltpu.make_async_copy(wu_h.at[0, :, cols], w1f.at[:, cols], f_sem.at[part])

        w2_copy = pltpu.make_async_copy(wd_h.at[0], w2f, f_sem.at[PARTS])
        for i in range(ftiles):
            x_copy(i).start()
            if i == 0:
                for part in range(PARTS):
                    w1_copy(part).start()
                w2_copy.start()
        for i in range(ftiles):
            r_copy(i).start()

        for cp in w_copies(0):
            cp.start()
        peers = 1 + jnp.where(z > 0, 1, 0) + jnp.where(z < CHIPS - 1, 1, 0)
        pl.semaphore_wait(barrier, peers)

        def tile(i, first):
            x_copy(i).wait()
            r_copy(i).wait()
            mask(i)
            x_val = xv[frows_of(i), :]
            for part in range(PARTS):
                cols = slice(part * width, (part + 1) * width)

                if first:
                    w1_copy(part).wait()
                h_val = dot(x_val, w1f[:, cols], ((1,), (0,))).astype(BF16).astype(F32)
                _, _, cdf = gelu_parts(h_val)
                a_scr[:, cols] = (h_val * cdf).astype(BF16)

            if first:
                w2_copy.wait()
            y_val = dot(a_scr[...], w2f[...], ((1,), (0,))).astype(BF16)
            xv[frows_of(i), :] = (x_val.astype(F32) + y_val.astype(F32)).astype(BF16)

        def rest(i, carry):
            tile(i, False)
            return carry

        tile(0, True)
        lax.fori_loop(1, ftiles, rest, 0)

    pl.run_scoped(
        forward,
        pltpu.VMEM((dim, ff), BF16), pltpu.VMEM((ff, dim), BF16), pltpu.VMEM((fblock, ff), BF16))

    def backward(dxa):
        def clear(i, carry):
            dxa[rows_of(i), :] = jnp.zeros((block, dim), F32)
            return carry

        lax.fori_loop(0, tiles, clear, 0)

        def tile(m, i, back):
            slot = m % 2
            rows = rows_of(i)

            @pl.when(m == per_layer)
            def _():
                for k in range(block // fblock):
                    x_copy(i * (block // fblock) + k).wait()
                rv[rows, :] = (rv[rows, :].astype(F32) + dxa[rows, :]).astype(BF16)

            x_i, r_i = xv[rows, :], rv[rows, :]
            h_val = dot(x_i, w1v[slot], ((1,), (0,))).astype(BF16).astype(F32)
            da_val = dot(r_i, w2v[slot], ((1,), (1,)))
            sq, th, cdf = gelu_parts(h_val)
            a_val = (h_val * cdf).astype(BF16)
            slope = cdf + (h_val * (0.5 - 0.5 * (th * th))) * (C1 + K3 * sq)
            dh_val = (da_val * slope).astype(BF16)
            own_v[slot] += dot(a_val, r_i, ((0,), (0,))).reshape(own_v.shape[1:])
            own_u[slot] += dot(x_i, dh_val, ((0,), (0,))).reshape(own_u.shape[1:])
            if back:
                dxa[rows, :] += dot(dh_val, w1v[slot], ((1,), (1,)))

        def d_copies(m):
            slot = m % 2
            return (
                remote(own_u.at[slot, :, 1 - core], in_u.at[slot], ds_sem.at[0, slot], dr_sem.at[0, slot], peer),
                remote(own_v.at[slot, 1 - core], in_v.at[slot], ds_sem.at[1, slot], dr_sem.at[1, slot], peer),
            )

        def far_first(zz, going):
            return list(range(CHIPS - 1, zz, -1)) if going > 0 else list(range(zz))

        def u_copy(m, blk, going, first):
            slot = m % SLOTS
            dst, ssem, qsem = (rr_u, rs_u, rq_u) if going > 0 else (rl_u, ls_u, lq_u)
            src = sum_u if first else dst
            return remote(src.at[slot, blk], dst.at[slot, blk], ssem.at[blk, slot], qsem.at[blk, slot], me + 2 * going)

        def v_copy(m, p, going, first):
            slot = m % SLOTS
            dst, ssem, qsem = (rr_v, rs_v, rq_v) if going > 0 else (rl_v, ls_v, lq_v)
            src = sum_v if first else dst
            part = pl.ds(p * piece, piece)
            return remote(src.at[slot, part], dst.at[slot, part], ssem.at[p, slot], qsem.at[p, slot], me + 2 * going)

        def beyond(m, zz, going):
            return owner_of(m) > zz if going > 0 else owner_of(m) < zz

        def ends(zz, going):
            start, stop = (0, CHIPS - 1) if going > 0 else (CHIPS - 1, 0)
            return zz == start, zz == stop

        def turn(zz, going):
            return zz if going > 0 else CHIPS - 1 - zz

        def keeps(zz, going):
            return 2 * turn(zz, going) < CHIPS - 1

        def flow(m, zz, going):
            slot = m % SLOTS
            first, last = ends(zz, going)
            keep = keeps(zz, going)
            got_u, credit_u = (rr_u, ru_credit) if going > 0 else (rl_u, lu_credit)
            got_v, credit_v = (rr_v, rv_credit) if going > 0 else (rl_v, lv_credit)

            if not last:
                @pl.when(m >= SLOTS)
                def _():
                    pl.semaphore_wait(credit_u, 1)

                @pl.when((m >= SLOTS) & beyond(m, zz, going))
                def _():
                    pl.semaphore_wait(credit_v, 1)

            def pass_u(blk):
                if not first:
                    u_copy(m, blk, going, False).wait_recv()
                    if blk != zz or keep:
                        got_u[slot, blk] += sum_u[slot, blk]
                if blk != zz:
                    u_copy(m, blk, going, first).start()

            blocks = far_first(zz, going) + ([] if first else [zz])
            pass_u(blocks[0])
            if not last:
                @pl.when(beyond(m, zz, going))
                def _():
                    for p in range(PIECES):
                        if not first:
                            part = pl.ds(p * piece, piece)
                            v_copy(m, p, going, False).wait_recv()
                            got_v[slot, part] += sum_v[slot, part]
                        v_copy(m, p, going, first).start()

            if not first:
                @pl.when(owner_of(m) == zz)
                def _():
                    for p in range(PIECES):
                        v_copy(m, p, going, False).wait_recv()
                    if keep:
                        got_v[slot] += sum_v[slot]

            for blk in blocks[1:]:
                pass_u(blk)

        def out_copies_u(m):
            slot = m % 2
            return [
                pltpu.make_async_copy(out_u.at[slot, :, pl.ds(half * unit, unit)],
                                      gu_h.at[layer_of(m), :, pl.ds(start, unit)], ou_sem.at[slot, half])
                for half, start in enumerate(cols_of(m))
            ]

        def out_copy_v(m):
            start = pl.multiple_of(unit * ((m % per_layer) // CHIPS), unit)
            return pltpu.make_async_copy(out_v, gd_h.at[layer_of(m), pl.ds(start, unit), :], ov_sem)

        def terms(zz, total_ref, right_ref, left_ref):
            if zz == 0:
                return total_ref, left_ref
            if zz == CHIPS - 1:
                return total_ref, right_ref
            return right_ref, left_ref

        def finish(m, zz):
            slot = m % SLOTS

            @pl.when(m >= 2)
            def _():
                for cp in out_copies_u(m - 2):
                    cp.wait()

            one, two = terms(zz, sum_u, rr_u, rl_u)
            out_u[m % 2] = one[slot, zz] + two[slot, zz]
            for cp in out_copies_u(m):
                cp.start()

            @pl.when(owner_of(m) == zz)
            def _():
                @pl.when(m >= CHIPS)
                def _():
                    out_copy_v(m - CHIPS).wait()

                one, two = terms(zz, sum_v, rr_v, rl_v)
                out_v[...] = one[slot] + two[slot]
                out_copy_v(m).start()

            again = m < total - SLOTS
            for going in (1, -1):
                first, last = ends(zz, going)
                if not last:
                    for blk in far_first(zz, going):
                        u_copy(m, blk, going, first).wait_send()

                    @pl.when(beyond(m, zz, going))
                    def _():
                        for p in range(PIECES):
                            v_copy(m, p, going, first).wait_send()

                if not first:
                    @pl.when(again)
                    def _():
                        signal(ru_credit if going > 0 else lu_credit, me - 2 * going)

                    @pl.when(again & beyond(m, zz - going, going))
                    def _():
                        signal(rv_credit if going > 0 else lv_credit, me - 2 * going)

        def upto(k, n):
            late = n - total
            draining = jnp.where(late < k, total + 1 - HOP * (k - late), total)
            return jnp.maximum(jnp.where(n < total, n - HOP * k, draining), 0)

        def turns(k, n, body):
            def one(m, carry):
                body(m)
                return carry

            lax.fori_loop(upto(k, n - 1), upto(k, n), one, 0)

        def add_cores(m):
            for cp in d_copies(m):
                cp.wait_recv()
            sum_u[m % SLOTS] = own_u[m % 2, :, core] + in_u[m % 2]
            sum_v[m % SLOTS] = own_v[m % 2, core] + in_v[m % 2]
            for cp in d_copies(m):
                cp.wait_send()

            @pl.when(m < total - 2)
            def _():
                signal(du_credit, peer)
                signal(dv_credit, peer)

        def all_sums(n):
            turns(0, n, add_cores)
            for zz in range(CHIPS):
                @pl.when(z == zz)
                def _():
                    near, far = sorted((1, -1), key=lambda going: turn(zz, going))

                    def go(going):
                        turns(turn(zz, going), n, lambda m: flow(m, zz, going))

                    if turn(zz, near) == 0:
                        go(near)
                        go(far)
                    else:
                        @pl.when(n < total)
                        def _():
                            go(near)

                        go(far)

                        @pl.when(n >= total)
                        def _():
                            go(near)

                    turns(CHIPS - 1, n, lambda m: finish(m, zz))

        def step(n, carry):
            run = n < total

            @pl.when(run)
            def _():
                @pl.when(n + 1 < total)
                def _():
                    for cp in w_copies(n + 1):
                        cp.start()

                for cp in w_copies(n):
                    cp.wait()

                own_u[n % 2] = jnp.zeros(own_u.shape[1:], F32)
                own_v[n % 2] = jnp.zeros(own_v.shape[1:], F32)

                @pl.when(n == per_layer)
                def _():
                    for i in range(ftiles):
                        x_copy(i).start()


            def half(phase, c):
                lo = phase
                hi = jnp.where(phase == 0, 1, tiles)

                def loop(cond, back):
                    @pl.when(cond)
                    def _():
                        def body(i, cc):
                            tile(n, i, back)
                            return cc

                        lax.fori_loop(lo, hi, body, 0)

                loop(run & (n < per_layer), True)
                loop(run & (n >= per_layer), False)

                @pl.when(run & (phase == 1))
                def _():
                    @pl.when(n >= 2)
                    def _():
                        pl.semaphore_wait(du_credit, 1)
                        pl.semaphore_wait(dv_credit, 1)

                    for cp in d_copies(n):
                        cp.start()

                @pl.when(phase == 0)
                def _():
                    all_sums(n)

                return c

            lax.fori_loop(0, 2, half, 0)
            return carry

        lax.fori_loop(0, total + CHIPS, step, 0)

        for m in (total - 2, total - 1):
            for cp in out_copies_u(m):
                cp.wait()
        out_copy_v(total - CHIPS).wait()

    pl.run_scoped(backward, pltpu.VMEM(xv.shape, F32))


def gradients(x0, g, lengths, w_up, w_down, block, fblock, unit):
    toks, dim = x0.shape
    micro = lengths.shape[0]
    layers, _, ff = w_up.shape
    rows_u = dim // (2 * CHIPS)
    wide = 2 * unit
    ftiles = toks // fblock
    dma = pltpu.SemaphoreType.DMA
    vm = pltpu.VMEM
    u_blk = (CHIPS, rows_u, wide)
    v_blk = (unit, dim)
    scratch = [
        vm((toks, dim), BF16), vm((toks, dim), BF16),
        vm((2, dim, wide), BF16), vm((2, wide, dim), BF16),
        vm((2, CHIPS, 2, rows_u, wide), F32), vm((2, 2) + v_blk, F32),
        vm((2,) + u_blk, F32), vm((2,) + v_blk, F32),
        vm((SLOTS,) + u_blk, F32), vm((SLOTS,) + v_blk, F32),
        vm((SLOTS,) + u_blk, F32), vm((SLOTS,) + v_blk, F32),
        vm((SLOTS,) + u_blk, F32), vm((SLOTS,) + v_blk, F32),
        vm((2, rows_u, wide), F32), vm(v_blk, F32),
        dma((ftiles,)), dma((ftiles,)), dma((2, 4)), dma((PARTS + 1,)), dma((2, 2)), dma((2, 2)),
    ] + [dma((CHIPS, SLOTS))] * 4 + [dma((PIECES, SLOTS))] * 4 + [dma((2, 2)), dma] + [pltpu.SemaphoreType.REGULAR] * 6
    any_space = pl.BlockSpec(memory_space=pl.ANY)
    return pl.pallas_call(
        functools.partial(kernel, unit, block, fblock, micro),
        out_shape=[
            jax.ShapeDtypeStruct((layers, rows_u, ff), F32),
            jax.ShapeDtypeStruct((layers, ff // (2 * CHIPS), dim), F32),
        ],
        in_specs=[pl.BlockSpec(memory_space=pltpu.SMEM)] + [any_space] * 4,
        out_specs=[any_space] * 2,
        scratch_shapes=scratch,
        compiler_params=pltpu.CompilerParams(
            collective_id=0, has_side_effects=True, vmem_limit_bytes=62 * 1024 * 1024),
        name="grads",
    )(lengths, x0, g, w_up, w_down)


def solution(mesh, block=1024, fblock=512, unit=128):
    def local_step(acts_in, cot_out, lengths, w_up, w_down):
        micro, tok_rows, dim = acts_in.shape
        x0 = acts_in.reshape(micro * tok_rows, dim)
        g = cot_out.reshape(micro * tok_rows, dim)
        return gradients(x0, g, lengths.reshape(micro), w_up, w_down, block, fblock, unit)

    act_spec = P(None, ("part", "fsdp"), None)
    grad_spec = P("part", "fsdp", None)
    return jax.shard_map(
        local_step, mesh=mesh,
        in_specs=(act_spec, act_spec, P(None, ("part", "fsdp")), P(), P()),
        out_specs=(grad_spec, grad_spec), check_vma=False)
```

```python
import functools

import jax
import jax.numpy as jnp
from jax import lax
from jax.experimental import pallas as pl
from jax.experimental.pallas import tpu as pltpu
from jax.sharding import PartitionSpec as P

MESH = pl.DeviceIdType.MESH
F32 = jnp.float32
BF16 = jnp.bfloat16

C1 = 0.7978845608028654
K1 = C1 * 0.044715
K3 = 3.0 * K1

CHIPS = 4
HOP = 2
SLOTS = 8
PIECES = 4
PARTS = 4


def dot(lhs, rhs, dims):
    return lax.dot_general(lhs, rhs, (dims, ((), ())), preferred_element_type=F32)


def gelu_parts(h_wide):
    sq = h_wide * h_wide
    th = jnp.tanh(h_wide * (C1 + K1 * sq))
    return sq, th, 0.5 + 0.5 * th


def kernel(unit, block, fblock, micro, len_s, x0_h, g_h, wu_h, wd_h, gu_h, gd_h,
           xv, rv, x_extra, w1v, w2v, own_u, own_v, in_u, in_v, sum_u, sum_v,
           rr_u, rr_v, rl_u, rl_v, out_u, out_v,
           x_sem, r_sem, w_sem, f_sem, t_send, t_recv, ds_sem, dr_sem,
           rs_u, rq_u, ls_u, lq_u, rs_v, rq_v, ls_v, lq_v,
           ou_sem, ov_sem, du_credit, dv_credit, ru_credit, lu_credit, rv_credit, lv_credit):
    toks, dim = x0_h.shape
    layers, _, ff = wu_h.shape
    ftiles = toks // fblock
    piece = unit // PIECES
    wide = 2 * unit
    per_dev = ff // (2 * CHIPS)
    per_layer = ff // wide
    total = layers * per_layer

    me = lax.axis_index("fsdp")
    z = me // 2
    core = me % 2
    peer = z * 2 + (1 - core)
    at_end = (z == 0) | (z == CHIPS - 1)
    inward = jnp.where(z < CHIPS // 2, me + 2, me - 2)
    outward = jnp.where(z < CHIPS // 2, me - 2, me + 2)
    mine = jnp.where(at_end, ftiles - 1, ftiles + 1)
    full = mine // 2

    def signal(sem, dev):
        pl.semaphore_signal(sem, inc=1, device_id={"fsdp": dev}, device_id_type=MESH)

    def remote(src, dst, ssem, rsem, dev):
        return pltpu.make_async_remote_copy(
            src_ref=src, dst_ref=dst, send_sem=ssem, recv_sem=rsem,
            device_id={"fsdp": dev}, device_id_type=MESH)

    barrier = pltpu.get_barrier_semaphore()
    signal(barrier, peer)

    @pl.when(z > 0)
    def _():
        signal(barrier, me - 2)

    @pl.when(z < CHIPS - 1)
    def _():
        signal(barrier, me + 2)

    def layer_of(m):
        return layers - 1 - m // per_layer

    def owner_of(m):
        return (1 + 3 * (m % per_layer)) % CHIPS

    def cols_of(m):
        base = 2 * per_dev * owner_of(m) + unit * ((m % per_layer) // CHIPS)
        return pl.multiple_of(base, unit), pl.multiple_of(base + per_dev, unit)

    def w_copies(m):
        slot = m % 2
        out = []
        for half, start in enumerate(cols_of(m)):
            span = pl.ds(start, unit)
            here = pl.ds(half * unit, unit)
            out.append(pltpu.make_async_copy(
                wu_h.at[layer_of(m), :, span], w1v.at[slot, :, here], w_sem.at[slot, half]))
            out.append(pltpu.make_async_copy(
                wd_h.at[layer_of(m), span, :], w2v.at[slot, here, :], w_sem.at[slot, 2 + half]))
        return out

    def frows_of(i):
        return pl.ds(pl.multiple_of(i * fblock, fblock), fblock)

    def x_copy(i):
        return pltpu.make_async_copy(x0_h.at[frows_of(i), :], xv.at[frows_of(i), :], x_sem.at[i])

    def r_copy(i):
        return pltpu.make_async_copy(g_h.at[frows_of(i), :], rv.at[frows_of(i), :], r_sem.at[i])

    def mask(i):
        per = ftiles // micro
        left = len_s[i // per] - (i % per) * fblock
        r_val = rv[frows_of(i), :]
        row_ids = lax.broadcasted_iota(jnp.int32, r_val.shape, 0)
        rv[frows_of(i), :] = jnp.where(row_ids < left, r_val, jnp.zeros_like(r_val))

    def tile_copies(dev):
        src, dst = frows_of(ftiles - 1), frows_of(ftiles)
        return (
            remote(xv.at[src, :], xv.at[dst, :], t_send.at[0], t_recv.at[0], dev),
            remote(rv.at[src, :], rv.at[dst, :], t_send.at[1], t_recv.at[1], dev),
        )

    def d_u(m):
        slot = m % 2
        return remote(own_u.at[slot, :, 1 - core], in_u.at[slot], ds_sem.at[0, slot], dr_sem.at[0, slot], peer)

    def d_v(m):
        slot = m % 2
        return remote(own_v.at[slot, 1 - core], in_v.at[slot], ds_sem.at[1, slot], dr_sem.at[1, slot], peer)

    def forward(w1f, w2f, a_scr):
        width = ff // PARTS

        def w1_copy(part):
            cols = pl.ds(part * width, width)
            return pltpu.make_async_copy(wu_h.at[0, :, cols], w1f.at[:, cols], f_sem.at[part])

        w2_copy = pltpu.make_async_copy(wd_h.at[0], w2f, f_sem.at[PARTS])
        @pl.when(at_end)
        def _():
            x_copy(ftiles - 1).start()
            r_copy(ftiles - 1).start()

        for i in range(ftiles - 1):
            x_copy(i).start()
            if i == 0:
                for part in range(PARTS):
                    w1_copy(part).start()
                w2_copy.start()
                r_copy(0).start()
        for cp in w_copies(0):
            cp.start()
        for i in range(1, ftiles - 1):
            r_copy(i).start()

        @pl.when(~at_end)
        def _():
            x_copy(ftiles - 1).start()
            r_copy(ftiles - 1).start()

        own_v[0] = jnp.zeros(own_v.shape[1:], F32)
        peers = 1 + jnp.where(z > 0, 1, 0) + jnp.where(z < CHIPS - 1, 1, 0)
        pl.semaphore_wait(barrier, peers)

        @pl.when(at_end)
        def _():
            x_copy(ftiles - 1).wait()
            r_copy(ftiles - 1).wait()
            mask(ftiles - 1)
            for cp in tile_copies(inward):
                cp.start()

        def tile(i, first):
            @pl.when(i < ftiles)
            def _():
                x_copy(i).wait()
                r_copy(i).wait()
                mask(i)

            @pl.when(i == ftiles)
            def _():
                for cp in tile_copies(outward):
                    cp.wait_recv()
                x_extra[...] = xv[frows_of(i), :]

            x_val = xv[frows_of(i), :]
            for part in range(PARTS):
                cols = slice(part * width, (part + 1) * width)

                if first:
                    w1_copy(part).wait()
                h_val = dot(x_val, w1f[:, cols], ((1,), (0,))).astype(BF16).astype(F32)
                _, _, cdf = gelu_parts(h_val)
                a_scr[:, cols] = (h_val * cdf).astype(BF16)

            if first:
                w2_copy.wait()
            y_val = dot(a_scr[...], w2f[...], ((1,), (0,))).astype(BF16)
            x1_val = (x_val.astype(F32) + y_val.astype(F32)).astype(BF16)
            xv[frows_of(i), :] = x1_val
            if first:
                for cp in w_copies(0):
                    cp.wait()
            h_val = dot(x1_val, w1v[0], ((1,), (0,))).astype(BF16).astype(F32)
            _, _, cdf = gelu_parts(h_val)
            own_v[0] += dot((h_val * cdf).astype(BF16), rv[frows_of(i), :], ((0,), (0,))).reshape(own_v.shape[1:])

        def rest(i, carry):
            tile(i, False)
            return carry

        tile(0, True)
        lax.fori_loop(1, mine, rest, 0)
        d_v(0).start()

        @pl.when(at_end)
        def _():
            for cp in tile_copies(inward):
                cp.wait_send()

    pl.run_scoped(
        forward,
        pltpu.VMEM((dim, ff), BF16), pltpu.VMEM((ff, dim), BF16), pltpu.VMEM((fblock, ff), BF16))

    def backward(dxa):
        def clear(i, carry):
            dxa[frows_of(i), :] = jnp.zeros((fblock, dim), F32)
            return carry

        lax.fori_loop(0, mine, clear, 0)

        def tile(m, i, back, short=False):
            slot = m % 2
            v_slot = jnp.where(m == 0, 1, slot)
            rows = pl.ds(pl.multiple_of(i * block, block), fblock if short else block)

            @pl.when(m == per_layer)
            def _():
                if short:
                    @pl.when(at_end)
                    def _():
                        x_copy(2 * i).wait()

                    @pl.when(~at_end)
                    def _():
                        xv[rows, :] = x_extra[...]
                else:
                    x_copy(2 * i).wait()
                    x_copy(2 * i + 1).wait()
                rv[rows, :] = (rv[rows, :].astype(F32) + dxa[rows, :]).astype(BF16)

            x_i, r_i = xv[rows, :], rv[rows, :]
            h_val = dot(x_i, w1v[slot], ((1,), (0,))).astype(BF16).astype(F32)
            da_val = dot(r_i, w2v[slot], ((1,), (1,)))
            sq, th, cdf = gelu_parts(h_val)
            a_val = (h_val * cdf).astype(BF16)
            slope = cdf + (h_val * (0.5 - 0.5 * (th * th))) * (C1 + K3 * sq)
            dh_val = (da_val * slope).astype(BF16)
            own_v[v_slot] += dot(a_val, r_i, ((0,), (0,))).reshape(own_v.shape[1:])
            own_u[slot] += dot(x_i, dh_val, ((0,), (0,))).reshape(own_u.shape[1:])
            if back:
                dxa[rows, :] += dot(dh_val, w1v[slot], ((1,), (1,)))

        def far_first(zz, going):
            return list(range(CHIPS - 1, zz, -1)) if going > 0 else list(range(zz))

        def u_copy(m, blk, going, first):
            slot = m % SLOTS
            dst, ssem, qsem = (rr_u, rs_u, rq_u) if going > 0 else (rl_u, ls_u, lq_u)
            src = sum_u if first else dst
            return remote(src.at[slot, blk], dst.at[slot, blk], ssem.at[blk, slot], qsem.at[blk, slot], me + 2 * going)

        def v_copy(m, p, going, first):
            slot = m % SLOTS
            dst, ssem, qsem = (rr_v, rs_v, rq_v) if going > 0 else (rl_v, ls_v, lq_v)
            src = sum_v if first else dst
            part = pl.ds(p * piece, piece)
            return remote(src.at[slot, part], dst.at[slot, part], ssem.at[p, slot], qsem.at[p, slot], me + 2 * going)

        def beyond(m, zz, going):
            return owner_of(m) > zz if going > 0 else owner_of(m) < zz

        def ends(zz, going):
            start, stop = (0, CHIPS - 1) if going > 0 else (CHIPS - 1, 0)
            return zz == start, zz == stop

        def turn(zz, going):
            return zz if going > 0 else CHIPS - 1 - zz

        def keeps(zz, going):
            return 2 * turn(zz, going) < CHIPS - 1

        def flow(m, zz, going):
            slot = m % SLOTS
            first, last = ends(zz, going)
            keep = keeps(zz, going)
            got_u, credit_u = (rr_u, ru_credit) if going > 0 else (rl_u, lu_credit)
            got_v, credit_v = (rr_v, rv_credit) if going > 0 else (rl_v, lv_credit)

            if not last:
                @pl.when(m >= SLOTS)
                def _():
                    pl.semaphore_wait(credit_u, 1)

                @pl.when((m >= SLOTS) & beyond(m, zz, going))
                def _():
                    pl.semaphore_wait(credit_v, 1)

            def pass_u(blk):
                if not first:
                    u_copy(m, blk, going, False).wait_recv()
                    if blk != zz or keep:
                        got_u[slot, blk] += sum_u[slot, blk]
                if blk != zz:
                    u_copy(m, blk, going, first).start()

            blocks = far_first(zz, going) + ([] if first else [zz])
            pass_u(blocks[0])
            if not last:
                @pl.when(beyond(m, zz, going) & (m > 0) if first else beyond(m, zz, going))
                def _():
                    for p in range(PIECES):
                        if not first:
                            part = pl.ds(p * piece, piece)
                            v_copy(m, p, going, False).wait_recv()
                            got_v[slot, part] += sum_v[slot, part]
                        v_copy(m, p, going, first).start()

            if not first:
                @pl.when(owner_of(m) == zz)
                def _():
                    for p in range(PIECES):
                        v_copy(m, p, going, False).wait_recv()
                    if keep:
                        got_v[slot] += sum_v[slot]

            for blk in blocks[1:]:
                pass_u(blk)

        def out_copies_u(m):
            slot = m % 2
            return [
                pltpu.make_async_copy(out_u.at[slot, :, pl.ds(half * unit, unit)],
                                      gu_h.at[layer_of(m), :, pl.ds(start, unit)], ou_sem.at[slot, half])
                for half, start in enumerate(cols_of(m))
            ]

        def out_copy_v(m):
            start = pl.multiple_of(unit * ((m % per_layer) // CHIPS), unit)
            return pltpu.make_async_copy(out_v, gd_h.at[layer_of(m), pl.ds(start, unit), :], ov_sem)

        def terms(zz, total_ref, right_ref, left_ref):
            if zz == 0:
                return total_ref, left_ref
            if zz == CHIPS - 1:
                return total_ref, right_ref
            return right_ref, left_ref

        def finish(m, zz):
            slot = m % SLOTS

            @pl.when(m >= 2)
            def _():
                for cp in out_copies_u(m - 2):
                    cp.wait()

            one, two = terms(zz, sum_u, rr_u, rl_u)
            out_u[m % 2] = one[slot, zz] + two[slot, zz]
            for cp in out_copies_u(m):
                cp.start()

            @pl.when(owner_of(m) == zz)
            def _():
                @pl.when(m >= CHIPS)
                def _():
                    out_copy_v(m - CHIPS).wait()

                one, two = terms(zz, sum_v, rr_v, rl_v)
                out_v[...] = one[slot] + two[slot]
                out_copy_v(m).start()

            again = m < total - SLOTS
            for going in (1, -1):
                first, last = ends(zz, going)
                if not last:
                    for blk in far_first(zz, going):
                        u_copy(m, blk, going, first).wait_send()

                    @pl.when(beyond(m, zz, going))
                    def _():
                        for p in range(PIECES):
                            v_copy(m, p, going, first).wait_send()

                if not first:
                    @pl.when(again)
                    def _():
                        signal(ru_credit if going > 0 else lu_credit, me - 2 * going)

                    @pl.when(again & beyond(m, zz - going, going))
                    def _():
                        signal(rv_credit if going > 0 else lv_credit, me - 2 * going)

        def upto(k, n):
            late = n - total
            draining = jnp.where(late < k, total + 1 - HOP * (k - late), total)
            return jnp.maximum(jnp.where(n < total, n - HOP * k, draining), 0)

        def turns(k, n, body):
            def one(m, carry):
                body(m)
                return carry

            lax.fori_loop(upto(k, n - 1), upto(k, n), one, 0)

        def add_cores(m):
            d_u(m).wait_recv()
            sum_u[m % SLOTS] = own_u[m % 2, :, core] + in_u[m % 2]
            d_u(m).wait_send()

            @pl.when(m < total - 2)
            def _():
                signal(du_credit, peer)

            @pl.when(m > 0)
            def _():
                add_cores_v(m)

        def add_cores_v(m):
            d_v(m).wait_recv()
            sum_v[m % SLOTS] = own_v[m % 2, core] + in_v[m % 2]
            d_v(m).wait_send()

            @pl.when(m < total - 2)
            def _():
                signal(dv_credit, peer)

        def first_rows():
            add_cores_v(0)
            for zz, going in ((0, 1), (CHIPS - 1, -1)):
                @pl.when((z == zz) & beyond(0, zz, going))
                def _():
                    for p in range(PIECES):
                        v_copy(0, p, going, True).start()

        def all_sums(n):
            turns(0, n, add_cores)
            for zz in range(CHIPS):
                @pl.when(z == zz)
                def _():
                    near, far = sorted((1, -1), key=lambda going: turn(zz, going))

                    def go(going):
                        turns(turn(zz, going), n, lambda m: flow(m, zz, going))

                    if turn(zz, near) == 0:
                        go(near)
                        go(far)
                    else:
                        @pl.when(n < total)
                        def _():
                            go(near)

                        go(far)

                        @pl.when(n >= total)
                        def _():
                            go(near)

                    turns(CHIPS - 1, n, lambda m: finish(m, zz))

        def step(n, carry):
            run = n < total

            @pl.when(run)
            def _():
                @pl.when(n + 1 < total)
                def _():
                    for cp in w_copies(n + 1):
                        cp.start()

                @pl.when(n > 0)
                def _():
                    for cp in w_copies(n):
                        cp.wait()

                    own_v[n % 2] = jnp.zeros(own_v.shape[1:], F32)

                @pl.when(n == 0)
                def _():
                    own_v[1] = jnp.zeros(own_v.shape[1:], F32)

                own_u[n % 2] = jnp.zeros(own_u.shape[1:], F32)

                @pl.when(n == per_layer)
                def _():
                    for i in range(ftiles - 1):
                        x_copy(i).start()

                    @pl.when(~at_end)
                    def _():
                        x_copy(ftiles - 1).start()


            def half(phase, c):
                lo = phase
                hi = jnp.where(phase == 0, 1, full)

                def loop(cond, back):
                    @pl.when(cond)
                    def _():
                        def body(i, cc):
                            tile(n, i, back)
                            return cc

                        lax.fori_loop(lo, hi, body, 0)

                        @pl.when(phase == 1)
                        def _():
                            tile(n, full, back, True)

                loop(run & (n < per_layer), True)
                loop(run & (n >= per_layer), False)

                @pl.when(run & (phase == 1))
                def _():
                    @pl.when(n >= 2)
                    def _():
                        pl.semaphore_wait(du_credit, 1)
                        pl.semaphore_wait(dv_credit, 1)

                    d_u(n).start()

                    @pl.when(n > 0)
                    def _():
                        d_v(n).start()

                @pl.when((phase == 0) & (n == 0))
                def _():
                    first_rows()

                @pl.when((phase == 0) & (n > 0))
                def _():
                    all_sums(n)

                return c

            lax.fori_loop(0, 2, half, 0)
            return carry

        lax.fori_loop(0, total + CHIPS, step, 0)

        for m in (total - 2, total - 1):
            for cp in out_copies_u(m):
                cp.wait()
        out_copy_v(total - CHIPS).wait()

    pl.run_scoped(backward, pltpu.VMEM(xv.shape, F32))


def gradients(x0, g, lengths, w_up, w_down, block, fblock, unit):
    toks, dim = x0.shape
    micro = lengths.shape[0]
    layers, _, ff = w_up.shape
    rows_u = dim // (2 * CHIPS)
    wide = 2 * unit
    ftiles = toks // fblock
    held = toks + fblock
    dma = pltpu.SemaphoreType.DMA
    vm = pltpu.VMEM
    u_blk = (CHIPS, rows_u, wide)
    v_blk = (unit, dim)
    scratch = [
        vm((held, dim), BF16), vm((held, dim), BF16), vm((fblock, dim), BF16),
        vm((2, dim, wide), BF16), vm((2, wide, dim), BF16),
        vm((2, CHIPS, 2, rows_u, wide), F32), vm((2, 2) + v_blk, F32),
        vm((2,) + u_blk, F32), vm((2,) + v_blk, F32),
        vm((SLOTS,) + u_blk, F32), vm((SLOTS,) + v_blk, F32),
        vm((SLOTS,) + u_blk, F32), vm((SLOTS,) + v_blk, F32),
        vm((SLOTS,) + u_blk, F32), vm((SLOTS,) + v_blk, F32),
        vm((2, rows_u, wide), F32), vm(v_blk, F32),
        dma((ftiles,)), dma((ftiles,)), dma((2, 4)), dma((PARTS + 1,)), dma((2,)), dma((2,)), dma((2, 2)), dma((2, 2)),
    ] + [dma((CHIPS, SLOTS))] * 4 + [dma((PIECES, SLOTS))] * 4 + [dma((2, 2)), dma] + [pltpu.SemaphoreType.REGULAR] * 6
    any_space = pl.BlockSpec(memory_space=pl.ANY)
    return pl.pallas_call(
        functools.partial(kernel, unit, block, fblock, micro),
        out_shape=[
            jax.ShapeDtypeStruct((layers, rows_u, ff), F32),
            jax.ShapeDtypeStruct((layers, ff // (2 * CHIPS), dim), F32),
        ],
        in_specs=[pl.BlockSpec(memory_space=pltpu.SMEM)] + [any_space] * 4,
        out_specs=[any_space] * 2,
        scratch_shapes=scratch,
        compiler_params=pltpu.CompilerParams(
            collective_id=0, has_side_effects=True, vmem_limit_bytes=67_043_328),
        name="grads",
    )(lengths, x0, g, w_up, w_down)


def solution(mesh, block=1024, fblock=512, unit=128):
    def local_step(acts_in, cot_out, lengths, w_up, w_down):
        micro, tok_rows, dim = acts_in.shape
        x0 = acts_in.reshape(micro * tok_rows, dim)
        g = cot_out.reshape(micro * tok_rows, dim)
        return gradients(x0, g, lengths.reshape(micro), w_up, w_down, block, fblock, unit)

    act_spec = P(None, ("part", "fsdp"), None)
    grad_spec = P("part", "fsdp", None)
    return jax.shard_map(
        local_step, mesh=mesh,
        in_specs=(act_spec, act_spec, P(None, ("part", "fsdp")), P(), P()),
        out_specs=(grad_spec, grad_spec), check_vma=False)
```

```python
import functools

import jax
import jax.numpy as jnp
from jax import lax
from jax.experimental import pallas as pl
from jax.experimental.pallas import tpu as pltpu
from jax.sharding import PartitionSpec as P

MESH = pl.DeviceIdType.MESH
F32 = jnp.float32
BF16 = jnp.bfloat16

C1 = 0.7978845608028654
K1 = C1 * 0.044715
K3 = 3.0 * K1

CHIPS = 4
HOP = 2
SLOTS = 8
PIECES = 4
PARTS = 4


def dot(lhs, rhs, dims):
    return lax.dot_general(lhs, rhs, (dims, ((), ())), preferred_element_type=F32)


def gelu_parts(h_wide):
    sq = h_wide * h_wide
    th = jnp.tanh(h_wide * (C1 + K1 * sq))
    return sq, th, 0.5 + 0.5 * th


def kernel(unit, block, fblock, micro, len_s, x0_h, g_h, wu_h, wd_h, gu_h, gd_h,
           xv, rv, x_extra, w1v, w2v, own_u, own_v, in_u, in_v, sum_u, sum_v,
           rr_u, rr_v, rl_u, rl_v, out_u, out_v,
           x_sem, r_sem, w_sem, f_sem, t_send, t_recv, ds_sem, dr_sem,
           rs_u, rq_u, ls_u, lq_u, rs_v, rq_v, ls_v, lq_v,
           ou_sem, ov_sem, du_credit, dv_credit, ru_credit, lu_credit, rv_credit, lv_credit):
    toks, dim = x0_h.shape
    layers, _, ff = wu_h.shape
    ftiles = toks // fblock
    piece = unit // PIECES
    wide = 2 * unit
    per_dev = ff // (2 * CHIPS)
    per_layer = ff // wide
    total = layers * per_layer

    me = lax.axis_index("fsdp")
    z = me // 2
    core = me % 2
    peer = z * 2 + (1 - core)
    at_end = (z == 0) | (z == CHIPS - 1)
    inward = jnp.where(z < CHIPS // 2, me + 2, me - 2)
    outward = jnp.where(z < CHIPS // 2, me - 2, me + 2)
    mine = jnp.where(at_end, ftiles - 1, ftiles + 1)
    full = mine // 2

    def signal(sem, dev):
        pl.semaphore_signal(sem, inc=1, device_id={"fsdp": dev}, device_id_type=MESH)

    def remote(src, dst, ssem, rsem, dev):
        return pltpu.make_async_remote_copy(
            src_ref=src, dst_ref=dst, send_sem=ssem, recv_sem=rsem,
            device_id={"fsdp": dev}, device_id_type=MESH)

    barrier = pltpu.get_barrier_semaphore()
    signal(barrier, peer)

    @pl.when(z > 0)
    def _():
        signal(barrier, me - 2)

    @pl.when(z < CHIPS - 1)
    def _():
        signal(barrier, me + 2)

    def layer_of(m):
        return layers - 1 - m // per_layer

    def owner_of(m):
        return (1 + 3 * (m % per_layer)) % CHIPS

    def cols_of(m):
        base = 2 * per_dev * owner_of(m) + unit * ((m % per_layer) // CHIPS)
        return pl.multiple_of(base, unit), pl.multiple_of(base + per_dev, unit)

    def w_copies(m):
        slot = m % 2
        out = []
        for half, start in enumerate(cols_of(m)):
            span = pl.ds(start, unit)
            here = pl.ds(half * unit, unit)
            out.append(pltpu.make_async_copy(
                wu_h.at[layer_of(m), :, span], w1v.at[slot, :, here], w_sem.at[slot, half]))
            out.append(pltpu.make_async_copy(
                wd_h.at[layer_of(m), span, :], w2v.at[slot, here, :], w_sem.at[slot, 2 + half]))
        return out

    def frows_of(i):
        return pl.ds(pl.multiple_of(i * fblock, fblock), fblock)

    def x_copy(i):
        return pltpu.make_async_copy(x0_h.at[frows_of(i), :], xv.at[frows_of(i), :], x_sem.at[i])

    def r_copy(i):
        return pltpu.make_async_copy(g_h.at[frows_of(i), :], rv.at[frows_of(i), :], r_sem.at[i])

    def mask(i):
        per = ftiles // micro
        left = len_s[i // per] - (i % per) * fblock
        r_val = rv[frows_of(i), :]
        row_ids = lax.broadcasted_iota(jnp.int32, r_val.shape, 0)
        rv[frows_of(i), :] = jnp.where(row_ids < left, r_val, jnp.zeros_like(r_val))

    def tile_copies(dev):
        src, dst = frows_of(ftiles - 1), frows_of(ftiles)
        return (
            remote(xv.at[src, :], xv.at[dst, :], t_send.at[0], t_recv.at[0], dev),
            remote(rv.at[src, :], rv.at[dst, :], t_send.at[1], t_recv.at[1], dev),
        )

    def d_u(m):
        return remote(own_u.at[m % 2, :, 1 - core], in_u, ds_sem.at[0], dr_sem.at[0], peer)

    def d_v(m):
        return remote(own_v.at[m % 2, 1 - core], in_v, ds_sem.at[1], dr_sem.at[1], peer)

    def forward(w1f, w2f, a_scr):
        width = ff // PARTS

        def w1_copy(part):
            cols = pl.ds(part * width, width)
            return pltpu.make_async_copy(wu_h.at[0, :, cols], w1f.at[:, cols], f_sem.at[part])

        w2_copy = pltpu.make_async_copy(wd_h.at[0], w2f, f_sem.at[PARTS])
        @pl.when(at_end)
        def _():
            x_copy(ftiles - 1).start()
            r_copy(ftiles - 1).start()

        for i in range(ftiles - 1):
            x_copy(i).start()
            if i == 0:
                for part in range(PARTS):
                    w1_copy(part).start()
                w2_copy.start()
                r_copy(0).start()
        for cp in w_copies(0):
            cp.start()
        for i in range(1, ftiles - 1):
            r_copy(i).start()

        @pl.when(~at_end)
        def _():
            x_copy(ftiles - 1).start()
            r_copy(ftiles - 1).start()

        peers = 1 + jnp.where(z > 0, 1, 0) + jnp.where(z < CHIPS - 1, 1, 0)
        pl.semaphore_wait(barrier, peers)

        @pl.when(at_end)
        def _():
            x_copy(ftiles - 1).wait()
            r_copy(ftiles - 1).wait()
            mask(ftiles - 1)
            for cp in tile_copies(inward):
                cp.start()

        def tile(i, first):
            @pl.when(i < ftiles)
            def _():
                x_copy(i).wait()
                r_copy(i).wait()
                mask(i)

            @pl.when(i == ftiles)
            def _():
                for cp in tile_copies(outward):
                    cp.wait_recv()
                x_extra[...] = xv[frows_of(i), :]

            x_val = xv[frows_of(i), :]
            for part in range(PARTS):
                cols = slice(part * width, (part + 1) * width)

                if first:
                    w1_copy(part).wait()
                h_val = dot(x_val, w1f[:, cols], ((1,), (0,))).astype(BF16).astype(F32)
                _, _, cdf = gelu_parts(h_val)
                a_scr[:, cols] = (h_val * cdf).astype(BF16)

            if first:
                w2_copy.wait()
            y_val = dot(a_scr[...], w2f[...], ((1,), (0,))).astype(BF16)
            xv[frows_of(i), :] = (x_val.astype(F32) + y_val.astype(F32)).astype(BF16)

        def rest(i, carry):
            tile(i, False)
            return carry

        tile(0, True)
        lax.fori_loop(1, mine, rest, 0)

        @pl.when(at_end)
        def _():
            for cp in tile_copies(inward):
                cp.wait_send()

    pl.run_scoped(
        forward,
        pltpu.VMEM((dim, ff), BF16), pltpu.VMEM((ff, dim), BF16), pltpu.VMEM((fblock, ff), BF16))

    def backward(dxa):
        def clear(i, carry):
            dxa[frows_of(i), :] = jnp.zeros((fblock, dim), F32)
            return carry

        lax.fori_loop(0, mine, clear, 0)

        def tile(m, i, back, short=False):
            slot = m % 2
            rows = pl.ds(pl.multiple_of(i * block, block), fblock if short else block)

            @pl.when(m == per_layer)
            def _():
                if short:
                    @pl.when(at_end)
                    def _():
                        x_copy(2 * i).wait()

                    @pl.when(~at_end)
                    def _():
                        xv[rows, :] = x_extra[...]
                else:
                    x_copy(2 * i).wait()
                    x_copy(2 * i + 1).wait()
                rv[rows, :] = (rv[rows, :].astype(F32) + dxa[rows, :]).astype(BF16)

            x_i, r_i = xv[rows, :], rv[rows, :]
            da_val = dot(r_i, w2v[slot], ((1,), (1,)))
            h_val = dot(x_i, w1v[slot], ((1,), (0,))).astype(BF16).astype(F32)
            sq, th, cdf = gelu_parts(h_val)
            a_val = (h_val * cdf).astype(BF16)
            slope = cdf + (h_val * (0.5 - 0.5 * (th * th))) * (C1 + K3 * sq)
            dh_val = (da_val * slope).astype(BF16)
            if back:
                dxa[rows, :] += dot(dh_val, w1v[slot], ((1,), (1,)))
            own_u[slot] += dot(x_i, dh_val, ((0,), (0,))).reshape(own_u.shape[1:])
            own_v[slot] += dot(a_val, r_i, ((0,), (0,))).reshape(own_v.shape[1:])

        def far_first(zz, going):
            return list(range(CHIPS - 1, zz, -1)) if going > 0 else list(range(zz))

        def held(blk, going):
            return blk - 1 if going > 0 else blk

        def u_copy(m, blk, going, first):
            slot = m % SLOTS
            dst, ssem, qsem = (rr_u, rs_u, rq_u) if going > 0 else (rl_u, ls_u, lq_u)
            at = held(blk, going)
            src = sum_u.at[slot, blk] if first else dst.at[slot, at]
            return remote(src, dst.at[slot, at], ssem.at[blk, slot], qsem.at[blk, slot], me + 2 * going)

        def v_copy(m, p, going, first):
            slot = m % SLOTS
            dst, ssem, qsem = (rr_v, rs_v, rq_v) if going > 0 else (rl_v, ls_v, lq_v)
            src = sum_v if first else dst
            part = pl.ds(p * piece, piece)
            return remote(src.at[slot, part], dst.at[slot, part], ssem.at[p, slot], qsem.at[p, slot], me + 2 * going)

        def beyond(m, zz, going):
            return owner_of(m) > zz if going > 0 else owner_of(m) < zz

        def ends(zz, going):
            start, stop = (0, CHIPS - 1) if going > 0 else (CHIPS - 1, 0)
            return zz == start, zz == stop

        def turn(zz, going):
            return zz if going > 0 else CHIPS - 1 - zz

        def keeps(zz, going):
            return 2 * turn(zz, going) < CHIPS - 1

        def flow(m, zz, going):
            slot = m % SLOTS
            first, last = ends(zz, going)
            keep = keeps(zz, going)
            got_u, credit_u = (rr_u, ru_credit) if going > 0 else (rl_u, lu_credit)
            got_v, credit_v = (rr_v, rv_credit) if going > 0 else (rl_v, lv_credit)

            if not last:
                @pl.when(m >= SLOTS)
                def _():
                    pl.semaphore_wait(credit_u, 1)

                @pl.when((m >= SLOTS) & beyond(m, zz, going))
                def _():
                    pl.semaphore_wait(credit_v, 1)

            def pass_u(blk):
                if not first:
                    u_copy(m, blk, going, False).wait_recv()
                    if blk != zz or keep:
                        got_u[slot, held(blk, going)] += sum_u[slot, blk]
                if blk != zz:
                    u_copy(m, blk, going, first).start()

            blocks = far_first(zz, going) + ([] if first else [zz])
            pass_u(blocks[0])
            if not last:
                @pl.when(beyond(m, zz, going))
                def _():
                    for p in range(PIECES):
                        if not first:
                            part = pl.ds(p * piece, piece)
                            v_copy(m, p, going, False).wait_recv()
                            got_v[slot, part] += sum_v[slot, part]
                        v_copy(m, p, going, first).start()

            if not first:
                @pl.when(owner_of(m) == zz)
                def _():
                    for p in range(PIECES):
                        v_copy(m, p, going, False).wait_recv()
                    if keep:
                        got_v[slot] += sum_v[slot]

            for blk in blocks[1:]:
                pass_u(blk)

        def out_copies_u(m):
            slot = m % 2
            return [
                pltpu.make_async_copy(out_u.at[slot, :, pl.ds(half * unit, unit)],
                                      gu_h.at[layer_of(m), :, pl.ds(start, unit)], ou_sem.at[slot, half])
                for half, start in enumerate(cols_of(m))
            ]

        def out_copy_v(m):
            start = pl.multiple_of(unit * ((m % per_layer) // CHIPS), unit)
            return pltpu.make_async_copy(out_v, gd_h.at[layer_of(m), pl.ds(start, unit), :], ov_sem)

        def terms(zz, total_ref, right_ref, left_ref):
            if zz == 0:
                return total_ref, left_ref
            if zz == CHIPS - 1:
                return total_ref, right_ref
            return right_ref, left_ref

        def finish(m, zz):
            slot = m % SLOTS

            @pl.when(m >= 2)
            def _():
                for cp in out_copies_u(m - 2):
                    cp.wait()

            parts = [sum_u[slot, zz]] if zz in (0, CHIPS - 1) else []
            if zz > 0:
                parts.append(rr_u[slot, held(zz, 1)])
            if zz < CHIPS - 1:
                parts.append(rl_u[slot, held(zz, -1)])
            out_u[m % 2] = parts[0] + parts[1]
            for cp in out_copies_u(m):
                cp.start()

            @pl.when(owner_of(m) == zz)
            def _():
                @pl.when(m >= CHIPS)
                def _():
                    out_copy_v(m - CHIPS).wait()

                one, two = terms(zz, sum_v, rr_v, rl_v)
                out_v[...] = one[slot] + two[slot]
                out_copy_v(m).start()

            again = m < total - SLOTS
            for going in (1, -1):
                first, last = ends(zz, going)
                if not last:
                    for blk in far_first(zz, going):
                        u_copy(m, blk, going, first).wait_send()

                    @pl.when(beyond(m, zz, going))
                    def _():
                        for p in range(PIECES):
                            v_copy(m, p, going, first).wait_send()

                if not first:
                    @pl.when(again)
                    def _():
                        signal(ru_credit if going > 0 else lu_credit, me - 2 * going)

                    @pl.when(again & beyond(m, zz - going, going))
                    def _():
                        signal(rv_credit if going > 0 else lv_credit, me - 2 * going)

        def upto(k, n):
            late = n - total
            draining = jnp.where(late < k, total + 1 - HOP * (k - late), total)
            return jnp.maximum(jnp.where(n < total, n - HOP * k, draining), 0)

        def turns(k, n, body):
            def one(m, carry):
                body(m)
                return carry

            lax.fori_loop(upto(k, n - 1), upto(k, n), one, 0)

        def add_cores(m):
            d_u(m).wait_recv()
            sum_u[m % SLOTS] = own_u[m % 2, :, core] + in_u[...]
            d_u(m).wait_send()

            @pl.when(m < total - 1)
            def _():
                signal(du_credit, peer)

            d_v(m).wait_recv()
            sum_v[m % SLOTS] = own_v[m % 2, core] + in_v[...]
            d_v(m).wait_send()

            @pl.when(m < total - 1)
            def _():
                signal(dv_credit, peer)

        def all_sums(n):
            turns(0, n, add_cores)
            for zz in range(CHIPS):
                @pl.when(z == zz)
                def _():
                    near, far = sorted((1, -1), key=lambda going: turn(zz, going))

                    def go(going):
                        turns(turn(zz, going), n, lambda m: flow(m, zz, going))

                    if turn(zz, near) == 0:
                        go(near)
                        go(far)
                    else:
                        @pl.when(n < total)
                        def _():
                            go(near)

                        go(far)

                        @pl.when(n >= total)
                        def _():
                            go(near)

                    turns(CHIPS - 1, n, lambda m: finish(m, zz))

        def step(n, carry):
            run = n < total

            @pl.when(run)
            def _():
                @pl.when(n + 1 < total)
                def _():
                    for cp in w_copies(n + 1):
                        cp.start()

                for cp in w_copies(n):
                    cp.wait()

                own_v[n % 2] = jnp.zeros(own_v.shape[1:], F32)
                own_u[n % 2] = jnp.zeros(own_u.shape[1:], F32)

                @pl.when(n == per_layer)
                def _():
                    for i in range(ftiles - 1):
                        x_copy(i).start()

                    @pl.when(~at_end)
                    def _():
                        x_copy(ftiles - 1).start()


            def half(phase, c):
                lo = phase
                hi = jnp.where(phase == 0, 1, full)

                def loop(cond, back):
                    @pl.when(cond)
                    def _():
                        def body(i, cc):
                            tile(n, i, back)
                            return cc

                        lax.fori_loop(lo, hi, body, 0)

                        @pl.when(phase == 1)
                        def _():
                            tile(n, full, back, True)

                loop(run & (n < per_layer), True)
                loop(run & (n >= per_layer), False)

                @pl.when(run & (phase == 1))
                def _():
                    @pl.when(n >= 1)
                    def _():
                        pl.semaphore_wait(du_credit, 1)
                        pl.semaphore_wait(dv_credit, 1)

                    d_u(n).start()
                    d_v(n).start()

                @pl.when(phase == 0)
                def _():
                    all_sums(n)

                return c

            lax.fori_loop(0, 2, half, 0)
            return carry

        lax.fori_loop(0, total + CHIPS, step, 0)

        for m in (total - 2, total - 1):
            for cp in out_copies_u(m):
                cp.wait()
        out_copy_v(total - CHIPS).wait()

    pl.run_scoped(backward, pltpu.VMEM(xv.shape, F32))


def gradients(x0, g, lengths, w_up, w_down, block, fblock, unit):
    toks, dim = x0.shape
    micro = lengths.shape[0]
    layers, _, ff = w_up.shape
    rows_u = dim // (2 * CHIPS)
    wide = 2 * unit
    ftiles = toks // fblock
    held = toks + fblock
    dma = pltpu.SemaphoreType.DMA
    vm = pltpu.VMEM
    u_blk = (CHIPS, rows_u, wide)
    line_blk = (CHIPS - 1, rows_u, wide)
    v_blk = (unit, dim)
    scratch = [
        vm((held, dim), BF16), vm((held, dim), BF16), vm((fblock, dim), BF16),
        vm((2, dim, wide), BF16), vm((2, wide, dim), BF16),
        vm((2, CHIPS, 2, rows_u, wide), F32), vm((2, 2) + v_blk, F32),
        vm(u_blk, F32), vm(v_blk, F32),
        vm((SLOTS,) + u_blk, F32), vm((SLOTS,) + v_blk, F32),
        vm((SLOTS,) + line_blk, F32), vm((SLOTS,) + v_blk, F32),
        vm((SLOTS,) + line_blk, F32), vm((SLOTS,) + v_blk, F32),
        vm((2, rows_u, wide), F32), vm(v_blk, F32),
        dma((ftiles,)), dma((ftiles,)), dma((2, 4)), dma((PARTS + 1,)), dma((2,)), dma((2,)), dma((2,)), dma((2,)),
    ] + [dma((CHIPS, SLOTS))] * 4 + [dma((PIECES, SLOTS))] * 4 + [dma((2, 2)), dma] + [pltpu.SemaphoreType.REGULAR] * 6
    any_space = pl.BlockSpec(memory_space=pl.ANY)
    return pl.pallas_call(
        functools.partial(kernel, unit, block, fblock, micro),
        out_shape=[
            jax.ShapeDtypeStruct((layers, rows_u, ff), F32),
            jax.ShapeDtypeStruct((layers, ff // (2 * CHIPS), dim), F32),
        ],
        in_specs=[pl.BlockSpec(memory_space=pltpu.SMEM)] + [any_space] * 4,
        out_specs=[any_space] * 2,
        scratch_shapes=scratch,
        compiler_params=pltpu.CompilerParams(
            collective_id=0, has_side_effects=True, vmem_limit_bytes=67_043_328),
        name="grads",
    )(lengths, x0, g, w_up, w_down)


def hand_on_kernel(cuts, u_in, v_in, u_out, v_out, u_held, v_held, in_sem, out_sem):
    jobs = []
    for src, held, dst in ((v_in, v_held, v_out), (u_in, u_held, u_out)):
        rows = src.shape[1] // cuts
        for layer in range(src.shape[0]):
            for cut in range(cuts):
                part = pl.ds(cut * rows, rows)
                k = len(jobs)
                jobs.append((
                    pltpu.make_async_copy(src.at[layer, part], held.at[layer, part], in_sem.at[k]),
                    pltpu.make_async_copy(held.at[layer, part], dst.at[layer, part], out_sem.at[k])))
    for get, _ in jobs:
        get.start()
    for get, put in jobs:
        get.wait()
        put.start()
    for _, put in jobs:
        put.wait()


def hand_on(u, v, cuts=2):
    any_space = pl.BlockSpec(memory_space=pl.ANY)
    count = 2 * cuts * u.shape[0]
    return pl.pallas_call(
        functools.partial(hand_on_kernel, cuts),
        out_shape=[jax.ShapeDtypeStruct(u.shape, F32), jax.ShapeDtypeStruct(v.shape, F32)],
        in_specs=[any_space] * 2,
        out_specs=[any_space] * 2,
        scratch_shapes=[pltpu.VMEM(u.shape, F32), pltpu.VMEM(v.shape, F32),
                        pltpu.SemaphoreType.DMA((count,)), pltpu.SemaphoreType.DMA((count,))],
        compiler_params=pltpu.CompilerParams(vmem_limit_bytes=62 * 1024 * 1024),
        name="hand_on",
    )(u, v)


def solution(mesh, block=1024, fblock=512, unit=128):
    def local_step(acts_in, cot_out, lengths, w_up, w_down):
        micro, tok_rows, dim = acts_in.shape
        x0 = acts_in.reshape(micro * tok_rows, dim)
        g = cot_out.reshape(micro * tok_rows, dim)
        return tuple(hand_on(*gradients(x0, g, lengths.reshape(micro), w_up, w_down, block, fblock, unit)))

    act_spec = P(None, ("part", "fsdp"), None)
    grad_spec = P("part", "fsdp", None)
    return jax.shard_map(
        local_step, mesh=mesh,
        in_specs=(act_spec, act_spec, P(None, ("part", "fsdp")), P(), P()),
        out_specs=(grad_spec, grad_spec), check_vma=False)
```

```python
import functools

import jax
import jax.numpy as jnp
from jax import lax
from jax.experimental import pallas as pl
from jax.experimental.pallas import tpu as pltpu
from jax.sharding import PartitionSpec as P

MESH = pl.DeviceIdType.MESH
F32 = jnp.float32
BF16 = jnp.bfloat16

C1 = 0.7978845608028654
K1 = C1 * 0.044715
K3 = 3.0 * K1

CHIPS = 4
HOP = 2
SLOTS = 8
PIECES = 4
PARTS = 4


def dot(lhs, rhs, dims):
    return lax.dot_general(lhs, rhs, (dims, ((), ())), preferred_element_type=F32)


def gelu_parts(h_wide):
    sq = h_wide * h_wide
    th = jnp.tanh(h_wide * (C1 + K1 * sq))
    return sq, th, 0.5 + 0.5 * th


def kernel(unit, block, fblock, micro, len_s, x0_h, g_h, wu_h, wd_h, gu_h, gd_h,
           xv, rv, w1v, w2v, own_u, own_v, in_u, in_v, sum_u, sum_v,
           rr_u, rr_v, rl_u, rl_v, out_u, out_v,
           x_sem, r_sem, w_sem, f_sem, t_send, t_recv, ds_sem, dr_sem,
           rs_u, rq_u, ls_u, lq_u, rs_v, rq_v, ls_v, lq_v,
           ou_sem, ov_sem, du_credit, dv_credit, ru_credit, lu_credit, rv_credit, lv_credit):
    toks, dim = x0_h.shape
    layers, _, ff = wu_h.shape
    tiles = toks // block
    ftiles = toks // fblock
    piece = unit // PIECES
    wide = 2 * unit
    per_dev = ff // (2 * CHIPS)
    per_layer = ff // wide
    total = layers * per_layer

    me = lax.axis_index("fsdp")
    z = me // 2
    core = me % 2
    peer = z * 2 + (1 - core)
    at_end = (z == 0) | (z == CHIPS - 1)
    inward = jnp.where(z < CHIPS // 2, me + 2, me - 2)
    outward = jnp.where(z < CHIPS // 2, me - 2, me + 2)
    mine = jnp.where(at_end, ftiles - 1, ftiles + 1)
    guest_turn = ftiles // 2

    def signal(sem, dev):
        pl.semaphore_signal(sem, inc=1, device_id={"fsdp": dev}, device_id_type=MESH)

    def remote(src, dst, ssem, rsem, dev):
        return pltpu.make_async_remote_copy(
            src_ref=src, dst_ref=dst, send_sem=ssem, recv_sem=rsem,
            device_id={"fsdp": dev}, device_id_type=MESH)

    barrier = pltpu.get_barrier_semaphore()
    signal(barrier, peer)

    @pl.when(z > 0)
    def _():
        signal(barrier, me - 2)

    @pl.when(z < CHIPS - 1)
    def _():
        signal(barrier, me + 2)

    def layer_of(m):
        return layers - 1 - m // per_layer

    def owner_of(m):
        return (1 + 3 * (m % per_layer)) % CHIPS

    def cols_of(m):
        base = 2 * per_dev * owner_of(m) + unit * ((m % per_layer) // CHIPS)
        return pl.multiple_of(base, unit), pl.multiple_of(base + per_dev, unit)

    def w_copies(m):
        slot = m % 2
        out = []
        for half, start in enumerate(cols_of(m)):
            span = pl.ds(start, unit)
            here = pl.ds(half * unit, unit)
            out.append(pltpu.make_async_copy(
                wu_h.at[layer_of(m), :, span], w1v.at[slot, :, here], w_sem.at[slot, half]))
            out.append(pltpu.make_async_copy(
                wd_h.at[layer_of(m), span, :], w2v.at[slot, here, :], w_sem.at[slot, 2 + half]))
        return out

    def frows_of(i):
        return pl.ds(pl.multiple_of(i * fblock, fblock), fblock)

    def x_copy(i):
        return pltpu.make_async_copy(x0_h.at[frows_of(i), :], xv.at[frows_of(i), :], x_sem.at[i])

    def r_copy(i):
        return pltpu.make_async_copy(g_h.at[frows_of(i), :], rv.at[frows_of(i), :], r_sem.at[i])

    def mask(i):
        per = ftiles // micro
        left = len_s[i // per] - (i % per) * fblock
        r_val = rv[frows_of(i), :]
        row_ids = lax.broadcasted_iota(jnp.int32, r_val.shape, 0)
        rv[frows_of(i), :] = jnp.where(row_ids < left, r_val, jnp.zeros_like(r_val))

    def guest_there(dev):
        return remote(xv.at[frows_of(ftiles - 1), :], xv.at[frows_of(ftiles), :], t_send.at[0], t_recv.at[0], dev)

    def guest_back(dev):
        rows = frows_of(ftiles)
        return remote(xv.at[rows, :], xv.at[rows, :], t_send.at[1], t_recv.at[1], dev)

    def d_u(m):
        return remote(own_u.at[m % 2, :, 1 - core], in_u, ds_sem.at[0], dr_sem.at[0], peer)

    def d_v(m):
        return remote(own_v.at[m % 2, 1 - core], in_v, ds_sem.at[1], dr_sem.at[1], peer)

    def forward(w1f, w2f, a_scr):
        width = ff // PARTS

        def w1_copy(part):
            cols = pl.ds(part * width, width)
            return pltpu.make_async_copy(wu_h.at[0, :, cols], w1f.at[:, cols], f_sem.at[part])

        w2_copy = pltpu.make_async_copy(wd_h.at[0], w2f, f_sem.at[PARTS])
        @pl.when(at_end)
        def _():
            x_copy(ftiles - 1).start()

        for i in range(ftiles):
            if i < ftiles - 1:
                x_copy(i).start()
            if i == 0:
                for part in range(PARTS):
                    w1_copy(part).start()
                w2_copy.start()
            r_copy(i).start()

        @pl.when(~at_end)
        def _():
            x_copy(ftiles - 1).start()

        for cp in w_copies(0):
            cp.start()
        peers = 1 + jnp.where(z > 0, 1, 0) + jnp.where(z < CHIPS - 1, 1, 0)
        pl.semaphore_wait(barrier, peers)

        @pl.when(at_end)
        def _():
            x_copy(ftiles - 1).wait()
            guest_there(inward).start()

        def tile(turn, first):
            guest = ~at_end & (turn == guest_turn)
            i = jnp.where(guest, ftiles, jnp.where(~at_end & (turn > guest_turn), turn - 1, turn))

            @pl.when(guest)
            def _():
                guest_there(outward).wait_recv()

            @pl.when(~guest)
            def _():
                x_copy(i).wait()
                r_copy(i).wait()
                mask(i)

            x_val = xv[frows_of(i), :]
            for part in range(PARTS):
                cols = slice(part * width, (part + 1) * width)

                if first:
                    w1_copy(part).wait()
                h_val = dot(x_val, w1f[:, cols], ((1,), (0,))).astype(BF16).astype(F32)
                _, _, cdf = gelu_parts(h_val)
                a_scr[:, cols] = (h_val * cdf).astype(BF16)

            if first:
                w2_copy.wait()
            y_val = dot(a_scr[...], w2f[...], ((1,), (0,))).astype(BF16)
            xv[frows_of(i), :] = (x_val.astype(F32) + y_val.astype(F32)).astype(BF16)

            @pl.when(guest)
            def _():
                guest_back(outward).start()

        def rest(turn, carry):
            tile(turn, False)
            return carry

        tile(0, True)
        lax.fori_loop(1, mine, rest, 0)

        @pl.when(at_end)
        def _():
            guest_there(inward).wait_send()
            r_copy(ftiles - 1).wait()
            mask(ftiles - 1)

        @pl.when(~at_end)
        def _():
            guest_back(outward).wait_send()

    pl.run_scoped(
        forward,
        pltpu.VMEM((dim, ff), BF16), pltpu.VMEM((ff, dim), BF16), pltpu.VMEM((fblock, ff), BF16))

    def backward(dxa):
        def clear(i, carry):
            dxa[frows_of(i), :] = jnp.zeros((fblock, dim), F32)
            return carry

        lax.fori_loop(0, ftiles, clear, 0)

        def tile(m, i, back):
            slot = m % 2
            rows = pl.ds(pl.multiple_of(i * block, block), block)

            if back:
                @pl.when((m == 0) & (i == tiles - 1) & at_end)
                def _():
                    guest_back(inward).wait_recv()
                    xv[frows_of(ftiles - 1), :] = xv[frows_of(ftiles), :]

            @pl.when(m == per_layer)
            def _():
                for k in range(block // fblock):
                    x_copy(i * (block // fblock) + k).wait()

                rv[rows, :] = (rv[rows, :].astype(F32) + dxa[rows, :]).astype(BF16)

            x_i, r_i = xv[rows, :], rv[rows, :]
            da_val = dot(r_i, w2v[slot], ((1,), (1,)))
            h_val = dot(x_i, w1v[slot], ((1,), (0,))).astype(BF16).astype(F32)
            sq, th, cdf = gelu_parts(h_val)
            a_val = (h_val * cdf).astype(BF16)
            slope = cdf + (h_val * (0.5 - 0.5 * (th * th))) * (C1 + K3 * sq)
            dh_val = (da_val * slope).astype(BF16)
            if back:
                dxa[rows, :] += dot(dh_val, w1v[slot], ((1,), (1,)))
            own_u[slot] += dot(x_i, dh_val, ((0,), (0,))).reshape(own_u.shape[1:])
            own_v[slot] += dot(a_val, r_i, ((0,), (0,))).reshape(own_v.shape[1:])

        def far_first(zz, going):
            return list(range(CHIPS - 1, zz, -1)) if going > 0 else list(range(zz))

        def held(blk, going):
            return blk - 1 if going > 0 else blk

        def u_copy(m, blk, going, first):
            slot = m % SLOTS
            dst, ssem, qsem = (rr_u, rs_u, rq_u) if going > 0 else (rl_u, ls_u, lq_u)
            at = held(blk, going)
            src = sum_u.at[slot, blk] if first else dst.at[slot, at]
            return remote(src, dst.at[slot, at], ssem.at[blk, slot], qsem.at[blk, slot], me + 2 * going)

        def v_copy(m, p, going, first):
            slot = m % SLOTS
            dst, ssem, qsem = (rr_v, rs_v, rq_v) if going > 0 else (rl_v, ls_v, lq_v)
            src = sum_v if first else dst
            part = pl.ds(p * piece, piece)
            return remote(src.at[slot, part], dst.at[slot, part], ssem.at[p, slot], qsem.at[p, slot], me + 2 * going)

        def beyond(m, zz, going):
            return owner_of(m) > zz if going > 0 else owner_of(m) < zz

        def ends(zz, going):
            start, stop = (0, CHIPS - 1) if going > 0 else (CHIPS - 1, 0)
            return zz == start, zz == stop

        def turn(zz, going):
            return zz if going > 0 else CHIPS - 1 - zz

        def keeps(zz, going):
            return 2 * turn(zz, going) < CHIPS - 1

        def flow(m, zz, going):
            slot = m % SLOTS
            first, last = ends(zz, going)
            keep = keeps(zz, going)
            got_u, credit_u = (rr_u, ru_credit) if going > 0 else (rl_u, lu_credit)
            got_v, credit_v = (rr_v, rv_credit) if going > 0 else (rl_v, lv_credit)

            if not last:
                @pl.when(m >= SLOTS)
                def _():
                    pl.semaphore_wait(credit_u, 1)

                @pl.when((m >= SLOTS) & beyond(m, zz, going))
                def _():
                    pl.semaphore_wait(credit_v, 1)

            def pass_u(blk):
                if not first:
                    u_copy(m, blk, going, False).wait_recv()
                    if blk != zz or keep:
                        got_u[slot, held(blk, going)] += sum_u[slot, blk]
                if blk != zz:
                    u_copy(m, blk, going, first).start()

            blocks = far_first(zz, going) + ([] if first else [zz])
            pass_u(blocks[0])
            if not last:
                @pl.when(beyond(m, zz, going))
                def _():
                    for p in range(PIECES):
                        if not first:
                            part = pl.ds(p * piece, piece)
                            v_copy(m, p, going, False).wait_recv()
                            got_v[slot, part] += sum_v[slot, part]
                        v_copy(m, p, going, first).start()

            if not first:
                @pl.when(owner_of(m) == zz)
                def _():
                    for p in range(PIECES):
                        v_copy(m, p, going, False).wait_recv()
                    if keep:
                        got_v[slot] += sum_v[slot]

            for blk in blocks[1:]:
                pass_u(blk)

        def out_copies_u(m):
            slot = m % 2
            return [
                pltpu.make_async_copy(out_u.at[slot, :, pl.ds(half * unit, unit)],
                                      gu_h.at[layer_of(m), :, pl.ds(start, unit)], ou_sem.at[slot, half])
                for half, start in enumerate(cols_of(m))
            ]

        def out_copy_v(m):
            start = pl.multiple_of(unit * ((m % per_layer) // CHIPS), unit)
            return pltpu.make_async_copy(out_v, gd_h.at[layer_of(m), pl.ds(start, unit), :], ov_sem)

        def terms(zz, total_ref, right_ref, left_ref):
            if zz == 0:
                return total_ref, left_ref
            if zz == CHIPS - 1:
                return total_ref, right_ref
            return right_ref, left_ref

        def finish(m, zz):
            slot = m % SLOTS

            @pl.when(m >= 2)
            def _():
                for cp in out_copies_u(m - 2):
                    cp.wait()

            parts = [sum_u[slot, zz]] if zz in (0, CHIPS - 1) else []
            if zz > 0:
                parts.append(rr_u[slot, held(zz, 1)])
            if zz < CHIPS - 1:
                parts.append(rl_u[slot, held(zz, -1)])
            out_u[m % 2] = parts[0] + parts[1]
            for cp in out_copies_u(m):
                cp.start()

            @pl.when(owner_of(m) == zz)
            def _():
                @pl.when(m >= CHIPS)
                def _():
                    out_copy_v(m - CHIPS).wait()

                one, two = terms(zz, sum_v, rr_v, rl_v)
                out_v[...] = one[slot] + two[slot]
                out_copy_v(m).start()

            again = m < total - SLOTS
            for going in (1, -1):
                first, last = ends(zz, going)
                if not last:
                    for blk in far_first(zz, going):
                        u_copy(m, blk, going, first).wait_send()

                    @pl.when(beyond(m, zz, going))
                    def _():
                        for p in range(PIECES):
                            v_copy(m, p, going, first).wait_send()

                if not first:
                    @pl.when(again)
                    def _():
                        signal(ru_credit if going > 0 else lu_credit, me - 2 * going)

                    @pl.when(again & beyond(m, zz - going, going))
                    def _():
                        signal(rv_credit if going > 0 else lv_credit, me - 2 * going)

        def upto(k, n):
            late = n - total
            draining = jnp.where(late < k, total + 1 - HOP * (k - late), total)
            return jnp.maximum(jnp.where(n < total, n - HOP * k, draining), 0)

        def turns(k, n, body):
            def one(m, carry):
                body(m)
                return carry

            lax.fori_loop(upto(k, n - 1), upto(k, n), one, 0)

        def add_cores(m):
            d_u(m).wait_recv()
            sum_u[m % SLOTS] = own_u[m % 2, :, core] + in_u[...]
            d_u(m).wait_send()

            @pl.when(m < total - 1)
            def _():
                signal(du_credit, peer)

            d_v(m).wait_recv()
            sum_v[m % SLOTS] = own_v[m % 2, core] + in_v[...]
            d_v(m).wait_send()

            @pl.when(m < total - 1)
            def _():
                signal(dv_credit, peer)

        def all_sums(n):
            turns(0, n, add_cores)
            for zz in range(CHIPS):
                @pl.when(z == zz)
                def _():
                    near, far = sorted((1, -1), key=lambda going: turn(zz, going))

                    def go(going):
                        turns(turn(zz, going), n, lambda m: flow(m, zz, going))

                    if turn(zz, near) == 0:
                        go(near)
                        go(far)
                    else:
                        @pl.when(n < total)
                        def _():
                            go(near)

                        go(far)

                        @pl.when(n >= total)
                        def _():
                            go(near)

                    turns(CHIPS - 1, n, lambda m: finish(m, zz))

        def step(n, carry):
            run = n < total

            @pl.when(run)
            def _():
                @pl.when(n + 1 < total)
                def _():
                    for cp in w_copies(n + 1):
                        cp.start()

                for cp in w_copies(n):
                    cp.wait()

                own_v[n % 2] = jnp.zeros(own_v.shape[1:], F32)
                own_u[n % 2] = jnp.zeros(own_u.shape[1:], F32)

                @pl.when(n == per_layer)
                def _():
                    for i in range(ftiles):
                        x_copy(i).start()


            def half(phase, c):
                lo = phase
                hi = jnp.where(phase == 0, 1, tiles)

                def loop(cond, back):
                    @pl.when(cond)
                    def _():
                        def body(i, cc):
                            tile(n, i, back)
                            return cc

                        lax.fori_loop(lo, hi, body, 0)

                loop(run & (n < per_layer), True)
                loop(run & (n >= per_layer), False)

                @pl.when(run & (phase == 1))
                def _():
                    @pl.when(n >= 1)
                    def _():
                        pl.semaphore_wait(du_credit, 1)
                        pl.semaphore_wait(dv_credit, 1)

                    d_u(n).start()
                    d_v(n).start()

                @pl.when(phase == 0)
                def _():
                    all_sums(n)

                return c

            lax.fori_loop(0, 2, half, 0)
            return carry

        lax.fori_loop(0, total + CHIPS, step, 0)

        for m in (total - 2, total - 1):
            for cp in out_copies_u(m):
                cp.wait()
        out_copy_v(total - CHIPS).wait()

    pl.run_scoped(backward, pltpu.VMEM(rv.shape, F32))


def gradients(x0, g, lengths, w_up, w_down, block, fblock, unit):
    toks, dim = x0.shape
    micro = lengths.shape[0]
    layers, _, ff = w_up.shape
    rows_u = dim // (2 * CHIPS)
    wide = 2 * unit
    ftiles = toks // fblock
    held = toks + fblock
    dma = pltpu.SemaphoreType.DMA
    vm = pltpu.VMEM
    u_blk = (CHIPS, rows_u, wide)
    line_blk = (CHIPS - 1, rows_u, wide)
    v_blk = (unit, dim)
    scratch = [
        vm((held, dim), BF16), vm((toks, dim), BF16),
        vm((2, dim, wide), BF16), vm((2, wide, dim), BF16),
        vm((2, CHIPS, 2, rows_u, wide), F32), vm((2, 2) + v_blk, F32),
        vm(u_blk, F32), vm(v_blk, F32),
        vm((SLOTS,) + u_blk, F32), vm((SLOTS,) + v_blk, F32),
        vm((SLOTS,) + line_blk, F32), vm((SLOTS,) + v_blk, F32),
        vm((SLOTS,) + line_blk, F32), vm((SLOTS,) + v_blk, F32),
        vm((2, rows_u, wide), F32), vm(v_blk, F32),
        dma((ftiles,)), dma((ftiles,)), dma((2, 4)), dma((PARTS + 1,)), dma((2,)), dma((2,)), dma((2,)), dma((2,)),
    ] + [dma((CHIPS, SLOTS))] * 4 + [dma((PIECES, SLOTS))] * 4 + [dma((2, 2)), dma] + [pltpu.SemaphoreType.REGULAR] * 6
    any_space = pl.BlockSpec(memory_space=pl.ANY)
    return pl.pallas_call(
        functools.partial(kernel, unit, block, fblock, micro),
        out_shape=[
            jax.ShapeDtypeStruct((layers, rows_u, ff), F32),
            jax.ShapeDtypeStruct((layers, ff // (2 * CHIPS), dim), F32),
        ],
        in_specs=[pl.BlockSpec(memory_space=pltpu.SMEM)] + [any_space] * 4,
        out_specs=[any_space] * 2,
        scratch_shapes=scratch,
        compiler_params=pltpu.CompilerParams(
            collective_id=0, has_side_effects=True, vmem_limit_bytes=67_043_328),
        name="grads",
    )(lengths, x0, g, w_up, w_down)


def hand_on_kernel(cuts, u_in, v_in, u_out, v_out, u_held, v_held, in_sem, out_sem):
    jobs = []
    for src, held, dst in ((v_in, v_held, v_out), (u_in, u_held, u_out)):
        rows = src.shape[1] // cuts
        for layer in range(src.shape[0]):
            for cut in range(cuts):
                part = pl.ds(cut * rows, rows)
                k = len(jobs)
                jobs.append((
                    pltpu.make_async_copy(src.at[layer, part], held.at[layer, part], in_sem.at[k]),
                    pltpu.make_async_copy(held.at[layer, part], dst.at[layer, part], out_sem.at[k])))
    for get, _ in jobs:
        get.start()
    for get, put in jobs:
        get.wait()
        put.start()
    for _, put in jobs:
        put.wait()


def hand_on(u, v, cuts=2):
    any_space = pl.BlockSpec(memory_space=pl.ANY)
    count = 2 * cuts * u.shape[0]
    return pl.pallas_call(
        functools.partial(hand_on_kernel, cuts),
        out_shape=[jax.ShapeDtypeStruct(u.shape, F32), jax.ShapeDtypeStruct(v.shape, F32)],
        in_specs=[any_space] * 2,
        out_specs=[any_space] * 2,
        scratch_shapes=[pltpu.VMEM(u.shape, F32), pltpu.VMEM(v.shape, F32),
                        pltpu.SemaphoreType.DMA((count,)), pltpu.SemaphoreType.DMA((count,))],
        compiler_params=pltpu.CompilerParams(vmem_limit_bytes=62 * 1024 * 1024),
        name="hand_on",
    )(u, v)


def solution(mesh, block=1024, fblock=512, unit=128):
    def local_step(acts_in, cot_out, lengths, w_up, w_down):
        micro, tok_rows, dim = acts_in.shape
        x0 = acts_in.reshape(micro * tok_rows, dim)
        g = cot_out.reshape(micro * tok_rows, dim)
        return tuple(hand_on(*gradients(x0, g, lengths.reshape(micro), w_up, w_down, block, fblock, unit)))

    act_spec = P(None, ("part", "fsdp"), None)
    grad_spec = P("part", "fsdp", None)
    return jax.shard_map(
        local_step, mesh=mesh,
        in_specs=(act_spec, act_spec, P(None, ("part", "fsdp")), P(), P()),
        out_specs=(grad_spec, grad_spec), check_vma=False)
```

```python
import functools

import jax
import jax.numpy as jnp
from jax import lax
from jax.experimental import pallas as pl
from jax.experimental.pallas import tpu as pltpu
from jax.sharding import PartitionSpec as P

MESH = pl.DeviceIdType.MESH
F32 = jnp.float32
BF16 = jnp.bfloat16

C1 = 0.7978845608028654
K1 = C1 * 0.044715
K3 = 3.0 * K1

CHIPS = 4
HOP = 2
SLOTS = 8
CUTS = 4
PIECES = 4
PARTS = 4


def dot(lhs, rhs, dims):
    return lax.dot_general(lhs, rhs, (dims, ((), ())), preferred_element_type=F32)


def gelu_parts(h_wide):
    sq = h_wide * h_wide
    th = jnp.tanh(h_wide * (C1 + K1 * sq))
    return sq, th, 0.5 + 0.5 * th


def kernel(unit, block, fblock, micro, len_s, x0_h, g_h, wu_h, wd_h, gu_h, gd_h,
           xv, rv, w1v, w2v, own_u, own_v, in_u, in_v, sum_u, sum_v,
           rr_u, rr_v, rl_u, rl_v, out_u, out_v,
           x_sem, r_sem, w_sem, f_sem, t_send, t_recv, ds_sem, dr_sem,
           rs_u, rq_u, ls_u, lq_u, rs_v, rq_v, ls_v, lq_v,
           ou_sem, ov_sem, du_credit, dv_credit, ru_credit, lu_credit, rv_credit, lv_credit):
    toks, dim = x0_h.shape
    layers, _, ff = wu_h.shape
    tiles = toks // block
    ftiles = toks // fblock
    piece = unit // PIECES
    wide = 2 * unit
    per_dev = ff // (2 * CHIPS)
    per_layer = ff // wide
    total = layers * per_layer

    me = lax.axis_index("fsdp")
    z = me // 2
    core = me % 2
    peer = z * 2 + (1 - core)
    at_end = (z == 0) | (z == CHIPS - 1)
    inward = jnp.where(z < CHIPS // 2, me + 2, me - 2)
    outward = jnp.where(z < CHIPS // 2, me - 2, me + 2)
    mine = jnp.where(at_end, ftiles - 1, ftiles + 1)
    guest_turn = ftiles // 2

    def signal(sem, dev):
        pl.semaphore_signal(sem, inc=1, device_id={"fsdp": dev}, device_id_type=MESH)

    def remote(src, dst, ssem, rsem, dev):
        return pltpu.make_async_remote_copy(
            src_ref=src, dst_ref=dst, send_sem=ssem, recv_sem=rsem,
            device_id={"fsdp": dev}, device_id_type=MESH)

    barrier = pltpu.get_barrier_semaphore()
    signal(barrier, peer)

    @pl.when(z > 0)
    def _():
        signal(barrier, me - 2)

    @pl.when(z < CHIPS - 1)
    def _():
        signal(barrier, me + 2)

    def layer_of(m):
        return layers - 1 - m // per_layer

    def owner_of(m):
        return (1 + 3 * (m % per_layer)) % CHIPS

    def cols_of(m):
        base = 2 * per_dev * owner_of(m) + unit * ((m % per_layer) // CHIPS)
        return pl.multiple_of(base, unit), pl.multiple_of(base + per_dev, unit)

    def w_copies(m):
        slot = m % 2
        out = []
        for half, start in enumerate(cols_of(m)):
            span = pl.ds(start, unit)
            here = pl.ds(half * unit, unit)
            out.append(pltpu.make_async_copy(
                wu_h.at[layer_of(m), :, span], w1v.at[slot, :, here], w_sem.at[slot, half]))
            out.append(pltpu.make_async_copy(
                wd_h.at[layer_of(m), span, :], w2v.at[slot, here, :], w_sem.at[slot, 2 + half]))
        return out

    def frows_of(i):
        return pl.ds(pl.multiple_of(i * fblock, fblock), fblock)

    def x_copy(i):
        return pltpu.make_async_copy(x0_h.at[frows_of(i), :], xv.at[frows_of(i), :], x_sem.at[i])

    def r_copy(i):
        return pltpu.make_async_copy(g_h.at[frows_of(i), :], rv.at[frows_of(i), :], r_sem.at[i])

    def mask(i):
        per = ftiles // micro
        left = len_s[i // per] - (i % per) * fblock
        r_val = rv[frows_of(i), :]
        row_ids = lax.broadcasted_iota(jnp.int32, r_val.shape, 0)
        rv[frows_of(i), :] = jnp.where(row_ids < left, r_val, jnp.zeros_like(r_val))

    def guest_there(dev):
        return remote(xv.at[frows_of(ftiles - 1), :], xv.at[frows_of(ftiles), :], t_send.at[0], t_recv.at[0], dev)

    def guest_back(dev):
        rows = frows_of(ftiles)
        return remote(xv.at[rows, :], xv.at[rows, :], t_send.at[1], t_recv.at[1], dev)

    def d_u(m):
        return remote(own_u.at[m % 2, :, 1 - core], in_u, ds_sem.at[0], dr_sem.at[0], peer)

    def d_v(m):
        return remote(own_v.at[m % 2, 1 - core], in_v, ds_sem.at[1], dr_sem.at[1], peer)

    def forward(w1f, w2f, a_scr):
        width = ff // PARTS

        def w1_copy(part):
            cols = pl.ds(part * width, width)
            return pltpu.make_async_copy(wu_h.at[0, :, cols], w1f.at[:, cols], f_sem.at[part])

        w2_copy = pltpu.make_async_copy(wd_h.at[0], w2f, f_sem.at[PARTS])
        @pl.when(at_end)
        def _():
            x_copy(ftiles - 1).start()

        for i in range(ftiles):
            if i < ftiles - 1:
                x_copy(i).start()
            if i == 0:
                for part in range(PARTS):
                    w1_copy(part).start()
                w2_copy.start()
            r_copy(i).start()

        @pl.when(~at_end)
        def _():
            x_copy(ftiles - 1).start()

        for cp in w_copies(0):
            cp.start()
        peers = 1 + jnp.where(z > 0, 1, 0) + jnp.where(z < CHIPS - 1, 1, 0)
        pl.semaphore_wait(barrier, peers)

        @pl.when(at_end)
        def _():
            x_copy(ftiles - 1).wait()
            guest_there(inward).start()

        def tile(turn, first):
            guest = ~at_end & (turn == guest_turn)
            i = jnp.where(guest, ftiles, jnp.where(~at_end & (turn > guest_turn), turn - 1, turn))

            @pl.when(guest)
            def _():
                guest_there(outward).wait_recv()

            @pl.when(~guest)
            def _():
                x_copy(i).wait()
                r_copy(i).wait()
                mask(i)

            x_val = xv[frows_of(i), :]
            for part in range(PARTS):
                cols = slice(part * width, (part + 1) * width)

                if first:
                    w1_copy(part).wait()
                h_val = dot(x_val, w1f[:, cols], ((1,), (0,))).astype(BF16).astype(F32)
                _, _, cdf = gelu_parts(h_val)
                a_scr[:, cols] = (h_val * cdf).astype(BF16)

            if first:
                w2_copy.wait()
            y_val = dot(a_scr[...], w2f[...], ((1,), (0,))).astype(BF16)
            xv[frows_of(i), :] = (x_val.astype(F32) + y_val.astype(F32)).astype(BF16)

            @pl.when(guest)
            def _():
                guest_back(outward).start()

        def rest(turn, carry):
            tile(turn, False)
            return carry

        tile(0, True)
        lax.fori_loop(1, mine, rest, 0)

        @pl.when(at_end)
        def _():
            guest_there(inward).wait_send()
            r_copy(ftiles - 1).wait()
            mask(ftiles - 1)

        @pl.when(~at_end)
        def _():
            guest_back(outward).wait_send()

    pl.run_scoped(
        forward,
        pltpu.VMEM((dim, ff), BF16), pltpu.VMEM((ff, dim), BF16), pltpu.VMEM((fblock, ff), BF16))

    def backward(dxa):
        def clear(i, carry):
            dxa[frows_of(i), :] = jnp.zeros((fblock, dim), F32)
            return carry

        lax.fori_loop(0, ftiles, clear, 0)

        def tile(m, i, back):
            slot = m % 2
            rows = pl.ds(pl.multiple_of(i * block, block), block)

            if back:
                @pl.when((m == 0) & (i == tiles - 1) & at_end)
                def _():
                    guest_back(inward).wait_recv()
                    xv[frows_of(ftiles - 1), :] = xv[frows_of(ftiles), :]

            if not back:
                @pl.when(m == per_layer)
                def _():
                    for k in range(block // fblock):
                        x_copy(i * (block // fblock) + k).wait()

                    rv[rows, :] = (rv[rows, :].astype(F32) + dxa[rows, :]).astype(BF16)

            x_i, r_i = xv[rows, :], rv[rows, :]
            da_val = dot(r_i, w2v[slot], ((1,), (1,)))
            h_val = dot(x_i, w1v[slot], ((1,), (0,))).astype(BF16).astype(F32)
            sq, th, cdf = gelu_parts(h_val)
            a_val = (h_val * cdf).astype(BF16)
            slope = cdf + (h_val * (0.5 - 0.5 * (th * th))) * (C1 + K3 * sq)
            dh_val = (da_val * slope).astype(BF16)
            if back:
                dxa[rows, :] += dot(dh_val, w1v[slot], ((1,), (1,)))
            own_u[slot] += dot(x_i, dh_val, ((0,), (0,))).reshape(own_u.shape[1:])
            own_v[slot] += dot(a_val, r_i, ((0,), (0,))).reshape(own_v.shape[1:])

        def far_first(zz, going):
            return list(range(CHIPS - 1, zz, -1)) if going > 0 else list(range(zz))

        def held(blk, going):
            return blk - 1 if going > 0 else blk

        def u_copy(m, blk, going, first):
            slot = m % SLOTS
            dst, ssem, qsem = (rr_u, rs_u, rq_u) if going > 0 else (rl_u, ls_u, lq_u)
            at = held(blk, going)
            src = sum_u.at[slot, blk] if first else dst.at[slot, at]
            return remote(src, dst.at[slot, at], ssem.at[blk, slot], qsem.at[blk, slot], me + 2 * going)

        def v_copy(m, p, going, first):
            slot = m % SLOTS
            dst, ssem, qsem = (rr_v, rs_v, rq_v) if going > 0 else (rl_v, ls_v, lq_v)
            src = sum_v if first else dst
            part = pl.ds(p * piece, piece)
            return remote(src.at[slot, part], dst.at[slot, part], ssem.at[p, slot], qsem.at[p, slot], me + 2 * going)

        def beyond(m, zz, going):
            return owner_of(m) > zz if going > 0 else owner_of(m) < zz

        def ends(zz, going):
            start, stop = (0, CHIPS - 1) if going > 0 else (CHIPS - 1, 0)
            return zz == start, zz == stop

        def turn(zz, going):
            return zz if going > 0 else CHIPS - 1 - zz

        def keeps(zz, going):
            return 2 * turn(zz, going) < CHIPS - 1

        def flow(m, zz, going):
            slot = m % SLOTS
            first, last = ends(zz, going)
            keep = keeps(zz, going)
            got_u, credit_u = (rr_u, ru_credit) if going > 0 else (rl_u, lu_credit)
            got_v, credit_v = (rr_v, rv_credit) if going > 0 else (rl_v, lv_credit)

            if not last:
                @pl.when(m >= SLOTS)
                def _():
                    pl.semaphore_wait(credit_u, 1)

                @pl.when((m >= SLOTS) & beyond(m, zz, going))
                def _():
                    pl.semaphore_wait(credit_v, 1)

            def pass_u(blk):
                if not first:
                    u_copy(m, blk, going, False).wait_recv()
                    if blk != zz or keep:
                        got_u[slot, held(blk, going)] += sum_u[slot, blk]
                if blk != zz:
                    u_copy(m, blk, going, first).start()

            blocks = far_first(zz, going) + ([] if first else [zz])
            pass_u(blocks[0])
            if not last:
                @pl.when(beyond(m, zz, going))
                def _():
                    for p in range(PIECES):
                        if not first:
                            part = pl.ds(p * piece, piece)
                            v_copy(m, p, going, False).wait_recv()
                            got_v[slot, part] += sum_v[slot, part]
                        v_copy(m, p, going, first).start()

            if not first:
                @pl.when(owner_of(m) == zz)
                def _():
                    for p in range(PIECES):
                        v_copy(m, p, going, False).wait_recv()
                    if keep:
                        got_v[slot] += sum_v[slot]

            for blk in blocks[1:]:
                pass_u(blk)

        def out_copies_u(m):
            slot = m % 2
            return [
                pltpu.make_async_copy(out_u.at[slot, :, pl.ds(half * unit, unit)],
                                      gu_h.at[layer_of(m), :, pl.ds(start, unit)], ou_sem.at[slot, half])
                for half, start in enumerate(cols_of(m))
            ]

        def out_copy_v(m):
            start = pl.multiple_of(unit * ((m % per_layer) // CHIPS), unit)
            return pltpu.make_async_copy(out_v, gd_h.at[layer_of(m), pl.ds(start, unit), :], ov_sem)

        def terms(zz, total_ref, right_ref, left_ref):
            if zz == 0:
                return total_ref, left_ref
            if zz == CHIPS - 1:
                return total_ref, right_ref
            return right_ref, left_ref

        def finish(m, zz):
            slot = m % SLOTS

            @pl.when(m >= 2)
            def _():
                for cp in out_copies_u(m - 2):
                    cp.wait()

            parts = [sum_u[slot, zz]] if zz in (0, CHIPS - 1) else []
            if zz > 0:
                parts.append(rr_u[slot, held(zz, 1)])
            if zz < CHIPS - 1:
                parts.append(rl_u[slot, held(zz, -1)])
            out_u[m % 2] = parts[0] + parts[1]
            for cp in out_copies_u(m):
                cp.start()

            @pl.when(owner_of(m) == zz)
            def _():
                @pl.when(m >= CHIPS)
                def _():
                    out_copy_v(m - CHIPS).wait()

                one, two = terms(zz, sum_v, rr_v, rl_v)
                out_v[...] = one[slot] + two[slot]
                out_copy_v(m).start()

            again = m < total - SLOTS
            for going in (1, -1):
                first, last = ends(zz, going)
                if not last:
                    for blk in far_first(zz, going):
                        u_copy(m, blk, going, first).wait_send()

                    @pl.when(beyond(m, zz, going))
                    def _():
                        for p in range(PIECES):
                            v_copy(m, p, going, first).wait_send()

                if not first:
                    @pl.when(again)
                    def _():
                        signal(ru_credit if going > 0 else lu_credit, me - 2 * going)

                    @pl.when(again & beyond(m, zz - going, going))
                    def _():
                        signal(rv_credit if going > 0 else lv_credit, me - 2 * going)

        def upto(k, n):
            late = n - total
            draining = jnp.where(late < k, total + 1 - HOP * (k - late), total)
            return jnp.maximum(jnp.where(n < total, n - HOP * k, draining), 0)

        def turns(k, n, body):
            def one(m, carry):
                body(m)
                return carry

            lax.fori_loop(upto(k, n - 1), upto(k, n), one, 0)

        def add_cores(m):
            d_u(m).wait_recv()
            sum_u[m % SLOTS] = own_u[m % 2, :, core] + in_u[...]
            d_u(m).wait_send()

            @pl.when(m < total - 1)
            def _():
                signal(du_credit, peer)

            d_v(m).wait_recv()
            sum_v[m % SLOTS] = own_v[m % 2, core] + in_v[...]
            d_v(m).wait_send()

            @pl.when(m < total - 1)
            def _():
                signal(dv_credit, peer)

        def all_sums(n, drain):
            turns(0, n, add_cores)
            for zz in range(CHIPS):
                @pl.when(z == zz)
                def _():
                    near, far = sorted((1, -1), key=lambda going: turn(zz, going))

                    def go(going):
                        turns(turn(zz, going), n, lambda m: flow(m, zz, going))

                    if not drain or turn(zz, near) == 0:
                        go(near)
                        go(far)
                    else:
                        @pl.when(n < total)
                        def _():
                            go(near)

                        go(far)

                        @pl.when(n >= total)
                        def _():
                            go(near)

                    turns(CHIPS - 1, n, lambda m: finish(m, zz))

        def step(n, back):
            @pl.when(n + 1 < total)
            def _():
                for cp in w_copies(n + 1):
                    cp.start()

            for cp in w_copies(n):
                cp.wait()

            own_u[n % 2] = jnp.zeros(own_u.shape[1:], F32)
            own_v[n % 2] = jnp.zeros(own_v.shape[1:], F32)

            if not back:
                @pl.when(n == per_layer)
                def _():
                    for i in range(ftiles):
                        x_copy(i).start()

            tile(n, 0, back)

        def step_rest(n, back):
            def rest(i, carry):
                tile(n, i, back)
                return carry

            lax.fori_loop(1, tiles, rest, 0)

            @pl.when(n >= 1)
            def _():
                pl.semaphore_wait(du_credit, 1)
                pl.semaphore_wait(dv_credit, 1)

            d_u(n).start()
            d_v(n).start()

        def back_step(n):
            step(n, True)
            all_sums(n, False)
            step_rest(n, True)

        def front_step(n):
            @pl.when(n < total)
            def _():
                step(n, False)

            all_sums(n, True)

            @pl.when(n < total)
            def _():
                step_rest(n, False)

        def steps(lo, hi, body):
            def one(n, carry):
                body(n)
                return carry

            lax.fori_loop(lo, hi, one, 0)

        steps(0, per_layer, back_step)
        steps(per_layer, total + CHIPS, front_step)

        for m in (total - 2, total - 1):
            for cp in out_copies_u(m):
                cp.wait()
        out_copy_v(total - CHIPS).wait()

    pl.run_scoped(backward, pltpu.VMEM(rv.shape, F32))


def gradients(x0, g, lengths, w_up, w_down, block, fblock, unit):
    toks, dim = x0.shape
    micro = lengths.shape[0]
    layers, _, ff = w_up.shape
    rows_u = dim // (2 * CHIPS)
    wide = 2 * unit
    ftiles = toks // fblock
    held = toks + fblock
    dma = pltpu.SemaphoreType.DMA
    vm = pltpu.VMEM
    u_blk = (CHIPS, rows_u, wide)
    line_blk = (CHIPS - 1, rows_u, wide)
    v_blk = (unit, dim)
    scratch = [
        vm((held, dim), BF16), vm((toks, dim), BF16),
        vm((2, dim, wide), BF16), vm((2, wide, dim), BF16),
        vm((2, CHIPS, 2, rows_u, wide), F32), vm((2, 2) + v_blk, F32),
        vm(u_blk, F32), vm(v_blk, F32),
        vm((SLOTS,) + u_blk, F32), vm((SLOTS,) + v_blk, F32),
        vm((SLOTS,) + line_blk, F32), vm((SLOTS,) + v_blk, F32),
        vm((SLOTS,) + line_blk, F32), vm((SLOTS,) + v_blk, F32),
        vm((2, rows_u, wide), F32), vm(v_blk, F32),
        dma((ftiles,)), dma((ftiles,)), dma((2, 4)), dma((PARTS + 1,)), dma((2,)), dma((2,)), dma((2,)), dma((2,)),
    ] + [dma((CHIPS, SLOTS))] * 4 + [dma((PIECES, SLOTS))] * 4 + [dma((2, 2)), dma] + [pltpu.SemaphoreType.REGULAR] * 6
    any_space = pl.BlockSpec(memory_space=pl.ANY)
    return pl.pallas_call(
        functools.partial(kernel, unit, block, fblock, micro),
        out_shape=[
            jax.ShapeDtypeStruct((layers, rows_u, ff), F32),
            jax.ShapeDtypeStruct((layers, ff // (2 * CHIPS), dim), F32),
        ],
        in_specs=[pl.BlockSpec(memory_space=pltpu.SMEM)] + [any_space] * 4,
        out_specs=[any_space] * 2,
        scratch_shapes=scratch,
        compiler_params=pltpu.CompilerParams(
            collective_id=0, has_side_effects=True, vmem_limit_bytes=67_043_328),
        name="grads",
    )(lengths, x0, g, w_up, w_down)


def hand_on_kernel(cuts, u_in, v_in, u_out, v_out, u_held, v_held, in_sem, out_sem):
    jobs = []
    for src, held, dst in ((v_in, v_held, v_out), (u_in, u_held, u_out)):
        rows = src.shape[1] // cuts
        for layer in range(src.shape[0]):
            for cut in range(cuts):
                part = pl.ds(cut * rows, rows)
                k = len(jobs)
                jobs.append((
                    pltpu.make_async_copy(src.at[layer, part], held.at[layer, part], in_sem.at[k]),
                    pltpu.make_async_copy(held.at[layer, part], dst.at[layer, part], out_sem.at[k])))
    for get, _ in jobs:
        get.start()
    for get, put in jobs:
        get.wait()
        put.start()
    for _, put in jobs:
        put.wait()


def hand_on(u, v, cuts=CUTS):
    any_space = pl.BlockSpec(memory_space=pl.ANY)
    count = 2 * cuts * u.shape[0]
    return pl.pallas_call(
        functools.partial(hand_on_kernel, cuts),
        out_shape=[jax.ShapeDtypeStruct(u.shape, F32), jax.ShapeDtypeStruct(v.shape, F32)],
        in_specs=[any_space] * 2,
        out_specs=[any_space] * 2,
        scratch_shapes=[pltpu.VMEM(u.shape, F32), pltpu.VMEM(v.shape, F32),
                        pltpu.SemaphoreType.DMA((count,)), pltpu.SemaphoreType.DMA((count,))],
        compiler_params=pltpu.CompilerParams(vmem_limit_bytes=62 * 1024 * 1024),
        name="hand_on",
    )(u, v)


def solution(mesh, block=1024, fblock=512, unit=128):
    def local_step(acts_in, cot_out, lengths, w_up, w_down):
        micro, tok_rows, dim = acts_in.shape
        x0 = acts_in.reshape(micro * tok_rows, dim)
        g = cot_out.reshape(micro * tok_rows, dim)
        return tuple(hand_on(*gradients(x0, g, lengths.reshape(micro), w_up, w_down, block, fblock, unit)))

    act_spec = P(None, ("part", "fsdp"), None)
    grad_spec = P("part", "fsdp", None)
    return jax.shard_map(
        local_step, mesh=mesh,
        in_specs=(act_spec, act_spec, P(None, ("part", "fsdp")), P(), P()),
        out_specs=(grad_spec, grad_spec), check_vma=False)
```

```python
import functools

import jax
import jax.numpy as jnp
from jax import lax
from jax.experimental import pallas as pl
from jax.experimental.pallas import tpu as pltpu
from jax.sharding import PartitionSpec as P

MESH = pl.DeviceIdType.MESH
F32 = jnp.float32
BF16 = jnp.bfloat16

C1 = 0.7978845608028654
K1 = C1 * 0.044715
K3 = 3.0 * K1

CHIPS = 4
HOP = 2
SLOTS = 8
PIECES = 4
PARTS = 4


def dot(lhs, rhs, dims):
    return lax.dot_general(lhs, rhs, (dims, ((), ())), preferred_element_type=F32)


def gelu_parts(h_wide):
    sq = h_wide * h_wide
    th = jnp.tanh(h_wide * (C1 + K1 * sq))
    return sq, th, 0.5 + 0.5 * th


def kernel(unit, block, fblock, micro, len_s, x0_h, g_h, wu_h, wd_h, gu_h, gd_h,
           xv, rv, w1v, w2v, own_u, own_v, in_u, in_v, sum_u, sum_v,
           rr_u, rr_v, rl_u, rl_v, out_u, out_v,
           x_sem, r_sem, w_sem, f_sem, t_send, t_recv, ds_sem, dr_sem,
           rs_u, rq_u, ls_u, lq_u, rs_v, rq_v, ls_v, lq_v,
           ou_sem, ov_sem, du_credit, dv_credit, ru_credit, lu_credit, rv_credit, lv_credit):
    toks, dim = x0_h.shape
    layers, _, ff = wu_h.shape
    tiles = toks // block
    ftiles = toks // fblock
    piece = unit // PIECES
    wide = 2 * unit
    per_dev = ff // (2 * CHIPS)
    per_layer = ff // wide
    total = layers * per_layer

    me = lax.axis_index("fsdp")
    z = me // 2
    core = me % 2
    peer = z * 2 + (1 - core)
    at_end = (z == 0) | (z == CHIPS - 1)
    inward = jnp.where(z < CHIPS // 2, me + 2, me - 2)
    outward = jnp.where(z < CHIPS // 2, me - 2, me + 2)
    mine = jnp.where(at_end, ftiles - 1, ftiles + 1)
    guest_turn = ftiles // 2

    def signal(sem, dev):
        pl.semaphore_signal(sem, inc=1, device_id={"fsdp": dev}, device_id_type=MESH)

    def remote(src, dst, ssem, rsem, dev):
        return pltpu.make_async_remote_copy(
            src_ref=src, dst_ref=dst, send_sem=ssem, recv_sem=rsem,
            device_id={"fsdp": dev}, device_id_type=MESH)

    barrier = pltpu.get_barrier_semaphore()
    signal(barrier, peer)

    @pl.when(z > 0)
    def _():
        signal(barrier, me - 2)

    @pl.when(z < CHIPS - 1)
    def _():
        signal(barrier, me + 2)

    def layer_of(m):
        return layers - 1 - m // per_layer

    def owner_of(m):
        return (1 + 3 * (m % per_layer)) % CHIPS

    def cols_of(m):
        base = 2 * per_dev * owner_of(m) + unit * ((m % per_layer) // CHIPS)
        return pl.multiple_of(base, unit), pl.multiple_of(base + per_dev, unit)

    def w_copies(m):
        slot = m % 2
        out = []
        for half, start in enumerate(cols_of(m)):
            span = pl.ds(start, unit)
            here = pl.ds(half * unit, unit)
            out.append(pltpu.make_async_copy(
                wu_h.at[layer_of(m), :, span], w1v.at[slot, :, here], w_sem.at[slot, half]))
            out.append(pltpu.make_async_copy(
                wd_h.at[layer_of(m), span, :], w2v.at[slot, here, :], w_sem.at[slot, 2 + half]))
        return out

    def frows_of(i):
        return pl.ds(pl.multiple_of(i * fblock, fblock), fblock)

    def x_copy(i):
        return pltpu.make_async_copy(x0_h.at[frows_of(i), :], xv.at[frows_of(i), :], x_sem.at[i])

    def r_copy(i):
        return pltpu.make_async_copy(g_h.at[frows_of(i), :], rv.at[frows_of(i), :], r_sem.at[i])

    def mask(i):
        per = ftiles // micro
        left = len_s[i // per] - (i % per) * fblock
        r_val = rv[frows_of(i), :]
        row_ids = lax.broadcasted_iota(jnp.int32, r_val.shape, 0)
        rv[frows_of(i), :] = jnp.where(row_ids < left, r_val, jnp.zeros_like(r_val))

    def guest_there(dev):
        return remote(xv.at[frows_of(ftiles - 1), :], xv.at[frows_of(ftiles), :], t_send.at[0], t_recv.at[0], dev)

    def guest_back(dev):
        rows = frows_of(ftiles)
        return remote(xv.at[rows, :], xv.at[rows, :], t_send.at[1], t_recv.at[1], dev)

    def d_u(m):
        return remote(own_u.at[m % 2, :, 1 - core], in_u, ds_sem.at[0], dr_sem.at[0], peer)

    def d_v(m):
        return remote(own_v.at[m % 2, 1 - core], in_v, ds_sem.at[1], dr_sem.at[1], peer)

    def forward(w1f, w2f, a_scr):
        width = ff // PARTS

        def w1_copy(part):
            cols = pl.ds(part * width, width)
            return pltpu.make_async_copy(wu_h.at[0, :, cols], w1f.at[:, cols], f_sem.at[part])

        w2_copy = pltpu.make_async_copy(wd_h.at[0], w2f, f_sem.at[PARTS])
        @pl.when(at_end)
        def _():
            x_copy(ftiles - 1).start()

        for i in range(ftiles):
            if i < ftiles - 1:
                x_copy(i).start()
            if i == 0:
                for part in range(PARTS):
                    w1_copy(part).start()
                w2_copy.start()
            r_copy(i).start()

        @pl.when(~at_end)
        def _():
            x_copy(ftiles - 1).start()

        for cp in w_copies(0):
            cp.start()
        peers = 1 + jnp.where(z > 0, 1, 0) + jnp.where(z < CHIPS - 1, 1, 0)
        pl.semaphore_wait(barrier, peers)

        @pl.when(at_end)
        def _():
            x_copy(ftiles - 1).wait()
            guest_there(inward).start()

        def tile(turn, first):
            guest = ~at_end & (turn == guest_turn)
            i = jnp.where(guest, ftiles, jnp.where(~at_end & (turn > guest_turn), turn - 1, turn))

            @pl.when(guest)
            def _():
                guest_there(outward).wait_recv()

            @pl.when(~guest)
            def _():
                x_copy(i).wait()
                r_copy(i).wait()
                mask(i)

            x_val = xv[frows_of(i), :]
            for part in range(PARTS):
                cols = slice(part * width, (part + 1) * width)

                if first:
                    w1_copy(part).wait()
                h_val = dot(x_val, w1f[:, cols], ((1,), (0,))).astype(BF16).astype(F32)
                _, _, cdf = gelu_parts(h_val)
                a_scr[:, cols] = (h_val * cdf).astype(BF16)

            if first:
                w2_copy.wait()
            y_val = dot(a_scr[...], w2f[...], ((1,), (0,))).astype(BF16)
            xv[frows_of(i), :] = (x_val.astype(F32) + y_val.astype(F32)).astype(BF16)

            @pl.when(guest)
            def _():
                guest_back(outward).start()

        def rest(turn, carry):
            tile(turn, False)
            return carry

        tile(0, True)
        lax.fori_loop(1, mine, rest, 0)

        @pl.when(at_end)
        def _():
            guest_there(inward).wait_send()
            r_copy(ftiles - 1).wait()
            mask(ftiles - 1)

        @pl.when(~at_end)
        def _():
            guest_back(outward).wait_send()

    pl.run_scoped(
        forward,
        pltpu.VMEM((dim, ff), BF16), pltpu.VMEM((ff, dim), BF16), pltpu.VMEM((fblock, ff), BF16))

    def backward(dxa):
        def clear(i, carry):
            dxa[frows_of(i), :] = jnp.zeros((fblock, dim), F32)
            return carry

        lax.fori_loop(0, ftiles, clear, 0)

        def tile(m, i, back):
            slot = m % 2
            rows = pl.ds(pl.multiple_of(i * block, block), block)

            if back:
                @pl.when((m == 0) & (i == tiles - 1) & at_end)
                def _():
                    guest_back(inward).wait_recv()
                    xv[frows_of(ftiles - 1), :] = xv[frows_of(ftiles), :]

            @pl.when(m == per_layer)
            def _():
                for k in range(block // fblock):
                    x_copy(i * (block // fblock) + k).wait()

                rv[rows, :] = (rv[rows, :].astype(F32) + dxa[rows, :]).astype(BF16)

            x_i, r_i = xv[rows, :], rv[rows, :]
            da_val = dot(r_i, w2v[slot], ((1,), (1,)))
            h_val = dot(x_i, w1v[slot], ((1,), (0,))).astype(BF16).astype(F32)
            sq, th, cdf = gelu_parts(h_val)
            a_val = (h_val * cdf).astype(BF16)
            slope = cdf + (h_val * (0.5 - 0.5 * (th * th))) * (C1 + K3 * sq)
            dh_val = (da_val * slope).astype(BF16)
            if back:
                dxa[rows, :] += dot(dh_val, w1v[slot], ((1,), (1,)))
            own_u[slot] += dot(x_i, dh_val, ((0,), (0,))).reshape(own_u.shape[1:])
            own_v[slot] += dot(a_val, r_i, ((0,), (0,))).reshape(own_v.shape[1:])

        def far_first(zz, going):
            return list(range(CHIPS - 1, zz, -1)) if going > 0 else list(range(zz))

        def held(blk, going):
            return blk - 1 if going > 0 else blk

        def u_copy(m, blk, going, first):
            slot = m % SLOTS
            dst, ssem, qsem = (rr_u, rs_u, rq_u) if going > 0 else (rl_u, ls_u, lq_u)
            at = held(blk, going)
            src = sum_u.at[slot, blk] if first else dst.at[slot, at]
            return remote(src, dst.at[slot, at], ssem.at[blk, slot], qsem.at[blk, slot], me + 2 * going)

        def v_copy(m, p, going, first):
            slot = m % SLOTS
            dst, ssem, qsem = (rr_v, rs_v, rq_v) if going > 0 else (rl_v, ls_v, lq_v)
            src = sum_v if first else dst
            part = pl.ds(p * piece, piece)
            return remote(src.at[slot, part], dst.at[slot, part], ssem.at[p, slot], qsem.at[p, slot], me + 2 * going)

        def beyond(m, zz, going):
            return owner_of(m) > zz if going > 0 else owner_of(m) < zz

        def ends(zz, going):
            start, stop = (0, CHIPS - 1) if going > 0 else (CHIPS - 1, 0)
            return zz == start, zz == stop

        def turn(zz, going):
            return zz if going > 0 else CHIPS - 1 - zz

        def keeps(zz, going):
            return 2 * turn(zz, going) < CHIPS - 1

        def flow(m, zz, going, parts=(True, True)):
            slot = m % SLOTS
            first, last = ends(zz, going)
            keep = keeps(zz, going)
            got_u, credit_u = (rr_u, ru_credit) if going > 0 else (rl_u, lu_credit)
            got_v, credit_v = (rr_v, rv_credit) if going > 0 else (rl_v, lv_credit)

            if not last and parts[0]:
                @pl.when(m >= SLOTS)
                def _():
                    pl.semaphore_wait(credit_u, 1)

                @pl.when((m >= SLOTS) & beyond(m, zz, going))
                def _():
                    pl.semaphore_wait(credit_v, 1)

            def pass_u(blk):
                if not first:
                    u_copy(m, blk, going, False).wait_recv()
                    if blk != zz or keep:
                        got_u[slot, held(blk, going)] += sum_u[slot, blk]
                if blk != zz:
                    u_copy(m, blk, going, first).start()

            blocks = far_first(zz, going) + ([] if first else [zz])
            if parts[0]:
                pass_u(blocks[0])
            if not last and parts[0]:
                @pl.when(beyond(m, zz, going))
                def _():
                    for p in range(PIECES):
                        if not first:
                            part = pl.ds(p * piece, piece)
                            v_copy(m, p, going, False).wait_recv()
                            got_v[slot, part] += sum_v[slot, part]
                        v_copy(m, p, going, first).start()

            if not first and parts[0]:
                @pl.when(owner_of(m) == zz)
                def _():
                    for p in range(PIECES):
                        v_copy(m, p, going, False).wait_recv()
                    if keep:
                        got_v[slot] += sum_v[slot]

            for blk in blocks[1:] if parts[1] else ():
                pass_u(blk)

        def out_copies_u(m):
            slot = m % 2
            return [
                pltpu.make_async_copy(out_u.at[slot, :, pl.ds(half * unit, unit)],
                                      gu_h.at[layer_of(m), :, pl.ds(start, unit)], ou_sem.at[slot, half])
                for half, start in enumerate(cols_of(m))
            ]

        def out_copy_v(m):
            start = pl.multiple_of(unit * ((m % per_layer) // CHIPS), unit)
            return pltpu.make_async_copy(out_v, gd_h.at[layer_of(m), pl.ds(start, unit), :], ov_sem)

        def terms(zz, total_ref, right_ref, left_ref):
            if zz == 0:
                return total_ref, left_ref
            if zz == CHIPS - 1:
                return total_ref, right_ref
            return right_ref, left_ref

        def finish(m, zz):
            slot = m % SLOTS

            @pl.when(m >= 2)
            def _():
                for cp in out_copies_u(m - 2):
                    cp.wait()

            parts = [sum_u[slot, zz]] if zz in (0, CHIPS - 1) else []
            if zz > 0:
                parts.append(rr_u[slot, held(zz, 1)])
            if zz < CHIPS - 1:
                parts.append(rl_u[slot, held(zz, -1)])
            out_u[m % 2] = parts[0] + parts[1]
            for cp in out_copies_u(m):
                cp.start()

            @pl.when(owner_of(m) == zz)
            def _():
                @pl.when(m >= CHIPS)
                def _():
                    out_copy_v(m - CHIPS).wait()

                one, two = terms(zz, sum_v, rr_v, rl_v)
                out_v[...] = one[slot] + two[slot]
                out_copy_v(m).start()

            again = m < total - SLOTS
            for going in (1, -1):
                first, last = ends(zz, going)
                if not last:
                    for blk in far_first(zz, going):
                        u_copy(m, blk, going, first).wait_send()

                    @pl.when(beyond(m, zz, going))
                    def _():
                        for p in range(PIECES):
                            v_copy(m, p, going, first).wait_send()

                if not first:
                    @pl.when(again)
                    def _():
                        signal(ru_credit if going > 0 else lu_credit, me - 2 * going)

                    @pl.when(again & beyond(m, zz - going, going))
                    def _():
                        signal(rv_credit if going > 0 else lv_credit, me - 2 * going)

        def upto(k, n):
            late = n - total
            draining = jnp.where(late < k, total + 1 - HOP * (k - late), total)
            return jnp.maximum(jnp.where(n < total, n - HOP * k, draining), 0)

        def turns(k, n, body, limit=total):
            def one(m, carry):
                body(m)
                return carry

            lax.fori_loop(upto(k, n - 1), jnp.minimum(upto(k, n), limit), one, 0)

        def add_cores(m):
            d_u(m).wait_recv()
            sum_u[m % SLOTS] = own_u[m % 2, :, core] + in_u[...]
            d_u(m).wait_send()

            @pl.when(m < total - 1)
            def _():
                signal(du_credit, peer)

            d_v(m).wait_recv()
            sum_v[m % SLOTS] = own_v[m % 2, core] + in_v[...]
            d_v(m).wait_send()

            @pl.when(m < total - 1)
            def _():
                signal(dv_credit, peer)

        def all_sums(n):
            turns(0, n, add_cores)
            for zz in range(CHIPS):
                @pl.when(z == zz)
                def _():
                    near, far = sorted((1, -1), key=lambda going: turn(zz, going))

                    k_near, k_far = turn(zz, near), turn(zz, far)
                    end = total if k_near == 0 else total - 1

                    def go(going, k):
                        turns(k, n, lambda m: flow(m, zz, going), end)

                    if k_near == 0:
                        go(near, k_near)
                        go(far, k_far)
                    else:
                        @pl.when(n < total)
                        def _():
                            go(near, k_near)

                        go(far, k_far)

                        @pl.when(n >= total)
                        def _():
                            go(near, k_near)

                        @pl.when(n == total + k_near)
                        def _():
                            flow(end, zz, near, (True, False))
                            flow(end, zz, far, (True, False))
                            flow(end, zz, near, (False, True))

                        @pl.when(n == total + k_far)
                        def _():
                            flow(end, zz, far, (False, True))

                    turns(CHIPS - 1, n, lambda m: finish(m, zz))

        def step(n, carry):
            run = n < total

            @pl.when(run)
            def _():
                @pl.when(n + 1 < total)
                def _():
                    for cp in w_copies(n + 1):
                        cp.start()

                for cp in w_copies(n):
                    cp.wait()

                own_v[n % 2] = jnp.zeros(own_v.shape[1:], F32)
                own_u[n % 2] = jnp.zeros(own_u.shape[1:], F32)

                @pl.when(n == per_layer)
                def _():
                    for i in range(ftiles):
                        x_copy(i).start()


            def half(phase, c):
                lo = phase
                hi = jnp.where(phase == 0, 1, tiles)

                def loop(cond, back):
                    @pl.when(cond)
                    def _():
                        def body(i, cc):
                            tile(n, i, back)
                            return cc

                        lax.fori_loop(lo, hi, body, 0)

                loop(run & (n < per_layer), True)
                loop(run & (n >= per_layer), False)

                @pl.when(run & (phase == 1))
                def _():
                    @pl.when(n >= 1)
                    def _():
                        pl.semaphore_wait(du_credit, 1)
                        pl.semaphore_wait(dv_credit, 1)

                    d_u(n).start()
                    d_v(n).start()

                @pl.when(phase == 0)
                def _():
                    all_sums(n)

                return c

            lax.fori_loop(0, 2, half, 0)
            return carry

        lax.fori_loop(0, total + CHIPS, step, 0)

        for m in (total - 2, total - 1):
            for cp in out_copies_u(m):
                cp.wait()
        out_copy_v(total - CHIPS).wait()

    pl.run_scoped(backward, pltpu.VMEM(rv.shape, F32))


def gradients(x0, g, lengths, w_up, w_down, block, fblock, unit):
    toks, dim = x0.shape
    micro = lengths.shape[0]
    layers, _, ff = w_up.shape
    rows_u = dim // (2 * CHIPS)
    wide = 2 * unit
    ftiles = toks // fblock
    held = toks + fblock
    dma = pltpu.SemaphoreType.DMA
    vm = pltpu.VMEM
    u_blk = (CHIPS, rows_u, wide)
    line_blk = (CHIPS - 1, rows_u, wide)
    v_blk = (unit, dim)
    scratch = [
        vm((held, dim), BF16), vm((toks, dim), BF16),
        vm((2, dim, wide), BF16), vm((2, wide, dim), BF16),
        vm((2, CHIPS, 2, rows_u, wide), F32), vm((2, 2) + v_blk, F32),
        vm(u_blk, F32), vm(v_blk, F32),
        vm((SLOTS,) + u_blk, F32), vm((SLOTS,) + v_blk, F32),
        vm((SLOTS,) + line_blk, F32), vm((SLOTS,) + v_blk, F32),
        vm((SLOTS,) + line_blk, F32), vm((SLOTS,) + v_blk, F32),
        vm((2, rows_u, wide), F32), vm(v_blk, F32),
        dma((ftiles,)), dma((ftiles,)), dma((2, 4)), dma((PARTS + 1,)), dma((2,)), dma((2,)), dma((2,)), dma((2,)),
    ] + [dma((CHIPS, SLOTS))] * 4 + [dma((PIECES, SLOTS))] * 4 + [dma((2, 2)), dma] + [pltpu.SemaphoreType.REGULAR] * 6
    any_space = pl.BlockSpec(memory_space=pl.ANY)
    return pl.pallas_call(
        functools.partial(kernel, unit, block, fblock, micro),
        out_shape=[
            jax.ShapeDtypeStruct((layers, rows_u, ff), F32),
            jax.ShapeDtypeStruct((layers, ff // (2 * CHIPS), dim), F32),
        ],
        in_specs=[pl.BlockSpec(memory_space=pltpu.SMEM)] + [any_space] * 4,
        out_specs=[any_space] * 2,
        scratch_shapes=scratch,
        compiler_params=pltpu.CompilerParams(
            collective_id=0, has_side_effects=True, vmem_limit_bytes=67_043_328),
        name="grads",
    )(lengths, x0, g, w_up, w_down)


def hand_on_kernel(cuts, u_in, v_in, u_out, v_out, u_held, v_held, in_sem, out_sem):
    jobs = []
    for src, held, dst in ((v_in, v_held, v_out), (u_in, u_held, u_out)):
        rows = src.shape[1] // cuts
        for layer in range(src.shape[0]):
            for cut in range(cuts):
                part = pl.ds(cut * rows, rows)
                k = len(jobs)
                jobs.append((
                    pltpu.make_async_copy(src.at[layer, part], held.at[layer, part], in_sem.at[k]),
                    pltpu.make_async_copy(held.at[layer, part], dst.at[layer, part], out_sem.at[k])))
    for get, _ in jobs:
        get.start()
    for get, put in jobs:
        get.wait()
        put.start()
    for _, put in jobs:
        put.wait()


def hand_on(u, v, cuts=2):
    any_space = pl.BlockSpec(memory_space=pl.ANY)
    count = 2 * cuts * u.shape[0]
    return pl.pallas_call(
        functools.partial(hand_on_kernel, cuts),
        out_shape=[jax.ShapeDtypeStruct(u.shape, F32), jax.ShapeDtypeStruct(v.shape, F32)],
        in_specs=[any_space] * 2,
        out_specs=[any_space] * 2,
        scratch_shapes=[pltpu.VMEM(u.shape, F32), pltpu.VMEM(v.shape, F32),
                        pltpu.SemaphoreType.DMA((count,)), pltpu.SemaphoreType.DMA((count,))],
        compiler_params=pltpu.CompilerParams(vmem_limit_bytes=62 * 1024 * 1024),
        name="hand_on",
    )(u, v)


def solution(mesh, block=1024, fblock=512, unit=128):
    def local_step(acts_in, cot_out, lengths, w_up, w_down):
        micro, tok_rows, dim = acts_in.shape
        x0 = acts_in.reshape(micro * tok_rows, dim)
        g = cot_out.reshape(micro * tok_rows, dim)
        return tuple(hand_on(*gradients(x0, g, lengths.reshape(micro), w_up, w_down, block, fblock, unit)))

    act_spec = P(None, ("part", "fsdp"), None)
    grad_spec = P("part", "fsdp", None)
    return jax.shard_map(
        local_step, mesh=mesh,
        in_specs=(act_spec, act_spec, P(None, ("part", "fsdp")), P(), P()),
        out_specs=(grad_spec, grad_spec), check_vma=False)
```
